256 devices in a mesh: rep: 1, dp: 256 (over x, y, z, core).
Axes of the slice: x: 4, y: 4, z: 8, core: 2. Of those that a mesh axis runs over, the one named last changes fastest.
Arguments:
- x: bfloat16 [256, 1024, 768], P(('rep', 'dp'))
- dy: bfloat16 [256, 1024, 768], P(('rep', 'dp'))
- wq: bfloat16 [1, 768, 768], replicated
- wk: bfloat16 [1, 768, 256], replicated
- wv: bfloat16 [1, 768, 256], replicated
- wo: bfloat16 [1, 768, 768], replicated
- w_gate: bfloat16 [1, 768, 2304], replicated
- w_up: bfloat16 [1, 768, 2304], replicated
- w_down: bfloat16 [1, 2304, 768], replicated
- m_wq: float32 [1, 768, 768], P(None, 'dp')
- m_wk: float32 [1, 768, 256], P(None, 'dp')
- m_wv: float32 [1, 768, 256], P(None, 'dp')
- m_wo: float32 [1, 768, 768], P(None, 'dp')
- m_w_gate: float32 [1, 768, 2304], P(None, 'dp')
- m_w_up: float32 [1, 768, 2304], P(None, 'dp')
- m_w_down: float32 [1, 2304, 768], P(None, 'dp')
- v_wq: float32 [1, 768, 768], P(None, 'dp')
- v_wk: float32 [1, 768, 256], P(None, 'dp')
- v_wv: float32 [1, 768, 256], P(None, 'dp')
- v_wo: float32 [1, 768, 768], P(None, 'dp')
- v_w_gate: float32 [1, 768, 2304], P(None, 'dp')
- v_w_up: float32 [1, 768, 2304], P(None, 'dp')
- v_w_down: float32 [1, 2304, 768], P(None, 'dp')
Outputs:
- output 1: bfloat16 [1, 768, 768], P('rep')
- output 2: bfloat16 [1, 768, 256], P('rep')
- output 3: bfloat16 [1, 768, 256], P('rep')
- output 4: bfloat16 [1, 768, 768], P('rep')
- output 5: bfloat16 [1, 768, 2304], P('rep')
- output 6: bfloat16 [1, 768, 2304], P('rep')
- output 7: bfloat16 [1, 2304, 768], P('rep')
- output 8: float32 [1, 768, 768], P('rep', 'dp')
- output 9: float32 [1, 768, 256], P('rep', 'dp')
- output 10: float32 [1, 768, 256], P('rep', 'dp')
- output 11: float32 [1, 768, 768], P('rep', 'dp')
- output 12: float32 [1, 768, 2304], P('rep', 'dp')
- output 13: float32 [1, 768, 2304], P('rep', 'dp')
- output 14: float32 [1, 2304, 768], P('rep', 'dp')
- output 15: float32 [1, 768, 768], P('rep', 'dp')
- output 16: float32 [1, 768, 256], P('rep', 'dp')
- output 17: float32 [1, 768, 256], P('rep', 'dp')
- output 18: float32 [1, 768, 768], P('rep', 'dp')
- output 19: float32 [1, 768, 2304], P('rep', 'dp')
- output 20: float32 [1, 768, 2304], P('rep', 'dp')
- output 21: float32 [1, 2304, 768], P('rep', 'dp')
All inputs are finite; a program needn't handle non-finite values.
Results may differ from the reference program's by a relative error of at most 0.024.
Values are sent between devices in bfloat16 or wider.
A program may use at most 768 MiB of HBM per device.

```python
import jax
import jax.numpy as jnp
from jax import lax

SEQUENCES = 256
TOKENS = 1024
D = 768
HEADS = 6
KV_HEADS = 2
HEAD = 128
FF = 2304
LAYERS = 1
THETA = 10000
NAMES = ("wq", "wk", "wv", "wo", "w_gate", "w_up", "w_down")
SHAPES = {
    "wq": (LAYERS, D, HEADS * HEAD),
    "wk": (LAYERS, D, KV_HEADS * HEAD),
    "wv": (LAYERS, D, KV_HEADS * HEAD),
    "wo": (LAYERS, HEADS * HEAD, D),
    "w_gate": (LAYERS, D, FF),
    "w_up": (LAYERS, D, FF),
    "w_down": (LAYERS, FF, D),
}


def bump(key, n, height):
    away = (jnp.arange(n, dtype=jnp.int32) - jax.random.randint(key, (), 0, n, jnp.int32)) % n
    return jnp.where(away < n // 8, height, 1.0)


def together(key, own, strength):
    shared = jax.random.normal(key, own.shape[1:], jnp.float32)
    return (own + strength * shared) * lax.rsqrt(1 + strength * strength)


def setup_inputs(seed: int = 0, part: int = 0) -> dict:
    kx, kdy, ka, kb, kz, kf, kh, kl, *keys = jax.random.split(jax.random.key(seed), 8 + 3 * len(NAMES))
    kx, kdy, ka, kb = (jax.random.fold_in(k, part) for k in (kx, kdy, ka, kb))
    kw, km, kv = (keys[i::3] for i in range(3))
    shape = (SEQUENCES, TOKENS, D)
    much_x, much_dy = jax.random.uniform(kz, (2,), jnp.float32, 0.0, 1.0)
    loud = 2.0 ** jax.random.uniform(jax.random.fold_in(kz, 1), (), jnp.float32, -1.0, 2.0)
    layers = 2.0 ** jax.random.uniform(kl, (LAYERS, 1, 1), jnp.float32, -1.0, 1.0)
    times = {"wq": 1.0, "wk": 1.0, "wv": 2.0, "wo": layers, "w_gate": 1.0, "w_up": bump(kh, FF, 4.0), "w_down": layers}
    x = together(ka, jax.random.normal(kx, shape, jnp.float32), much_x) * bump(kf, D, 4.0)
    dy = together(kb, jax.random.normal(kdy, shape, jnp.float32), much_dy)
    drawn = {"x": x.astype(jnp.bfloat16), "dy": (loud * dy * (SEQUENCES * TOKENS) ** -0.5).astype(jnp.bfloat16)}
    for key, name in zip(kw, NAMES, strict=True):
        drawn[name] = (jax.random.normal(key, SHAPES[name], jnp.float32) * SHAPES[name][1] ** -0.5 * times[name]).astype(jnp.bfloat16)
    for key, name in zip(km, NAMES, strict=True):
        drawn[f"m_{name}"] = 0.1 * jax.random.normal(key, SHAPES[name], jnp.float32)
    for key, name in zip(kv, NAMES, strict=True):
        drawn[f"v_{name}"] = jax.random.uniform(key, SHAPES[name], jnp.float32, 0.02, 0.06)
    return drawn


def matmul(a, w):
    return jnp.dot(a, w, preferred_element_type=jnp.float32).astype(jnp.bfloat16)


def normed(h):
    wide = h.astype(jnp.float32)
    scale = lax.rsqrt(jnp.mean(wide**2, -1, keepdims=True) + 1e-6)
    return (wide * scale).astype(jnp.bfloat16)


def turned(t, theta):
    half = t.shape[-1] // 2
    angle = jnp.arange(t.shape[0], dtype=jnp.float32)[:, None] * theta ** (-jnp.arange(half, dtype=jnp.float32) / half)
    cos, sin = jnp.cos(angle)[:, None], jnp.sin(angle)[:, None]
    a, b = t[..., :half].astype(jnp.float32), t[..., half:].astype(jnp.float32)
    return jnp.concatenate([a * cos - b * sin, b * cos + a * sin], -1).astype(jnp.bfloat16)


def seen_by(q, k, v):
    tokens, kv = q.shape[0], k.shape[1]
    q = q.reshape(tokens, kv, -1, q.shape[-1])
    scores = jnp.einsum("tgsd,ugd->gstu", q.astype(jnp.float32), k.astype(jnp.float32)) * q.shape[-1] ** -0.5
    place = jnp.arange(tokens)
    weights = jax.nn.softmax(jnp.where(place[:, None] >= place, scores, -jnp.inf), -1).astype(jnp.bfloat16)
    return jnp.einsum("gstu,ugd->tgsd", weights.astype(jnp.float32), v.astype(jnp.float32)).astype(jnp.bfloat16).reshape(tokens, -1)


def layer(h, w):
    a = normed(h)
    q, k = (turned(matmul(a, w[name]).reshape(h.shape[0], -1, HEAD), THETA) for name in ("wq", "wk"))
    h = h + matmul(seen_by(q, k, matmul(a, w["wv"]).reshape(h.shape[0], -1, HEAD)), w["wo"])
    b = normed(h)
    gate = jnp.dot(b, w["w_gate"], preferred_element_type=jnp.float32)
    up = jnp.dot(b, w["w_up"], preferred_element_type=jnp.float32)
    return h + matmul((jax.nn.silu(gate) * up).astype(jnp.bfloat16), w["w_down"])


def adamw(w, m, v, g):
    m = 0.9 * m + 0.1 * g
    v = 0.95 * v + 0.05 * g * g
    step = m * lax.rsqrt(v + 1e-8) + 0.1 * w
    return (w - 0.02 * step).astype(jnp.bfloat16), m, v


def clipped(gradients, sum_of_squares, count):
    factor = jnp.minimum(1.0, 0.5 * lax.rsqrt(sum_of_squares / count + 1e-30))
    return [g * factor for g in gradients]


def stack(weights, h):
    return lax.scan(lambda h, w: (layer(h, w), None), h, weights)[0]


def reference(x, dy, wq, wk, wv, wo, w_gate, w_up, w_down, m_wq, m_wk, m_wv, m_wo, m_w_gate, m_w_up, m_w_down, v_wq, v_wk, v_wv, v_wo, v_w_gate, v_w_up, v_w_down):
    weights = dict(zip(NAMES, (wq, wk, wv, wo, w_gate, w_up, w_down), strict=True))

    def take(so_far, sequence):
        h, by_y = sequence
        _, back = jax.vjp(stack, weights, h)
        by_weights, by_h = back(by_y)
        return jax.tree.map(lambda total, term: total + term.astype(jnp.float32), so_far, by_weights), by_h

    none_yet = {name: jnp.zeros(w.shape, jnp.float32) for name, w in weights.items()}
    by_weights, by_x = lax.scan(take, none_yet, (x, dy))
    gradients = [by_weights[name].astype(jnp.bfloat16).astype(jnp.float32) for name in NAMES]
    gradients = clipped(gradients, sum(jnp.sum(g * g) for g in gradients), sum(g.size for g in gradients))
    first = (m_wq, m_wk, m_wv, m_wo, m_w_gate, m_w_up, m_w_down)
    second = (v_wq, v_wk, v_wv, v_wo, v_w_gate, v_w_up, v_w_down)
    new = [adamw(weights[name].astype(jnp.float32), m, v, g) for name, m, v, g in zip(NAMES, first, second, gradients, strict=True)]
    return tuple(one[which] for which in range(3) for one in new)
```

```python
import jax
import jax.numpy as jnp
import numpy as np
from jax import lax
from jax.experimental import pallas as pl
from jax.experimental.pallas import tpu as pltpu
from jax.sharding import PartitionSpec as P

HIDDEN = -2e30
LOG2E = 1.4426950408889634
HEAD = 128
THETA = 10000
ZERO, ONE, TWO = range(3)
NAMES = ("wq", "wk", "wv", "wo", "w_gate", "w_up", "w_down")
T, D, HEADS, KV, GROUP = 1024, 768, 6, TWO, 3
STEP = 256
SCALE = HEAD**-0.5
E = SCALE * LOG2E
HALF = HEAD // TWO
bf16, f32 = jnp.bfloat16, jnp.float32


def dot(a, b, ca=ONE, cb=ZERO):
    return lax.dot_general(a, b, (((ca,), (cb,)), ((), ())), preferred_element_type=f32)


def rotary():
    angle = np.arange(T, dtype=np.float32)[:, None] * np.float32(THETA) ** (-np.arange(HALF, dtype=np.float32) / np.float32(HALF))
    return np.concatenate([np.cos(angle), np.sin(angle)], axis=ONE).astype(np.float32)


def cos_sin(table):
    swapped = pltpu.roll(table, HALF, ONE)
    first = lax.broadcasted_iota(jnp.int32, table.shape, ONE) < HALF
    return jnp.where(first, table, swapped), jnp.where(first, -swapped, table)


def norm_scale(wide):
    return lax.rsqrt(jnp.mean(wide * wide, axis=ONE, keepdims=True) + 1e-6)


def causal(n):
    key = lax.broadcasted_iota(jnp.int32, (n, STEP), ZERO)
    return lax.broadcasted_iota(jnp.int32, (n, STEP), ONE) + (n - STEP) >= key


def _front(x_ref, wq_ref, wk_ref, wv_ref, wo_ref, table_ref, at_ref, q_ref, k_ref, v_ref, kt_ref, ot_ref, lse_ref, h_ref, b_ref, bt_ref, vt_s, o_s):
    for i in range(T // STEP):
        r = slice(i * STEP, (i + ONE) * STEP)
        wide = x_ref[r, :].astype(f32)
        a = (wide * norm_scale(wide)).astype(bf16)
        at_ref[:, r] = a.T
        cos, sin = cos_sin(table_ref[r, :])

        def turned(t):
            t = t.astype(bf16).astype(f32)
            return (t * cos + pltpu.roll(t, HALF, ONE) * sin).astype(bf16)

        q = dot(a, wq_ref[...])
        for h in range(HEADS):
            q_ref[h, r, :] = turned(q[:, h * HEAD : (h + ONE) * HEAD])
        k, v = dot(a, wk_ref[...]), dot(a, wv_ref[...]).astype(bf16)
        for g in range(KV):
            one = turned(k[:, g * HEAD : (g + ONE) * HEAD])
            k_ref[g, r, :] = one
            kt_ref[g, :, r] = one.T
            v_ref[g, r, :] = v[:, g * HEAD : (g + ONE) * HEAD]
            vt_s[g, :HEAD, r] = v[:, g * HEAD : (g + ONE) * HEAD].T
    for g in range(KV):
        vt_s[g, HEAD:, :] = jnp.ones((16, T), bf16)

    for i in range(T // STEP):
        n = (i + ONE) * STEP
        r = slice(i * STEP, n)
        ok = causal(STEP)

        def head(h, _):
            g = h // GROUP
            s = dot(k_ref[g, :n, :], q_ref[h, r, :], ONE, ONE)
            own = jnp.where(ok, s[n - STEP :, :], HIDDEN)
            top = jnp.max(own, axis=ZERO, keepdims=True)
            parts = [own]
            if i:
                top = jnp.maximum(top, jnp.max(s[: n - STEP, :], axis=ZERO, keepdims=True))
                parts = [s[: n - STEP, :], own]
            out = jnp.zeros((HEAD + 16, STEP), f32)
            at = ZERO
            p = jnp.concatenate([jnp.exp2((part - top) * E).astype(bf16) for part in parts], axis=ZERO)
            out = dot(vt_s[g, :, :n], p)
            total = out[HEAD : HEAD + ONE, :]
            o = (out[:HEAD, :] * (ONE / total)).astype(bf16)
            rows = pl.ds(pl.multiple_of(h * HEAD, HEAD), HEAD)
            ot_ref[rows, r] = o
            o_s[r, rows] = o.T
            lse_ref[h, :, r] = top * E + jnp.log2(total)

        lax.fori_loop(ZERO, HEADS, head, None)

    for i in range(T // STEP):
        r = slice(i * STEP, (i + ONE) * STEP)
        out = dot(o_s[r, :], wo_ref[...]).astype(bf16)
        h = (x_ref[r, :].astype(f32) + out.astype(f32)).astype(bf16)
        h_ref[r, :] = h
        wide = h.astype(f32)
        b = (wide * norm_scale(wide)).astype(bf16)
        b_ref[r, :] = b
        bt_ref[:, r] = b.T


def front(x, wq, wk, wv, wo):
    vmem = pl.BlockSpec(memory_space=pltpu.VMEM)
    out = lambda *s, t=bf16: pltpu.VMEM(s, t)
    return pl.pallas_call(
        _front,
        in_specs=[vmem] * 6,
        out_specs=[vmem] * 10,
        out_shape=[out(D, T), out(HEADS, T, HEAD), out(KV, T, HEAD), out(KV, T, HEAD), out(KV, HEAD, T), out(D, T), out(HEADS, ONE, T, t=f32), out(T, D), out(T, D), out(D, T)],
        scratch_shapes=[pltpu.VMEM((KV, HEAD + 16, T), bf16), pltpu.VMEM((T, D), bf16)],
        compiler_params=pltpu.CompilerParams(vmem_limit_bytes=36 * TWO**20),
        name="front",
    )(x, wq, wk, wv, wo, jnp.asarray(rotary()))

NX, NY, NZ = 4, 4, 8
PLANE = NX * NY
COLUMN = TWO * NZ
ROWS = 3 * COLUMN
LANES = 128
FF = 2304
TILES = FF // STEP
COUNT = 6881280
_run = lambda name, tiles: [(name, t, ONE) for t in range(tiles)]
ORDER = [*_run("w_gate", 9), ("w_down", ZERO, 3), ("w_down", TWO, 3), *_run("wq", 3), *_run("w_up", 9), ("w_down", ONE, 3), *_run("wo", 3), *_run("wk", ONE), *_run("wv", ONE)]
STARTS = [sum(n for _, _, n in ORDER[:i]) for i in range(len(ORDER))]
UNITS = sum(n for _, _, n in ORDER)
START = {(name, t): u for (name, t, _), u in zip(ORDER, STARTS)}
SPLIT = START["w_up", ZERO]
COLOURS = ((ZERO, SPLIT), (SPLIT, UNITS - SPLIT))
INDEX = {name: i for i, name in enumerate(NAMES)}
MESH = pl.DeviceIdType.MESH
THREE = [u for (_, _, n), u in zip(ORDER, STARTS) if n == ONE]
SLOT = {u: s for s, u in enumerate(THREE)}
SLOTS = len(THREE) + 4 * 3
ROW_SLOTS = len(THREE) + TWO * 3


class Flow:
    def __init__(self, number, name, t, n, late, base, slot):
        self.number, self.u, self.n, self.late, self.base, self.slot = number, START[name, t], n, late, base, slot
        self.colour = int(self.u >= SPLIT)


_flow = [("w_gate", ZERO), ("w_gate", 3), ("w_gate", 6), ("w_up", ZERO), ("w_up", 3), ("w_up", 6), ("w_down", ZERO), ("w_down", ONE), ("w_down", TWO), ("wo", ZERO)]
FLOWS = [Flow(i, name, t, 3, ZERO, START[name, t] - 3 * (START[name, t] >= SPLIT), s) for i, ((name, t), s) in enumerate(zip(_flow, (ZERO, ZERO, ZERO, 3, 3, 3, 6, 9, ZERO, 3)))]
FLOWS += [Flow(len(FLOWS), "wq", ZERO, 3, ONE, ZERO, 6), Flow(len(FLOWS) + ONE, "wk", ZERO, TWO, ONE, 3, 9)]
GATES, UPS, (DOWN0, DOWN1, DOWN2, WO, WQ, WKV) = FLOWS[:3], FLOWS[3:6], FLOWS[6:]
PIECE = (4, ONE)
FILLED = (30, 5)
KEYS = 512
GIVE = 12


def _mark(name):
    pass


def _back(*refs):
    it = iter(refs)
    take = lambda n: [next(it) for _ in range(n)]
    at_ref, q_ref, k_ref, v_ref, kt_ref, ot_ref, lse_ref, h_ref, b_ref, bt_ref, dy_ref, wo_ref, table_ref = take(13)
    wg_hbm, wu_hbm, wd_hbm = take(3)
    weights, m_in, v_in = take(7), take(7), take(7)
    out_w, out_g = take(TWO)
    wg_s, wu_s, wd_s, dg_s, du_s, act_s, db_s, dh_s, do_s, delta_s, dk_s, dv_s, dkv_s = take(13)
    give, relay, fin, relay2, fin2, col0, col1, zr0, zr1, gc0, gc1, old, packed, moments, m_nat, v_nat, m_down, v_down, norms, rows_out = take(20)
    s_w, s_old, s_d2d, r_d2d, s_rs, r_rs, s_zr, r_zr, s_za, r_za, s_norm, r_norm, s_mv, r_mv, s_ag, r_ag, s_agl, r_agl, s_core, r_core, s_rows, r_rows = take(22)

    me = lax.axis_index("dp")
    core, j, here, y, x = lax.rem(me, TWO), lax.rem(me, COLUMN), lax.div(me, COLUMN), lax.rem(lax.div(me, COLUMN), NY), lax.div(me, COLUMN * NY)
    z, other = lax.div(j, TWO), ONE - core
    turns = [[p, *(lax.rem(p + d, NX) for d in range(ONE, NX))] for p in (x, y)]
    above = [z, *(lax.rem(z + k, NZ) for k in range(ONE, NZ))]
    column_start = here * COLUMN
    plane = {(a, b): (turns[ZERO][a] * NY + turns[ONE][b]) * COLUMN + z * TWO for a in range(NX) for b in range(NY)}
    along = [[plane[d, ZERO] + core for d in (ONE, 3)], [plane[ZERO, d] + core for d in (ONE, 3)]]
    upward = [column_start + k * TWO + core for k in above]
    partner = column_start + z * TWO + other

    def copy(src, dst, s, r, to):
        return pltpu.make_async_remote_copy(src_ref=src, dst_ref=dst, send_sem=s, recv_sem=r, device_id={"dp": to}, device_id_type=MESH)

    def lanes(half, t, width):
        return pl.ds(pl.multiple_of(half * (width // TWO) + t * LANES, LANES), LANES)

    wide = lambda v: v.astype(f32)
    low = lambda v: v.astype(bf16)

    _mark("start")

    def stream(i, slot, wg_s, wu_s, wd_s):
        out = []
        for k, half in enumerate((core, other)):
            span, to = lanes(half, i, FF), pl.ds(k * LANES, LANES)
            out += [
                pltpu.make_async_copy(wg_hbm.at[:, span], wg_s.at[slot, :, to], s_w.at[slot, ZERO, k]),
                pltpu.make_async_copy(wu_hbm.at[:, span], wu_s.at[slot, :, to], s_w.at[slot, ONE, k]),
                pltpu.make_async_copy(wd_hbm.at[span, :], wd_s.at[slot, to, :], s_w.at[slot, TWO, k]),
            ]
        return out

    fetched = []
    for i, (name, t, n) in enumerate(ORDER):
        w = weights[INDEX[name]]
        fetched.append(pltpu.make_async_copy(w.at[x, y, :, :, lanes(core, t, w.shape[-ONE])], old.at[pl.ds(STARTS[i], n)], s_old.at[i]))
        fetched[-ONE].start()

    barrier = pltpu.get_barrier_semaphore()
    peers = [column_start + k * TWO + c for k in above[ONE:] for c in (ZERO, ONE)]
    peers += [first + c for ab, first in plane.items() if any(ab) for c in (ZERO, ONE)]
    peers += [partner]
    for to in peers:
        pl.semaphore_signal(barrier, inc=ONE, device_id={"dp": to}, device_id_type=MESH)

    packed[...] = jnp.zeros_like(packed)
    for half in (ZERO, ONE):
        for (name, t, n), u in zip(ORDER, STARTS):
            m, v = m_in[INDEX[name]], v_in[INDEX[name]]
            a = half * (m.shape[-ONE] // TWO) + t * LANES
            if n == ONE:
                packed[half, SLOT[u], ZERO:3, :] = m[:, ZERO, a : a + LANES]
                packed[half, SLOT[u], 3:6, :] = v[:, ZERO, a : a + LANES]
            else:
                for k, ref in enumerate((m, v)):
                    s = len(THREE) + 4 * t + TWO * k
                    packed[half, s] = ref[ZERO:8, ZERO, a : a + LANES]
                    packed[half, s + ONE, ZERO:ONE, :] = ref[8:9, ZERO, a : a + LANES]
    moments[j] = packed[core]
    for u in range(FILLED[ZERO], PIECE[ZERO] * NZ):
        col0[u] = jnp.zeros((ROWS, LANES), bf16)
    for u in range(FILLED[ONE], PIECE[ONE] * NZ):
        col1[u] = jnp.zeros((ROWS, LANES), bf16)
    _mark("barrier")
    pl.semaphore_wait(barrier, len(peers))

    mv = []
    for r in range(ONE, COLUMN):
        to = lax.rem(j + r, COLUMN)
        mv.append(copy(packed.at[lax.rem(to, TWO)], moments.at[j], s_mv.at[r - ONE], r_mv.at[r - ONE], column_start + to))
        mv[-ONE].start()

    def d2d(u, n, slot):
        return copy(give.at[:, :, pl.ds(slot, n)], out_w.at[core, :, :, pl.ds(u, n)], s_d2d.at[u], r_d2d.at[u], partner)

    def arrivals(flow):
        by_unit = flow in GATES or flow in UPS
        return [d2d(flow.u + i, ONE, i) for i in range(flow.n)] if by_unit else [d2d(flow.u, flow.n, ZERO)]

    def block(flow, k, a):
        units = pl.ds(flow.u, flow.n)
        return out_w.at[core, k, a, units] if flow.colour == ZERO else out_w.at[core, a, k, units]

    FIRST, LAST = pl.ds(ZERO, TWO), pl.ds(TWO, TWO)

    def hop(flow, i):
        axis, back = (flow.colour, ONE - flow.colour)[i // 6], i % TWO
        k = turns[axis][((TWO, TWO), (ONE, 3), (ONE, 3))[i % 6 // TWO][back]]
        s, r, to = s_rs.at[flow.number, i], r_rs.at[flow.number, i], along[axis][back]
        u, n = flow.u, flow.n
        if i < 6:
            part = (FIRST, LAST, LAST, FIRST, FIRST, LAST)[i]
            dst = relay.at[back, :, pl.ds(u, n)] if i < TWO else fin.at[back, part, pl.ds(u, n)]
            return copy(block(flow, k, part), dst, s, r, to)
        half = n // TWO
        lo, hi = pl.ds(u, half), pl.ds(u + half, n - half)
        part = (lo, hi, hi, lo, lo, hi)[i - 6]
        return copy(fin.at[ZERO, k, part], (relay2 if i < 8 else fin2).at[back, part], s, r, to)

    cols, zrs, gcs = (col0, col1), (zr0, zr1), (gc0, gc1)

    def stage(flow, k):
        u, n = flow.u, flow.n
        units = slice(u, u + n)
        first, second = turns[flow.colour], turns[ONE - flow.colour]
        if k == ZERO:
            for c in arrivals(flow):
                c.wait_recv()

            def add(i, _):
                a, b = lax.div(i, NY), lax.rem(i, NY)
                out_w[core, a, b, units] = low(wide(out_w[core, a, b, units]) + wide(out_w[other, a, b, units]))

            lax.fori_loop(ZERO, PLANE, add, None)
            for i in range(4):
                hop(flow, i).start()
        elif k == ONE:
            for d in (ZERO, ONE):
                hop(flow, d).wait_recv()
                for a in range(TWO):
                    dst = block(flow, first[ONE + TWO * d], TWO * d + a)
                    dst[...] = low(wide(dst[...]) + wide(relay[d, a, units]))
                hop(flow, 4 + d).start()
        elif k == TWO:
            for i in range(TWO, 6):
                hop(flow, i).wait_recv()

            def total(a, _):
                fin[ZERO, a, units] = low(wide(block(flow, first[ZERO], a)[...]) + wide(fin[ZERO, a, units]) + wide(fin[ONE, a, units]))

            lax.fori_loop(ZERO, 4, total, None)
            for i in range(4):
                hop(flow, 6 + i).start()
        elif k == 3:
            half = n // TWO
            for d, part in enumerate((slice(u, u + half), slice(u + half, u + n))):
                hop(flow, 6 + d).wait_recv()
                a = second[ONE + TWO * d]
                fin[ZERO, a, part] = low(wide(fin[ZERO, a, part]) + wide(relay2[d, part]))
                hop(flow, 10 + d).start()
        else:
            for i in range(8, 12):
                hop(flow, i).wait_recv()
            cols[flow.late][flow.base : flow.base + n] = low(wide(fin[ZERO, second[ZERO], units]) + wide(fin2[ZERO, units]) + wide(fin2[ONE, units]))

    def scatter(late, k):
        n = PIECE[late]
        return copy(cols[late].at[pl.ds(above[k] * n, n)], zrs[late].at[k - ONE], s_zr.at[late, k - ONE], r_zr.at[late, k - ONE], upward[k])

    def gather(late, k):
        own = pl.ds(z * PIECE[late], PIECE[late])
        return copy(gcs[late].at[own], gcs[late].at[own], s_za.at[late, k - ONE], r_za.at[late, k - ONE], upward[k])

    OTHERS = range(ONE, NZ)

    def column(late, step):
        if step == ZERO:
            for k in OTHERS:
                scatter(late, k).start()
        elif step == ONE:
            for k in OTHERS:
                scatter(late, k).wait_recv()
            n = PIECE[late]
            for i in range(n):
                total = wide(cols[late][z * n + i])
                for k in range(NZ - ONE):
                    total += wide(zrs[late][k, i])
                gcs[late][z * n + i] = low(total)
            for k in OTHERS:
                gather(late, k).start()
        else:
            for k in OTHERS:
                gather(late, k).wait_recv()

    def spread_moments():
        for c in mv:
            c.wait_recv()
        for name, n in (("w_gate", 9), ("wq", 3), ("w_up", 9), ("wo", 5)):
            u = START[name, ZERO]

            def move(i, _):
                for d in range(COLUMN):
                    m_nat[u + i, 3 * d : 3 * d + 3, :] = moments[d, SLOT[u] + i, ZERO:3, :]
                    v_nat[u + i, 3 * d : 3 * d + 3, :] = moments[d, SLOT[u] + i, 3:6, :]

            lax.fori_loop(ZERO, n, move, None)

        def move_down(t, _):
            for d in range(COLUMN):
                for k, nat in enumerate((m_down, v_down)):
                    s = len(THREE) + 4 * t + TWO * k
                    nat[t, 9 * d : 9 * d + 8, :] = moments[d, s]
                    nat[t, 9 * d + 8 : 9 * d + 9, :] = moments[d, s + ONE, ZERO:ONE, :]

        lax.fori_loop(ZERO, 3, move_down, None)

    def keep(r, u, slot):
        for k in range(PLANE):
            rows = slice(k * ROWS, (k + ONE) * ROWS)
            out_w[core, k // NY, k % NY, u] = low(r[rows, :LANES])
            give[k // NY, k % NY, slot] = low(r[rows, LANES:])

    def pair(ref, t):
        n = ref.shape[ONE]
        return jnp.concatenate([ref[:, lanes(core, t, n)], ref[:, lanes(other, t, n)]], axis=ONE)

    during = {}

    def when(i, *stages):
        during[i] = stages

    when(3, (GATES[ZERO], ZERO), (UPS[ZERO], ZERO))
    when(4, (GATES[ZERO], ONE), (UPS[ZERO], ONE))
    when(5, (GATES[ZERO], TWO), (UPS[ZERO], TWO))
    when(6, (GATES[ZERO], 3), (UPS[ZERO], 3), (GATES[ONE], ZERO), (UPS[ONE], ZERO))
    when(7, (GATES[ZERO], 4), (UPS[ZERO], 4), (GATES[ONE], ONE), (UPS[ONE], ONE))
    when(8, (GATES[ONE], TWO), (UPS[ONE], TWO))

    for c in stream(ZERO, ZERO, wg_s, wu_s, wd_s):
        c.start()
    db_s[...] = jnp.zeros_like(db_s)
    _mark("mlp")

    def step(i, _):
        slot = lax.rem(i, TWO)
        for c in stream(i, slot, wg_s, wu_s, wd_s):
            c.wait()

        @pl.when(i + ONE < TILES)
        def _():
            for c in stream(i + ONE, ONE - slot, wg_s, wu_s, wd_s):
                c.start()

        turn = lax.rem(i, 3)

        @pl.when(i >= 3)
        def _():
            d2d(START["w_gate", ZERO] + i - 3, ONE, turn).wait_send()
            d2d(START["w_up", ZERO] + i - 3, ONE, 3 + turn).wait_send()

        wg, wu, wd = wg_s[slot], wu_s[slot], wd_s[slot]
        own_rows, other_rows = lanes(core, i, FF), lanes(other, i, FF)
        for c in range(TWO):
            r = slice(c * (T // TWO), (c + ONE) * (T // TWO))
            g, u = dot(b_ref[r, :], wg), dot(b_ref[r, :], wu)
            da = wide(low(dot(dy_ref[r, :], wd, ONE, ONE)))
            s = ONE / (ONE + jnp.exp(-g))
            silu = g * s
            act = low(silu * u).T
            act_s[own_rows, r] = act[:LANES]
            act_s[other_rows, r] = act[LANES:]
            du_s[r, :] = low(da * silu)
            dg_s[r, :] = low(da * u * (s + silu * (ONE - s)))
        for k, stages in during.items():

            @pl.when(i == k)
            def _(stages=stages):
                for flow, n in stages:
                    stage(flow, n)

        keep(dot(bt_ref[...], dg_s[...]), START["w_gate", ZERO] + i, turn)
        d2d(START["w_gate", ZERO] + i, ONE, turn).start()
        keep(dot(bt_ref[...], du_s[...]), START["w_up", ZERO] + i, 3 + turn)
        d2d(START["w_up", ZERO] + i, ONE, 3 + turn).start()
        db_s[...] += dot(dg_s[...], wg, ONE, ONE) + dot(du_s[...], wu, ONE, ONE)

    lax.fori_loop(ZERO, TILES, step, None)

    def down(flow, t, reused):
        for c in reused:
            c.wait_send()
        dy = pair(dy_ref, t)
        for a in range(NX):
            n = FF // NX
            r = dot(act_s[a * n : (a + ONE) * n, :], dy)
            for k in range(NY):
                for i in range(3):
                    rows = slice((3 * k + i) * ROWS, (3 * k + i + ONE) * ROWS)
                    out_w[core, a, k, flow.u + i] = low(r[rows, :LANES])
                    give[a, k, flow.slot + i] = low(r[rows, LANES:])
        d2d(flow.u, 3, flow.slot).start()

    _mark("down0")
    down(DOWN0, ZERO, [])
    stage(GATES[ONE], 3)
    stage(UPS[ONE], 3)
    stage(GATES[TWO], ZERO)
    stage(UPS[TWO], ZERO)
    _mark("down1")
    down(DOWN1, ONE, [])
    stage(GATES[ONE], 4)
    stage(UPS[ONE], 4)
    _mark("down2")
    down(DOWN2, TWO, [d2d(GATES[TWO].u + i, ONE, i) for i in range(3)])
    stage(GATES[TWO], ONE)
    stage(UPS[TWO], ONE)
    stage(DOWN0, ZERO)

    _mark("norm")
    for i in range(T // STEP):
        r = slice(i * STEP, (i + ONE) * STEP)
        w, db = wide(h_ref[r, :]), db_s[r, :]
        s = norm_scale(w)
        dh = low(wide(dy_ref[r, :]) + s * (db - w * (s * s * jnp.mean(db * w, axis=ONE, keepdims=True))))
        dh_s[r, :] = dh
        do = low(dot(dh, wo_ref[...], ONE, ONE))
        do_s[r, :] = do
        for h in range(HEADS):
            rows = slice(h * HEAD, (h + ONE) * HEAD)
            delta_s[h, :, r] = jnp.sum(wide(do[:, rows].T) * wide(ot_ref[rows, r]), axis=ZERO, keepdims=True)
        if i == ONE:
            stage(DOWN1, ZERO)
    stage(GATES[TWO], TWO)
    stage(UPS[TWO], TWO)

    _mark("wo")
    for i in range(3):
        d2d(UPS[TWO].u + i, ONE, 3 + i).wait_send()
    lax.fori_loop(ZERO, 3, lambda i, _: keep(dot(ot_ref[...], pair(dh_s, i)), WO.u + i, WO.slot + i), None)
    d2d(WO.u, 3, WO.slot).start()
    stage(DOWN0, ONE)
    stage(DOWN2, ZERO)
    stage(DOWN1, ONE)

    _mark("att")
    later = {
        (ZERO, ZERO): [(GATES[TWO], 3), (UPS[TWO], 3), (WO, ZERO)],
        (ZERO, ONE): [(DOWN0, TWO)],
        (ZERO, TWO): [(DOWN2, ONE), (DOWN1, TWO), (GATES[TWO], 4), (UPS[TWO], 4)],
        (ZERO, 3): [(WO, ONE), (DOWN0, 3), (DOWN1, 3)],
        (ONE, ZERO): [(DOWN2, TWO)],
        (ONE, ONE): [(WO, TWO), (DOWN0, 4), (DOWN1, 4)],
        (ONE, TWO): [(DOWN2, 3), (WO, 3)],
        (ONE, 3): [(DOWN2, 4), (WO, 4)],
    }

    dq_s, p_s, ds_s = dh_s, act_s.at[:T, :D], act_s.at[T : TWO * T, :D]

    def group(g, _):
        for i in range(T // STEP):
            n = (i + ONE) * STEP
            r = slice(i * STEP, n)
            ok = causal(STEP)
            qs, dos = [], []
            for k in range(GROUP):
                h = g * GROUP + k
                q, do = q_ref[h, r, :], do_s[r, pl.ds(pl.multiple_of(h * HEAD, HEAD), HEAD)]
                qs.append(q)
                dos.append(do)
                to = slice(k * STEP, (k + ONE) * STEP)
                for a in range(ZERO, n, KEYS):
                    keys = slice(a, min(a + KEYS, n))
                    p = jnp.exp2(dot(k_ref[g, keys, :], q, ONE, ONE) * E - lse_ref[h, :, r])
                    if a + KEYS >= n:
                        own = jnp.where(ok, p[n - STEP - a :, :], 0.0)
                        p = own if n - STEP == a else jnp.concatenate([p[: n - STEP - a, :], own], axis=ZERO)
                    p_s[keys, to] = low(p)
                    ds_s[keys, to] = low(p * (dot(v_ref[g, keys, :], do, ONE, ONE) - delta_s[h, :, r]))
            dv = dot(p_s[:n, :], jnp.concatenate(dos, axis=ZERO))
            dk = dot(ds_s[:n, :], jnp.concatenate(qs, axis=ZERO))
            dq = dot(kt_ref[g, :, :n], ds_s[:n, :])
            cos, sin = cos_sin(table_ref[r, :])
            for k in range(GROUP):
                t = dq[:, k * STEP : (k + ONE) * STEP].T * SCALE
                dq_s[r, pl.ds(pl.multiple_of((g * GROUP + k) * HEAD, HEAD), HEAD)] = low(t * cos - pltpu.roll(t, HALF, ONE) * sin)
            if i == ZERO:
                dv_s[:n], dk_s[:n] = dv, dk
            else:
                dv_s[: n - STEP] += dv[: n - STEP]
                dk_s[: n - STEP] += dk[: n - STEP]
                dv_s[r], dk_s[r] = dv[n - STEP :], dk[n - STEP :]
            for which in (ZERO, ONE):
                if later[which, i]:

                    @pl.when(g == which)
                    def _():
                        for flow, m in later[which, i]:
                            stage(flow, m)

        span = pl.ds(pl.multiple_of(g * HEAD, HEAD), HEAD)
        for i in range(T // STEP):
            r = slice(i * STEP, (i + ONE) * STEP)
            cos, sin = cos_sin(table_ref[r, :])
            t = dk_s[r, :] * SCALE
            dkv_s[ZERO, r, span] = low(t * cos - pltpu.roll(t, HALF, ONE) * sin)
            dkv_s[ONE, r, span] = low(dv_s[r, :])

    lax.fori_loop(ZERO, KV, group, None)

    _mark("qkv")
    d2d(DOWN0.u, 3, DOWN0.slot).wait_send()
    d2d(DOWN1.u, 3, DOWN1.slot).wait_send()
    lax.fori_loop(ZERO, 3, lambda i, _: keep(dot(at_ref[...], pair(dq_s, i)), WQ.u + i, WQ.slot + i), None)
    d2d(WQ.u, 3, WQ.slot).start()
    lax.fori_loop(ZERO, TWO, lambda i, _: keep(dot(at_ref[...], pair(dkv_s.at[i], ZERO)), WKV.u + i, WKV.slot + i), None)
    d2d(WKV.u, TWO, WKV.slot).start()

    _mark("tail")
    column(ZERO, ZERO)
    stage(WQ, ZERO)
    stage(WKV, ZERO)
    spread_moments()
    stage(WKV, ONE)
    stage(WQ, ONE)
    _mark("tail_z0")
    column(ZERO, ONE)
    _mark("tail_2")
    stage(WKV, TWO)
    stage(WQ, TWO)
    _mark("tail_3")
    stage(WKV, 3)
    stage(WQ, 3)
    _mark("tail_4")
    stage(WKV, 4)
    stage(WQ, 4)
    column(ONE, ZERO)
    _mark("tail_z1")
    column(ZERO, TWO)
    _mark("tail_z2")
    column(ONE, ONE)
    _mark("tail_z3")
    column(ONE, TWO)

    for c in (DOWN2, WO, WQ, WKV):
        d2d(c.u, c.n, c.slot).wait_send()
    for flow in FLOWS:
        for i in range(12):
            hop(flow, i).wait_send()
    for late in (ZERO, ONE):
        for k in OTHERS:
            scatter(late, k).wait_send()
            gather(late, k).wait_send()
    for c in mv:
        c.wait_send()

    _mark("norms")
    squares = jnp.zeros((8, LANES), f32)
    for late in (ZERO, ONE):

        def more(i, total):
            g = wide(gcs[late][i])
            return total + (g * g).reshape(ROWS // 8, 8, LANES).sum(ZERO)

        squares = lax.fori_loop(ZERO, FILLED[late], more, squares)
    norms[here, core] = squares
    shared = []
    for ab, first in plane.items():
        for c in (core, other):
            if any(ab) or c is other:
                i = len(shared)
                shared.append(copy(norms.at[here, core], norms.at[here, core], s_norm.at[i], r_norm.at[i], first + c))
                shared[-ONE].start()
    for c in fetched:
        c.wait()
    for c in shared:
        c.wait_recv()
    total = norms[...].sum(axis=(ZERO, ONE))
    total = jnp.sum(jnp.sum(total, axis=ZERO, keepdims=True), axis=ONE, keepdims=True)
    factor = jnp.minimum(1.0, 0.5 * lax.rsqrt(total * (1.0 / COUNT) + 1e-30))

    _mark("adam")

    def stepped(w, m, v, g):
        g = g * factor
        m = 0.9 * m + 0.1 * g
        v = 0.95 * v + 0.05 * g * g
        return low(w - 0.02 * (m * lax.rsqrt(v + 1e-8) + 0.1 * w))

    for name, t, n in (("w_gate", ZERO, 9), ("w_up", ZERO, 9), ("w_down", ZERO, 3), ("w_down", ONE, 3), ("w_down", TWO, 3), ("wq", ZERO, 3), ("wo", ZERO, 3), ("wk", ZERO, TWO)):
        u = START[name, t]
        late = name in ("wq", "wk")
        first = (3 if u >= SPLIT else ZERO) if late else u - 3 * (u >= SPLIT)

        def unit(i, _):
            if name == "w_down":
                rows = pl.ds(pl.multiple_of(i * ROWS, ROWS), ROWS)
                m, v = m_down[t, rows, :], v_down[t, rows, :]
            else:
                m, v = m_nat[u + i], v_nat[u + i]
            out_w[core, x, y, u + i] = stepped(wide(old[u + i]), m, v, wide(gcs[late][first + i]))

        lax.fori_loop(ZERO, n, unit, None)

    _mark("ag0")
    sent = []

    def slot(colour, ps, pb, h=None):
        u, n = COLOURS[colour]
        if h is not None:
            u, n = (u, n // TWO) if h == ZERO else (u + n // TWO, n - n // TWO)
        units = pl.ds(u, n)
        return out_w.at[core, pb, ps, units] if colour == ZERO else out_w.at[core, ps, pb, units]

    core_copies = []

    def to_partner(colour, ps, pb):
        v, i = slot(colour, ps, pb), len(core_copies)
        core_copies.append(copy(v, v, s_core.at[i], r_core.at[i], partner))
        core_copies[-ONE].start()

    ring = {}

    def send(colour, big, rel, ps, pb, h, d, kind):
        v = slot(colour, ps, pb, h)
        s, r = (s_agl.at[colour, rel, d, kind], r_agl.at[colour, rel, d, kind]) if big else (s_ag.at[colour, d, kind], r_ag.at[colour, d, kind])
        c = copy(v, v, s, r, along[colour if big else ONE - colour][d])
        c.start()
        ring[colour, big, rel, d, kind] = c

    def spot(colour):
        return turns[ONE - colour], turns[colour]

    def big_own(colour, rel):
        ps, pb = spot(colour)
        for d in (ZERO, ONE):
            send(colour, ONE, rel, ps[rel], pb[ZERO], None, d, ZERO)

    def big_forward(colour, rel):
        ps, pb = spot(colour)
        for d in (ZERO, ONE):
            ring[colour, ONE, rel, d, ZERO].wait_recv()
            send(colour, ONE, rel, ps[rel], pb[3 - TWO * d], d, d, ONE)
        for d in (ZERO, ONE):
            to_partner(colour, ps[rel], pb[3 - TWO * d])

    def big_far(colour, rel):
        ps, pb = spot(colour)
        for d in (ZERO, ONE):
            ring[colour, ONE, rel, d, ONE].wait_recv()
        to_partner(colour, ps[rel], pb[TWO])

    for colour in (ZERO, ONE):
        ps, pb = spot(colour)
        for d in (ZERO, ONE):
            send(colour, ZERO, ZERO, ps[ZERO], pb[ZERO], None, d, ZERO)
    for colour in (ZERO, ONE):
        big_own(colour, ZERO)
        ps, pb = spot(colour)
        to_partner(colour, ps[ZERO], pb[ZERO])
    for colour in (ZERO, ONE):
        ps, pb = spot(colour)
        for d in (ZERO, ONE):
            ring[colour, ZERO, ZERO, d, ZERO].wait_recv()
            send(colour, ZERO, ZERO, ps[3 - TWO * d], pb[ZERO], d, d, ONE)
        for rel in (3, ONE):
            big_own(colour, rel)
            to_partner(colour, ps[rel], pb[ZERO])

    _mark("rows")

    def picker(height, each, of):
        row, col = lax.broadcasted_iota(jnp.int32, (height, of), ZERO), lax.broadcasted_iota(jnp.int32, (height, of), ONE)
        half = height // TWO
        ours = (row < each) & (col == each * j + row)
        theirs = (row >= half) & (row < half + each) & (col == each * (j + ONE - TWO * core) + row - half)
        return (ours | theirs).astype(f32).astype(bf16)

    three, nine = picker(16, 3, ROWS), picker(32, 9, 3 * ROWS)
    for (name, t, n), u in zip(ORDER, STARTS):
        late = name in ("wq", "wk", "wv")
        a = ((u - START["wk", ZERO] + 3 if u >= SPLIT else u - START["wq", ZERO]) if late else u - 3 * (u >= SPLIT))
        if n == ONE:
            rows = dot(three, gcs[late][a]) * factor
            out_g[core, SLOT[u]], rows_out[SLOT[u]] = rows[:8], rows[8:]
        else:
            rows = dot(nine, gcs[late][a : a + 3].reshape(3 * ROWS, LANES)) * factor
            s = len(THREE) + TWO * t
            for k in (ZERO, ONE):
                out_g[core, s + k], rows_out[s + k] = rows[8 * k : 8 * k + 8], rows[16 + 8 * k : 24 + 8 * k]
    own_rows = copy(rows_out, out_g.at[core], s_rows, r_rows, partner)
    own_rows.start()

    _mark("ag2")
    for colour in (ZERO, ONE):
        ps, pb = spot(colour)
        big_forward(colour, ZERO)
        for d in (ZERO, ONE):
            ring[colour, ZERO, ZERO, d, ONE].wait_recv()
        big_own(colour, TWO)
        to_partner(colour, ps[TWO], pb[ZERO])
    _mark("ag3")
    for colour in (ZERO, ONE):
        big_forward(colour, 3)
        big_forward(colour, ONE)
        big_far(colour, ZERO)
    _mark("ag4")
    for colour in (ZERO, ONE):
        big_forward(colour, TWO)
        big_far(colour, 3)
        big_far(colour, ONE)
    _mark("ag5")
    for colour in (ZERO, ONE):
        big_far(colour, TWO)
    own_rows.wait()
    for c in core_copies:
        c.wait_recv()
    for c in [*core_copies, *shared, *ring.values()]:
        c.wait_send()
    _mark("end")


def exchange(kept, dy, weights, m, v):
    view = lambda t: t.reshape(NX, NY, t.shape[ZERO] // (PLANE * ROWS), ROWS, t.shape[ONE])
    any_ = pl.BlockSpec(memory_space=pl.ANY)
    vmem = pl.BlockSpec(memory_space=pltpu.VMEM)
    low, wide = lambda *s: pltpu.VMEM(s, bf16), lambda *s: pltpu.VMEM(s, f32)
    unit = lambda *lead: low(*lead, ROWS, LANES)
    dma = lambda *shape: pltpu.SemaphoreType.DMA(shape)
    n = len(ORDER)
    scratch = [
        low(TWO, D, STEP), low(TWO, D, STEP), low(TWO, STEP, D), low(T, STEP), low(T, STEP),
        low(FF, T), wide(T, D), low(T, D), low(T, D), wide(HEADS, ONE, T),
        wide(T, HEAD), wide(T, HEAD), low(TWO, T, KV * HEAD),
        unit(NX, NY, GIVE), unit(TWO, TWO, UNITS), unit(TWO, 4, UNITS), unit(TWO, UNITS), unit(TWO, UNITS),
        *(unit(NZ * p) for p in PIECE), *(unit(NZ - ONE, p) for p in PIECE), *(unit(NZ * p) for p in PIECE),
        unit(UNITS), wide(TWO, SLOTS, 8, LANES), wide(COLUMN, SLOTS, 8, LANES),
        wide(UNITS, ROWS, LANES), wide(UNITS, ROWS, LANES), wide(3, 3 * ROWS, LANES), wide(3, 3 * ROWS, LANES),
        wide(PLANE, TWO, 8, LANES), wide(ROW_SLOTS, 8, LANES),
        dma(TWO, 3, TWO), dma(n),
    ]
    for shape in ((UNITS,), (len(FLOWS), 12), (TWO, NZ - ONE), (TWO, NZ - ONE), (TWO * PLANE - ONE,), (COLUMN - ONE,), (TWO, TWO, TWO), (TWO, 4, TWO, TWO), (TWO * PLANE,), ()):
        scratch += [dma(*shape), dma(*shape)]
    return pl.pallas_call(
        _back,
        in_specs=[vmem] * 13 + [any_] * 10 + [vmem] * 14,
        out_specs=[vmem, vmem],
        out_shape=[pltpu.VMEM((TWO, NX, NY, UNITS, ROWS, LANES), bf16), pltpu.VMEM((TWO, ROW_SLOTS, 8, LANES), f32)],
        scratch_shapes=scratch,
        compiler_params=pltpu.CompilerParams(collective_id=ZERO, has_side_effects=True, vmem_limit_bytes=50 * TWO**20),
        name="back",
    )(*kept, dy, weights[INDEX["wo"]], jnp.asarray(rotary()), *(weights[INDEX[name]] for name in ("w_gate", "w_up", "w_down")), *map(view, weights), *m, *v)


def _finish(*refs):
    w_ref, g_ref, m_in, v_in = refs[ZERO], refs[ONE], refs[TWO:9], refs[9:16]
    w_out, m_out, v_out, sem = refs[16:23], refs[23:30], refs[30:37], refs[37]
    copies = []
    for half in (ZERO, ONE):
        for i, (name, t, n) in enumerate(ORDER):
            o = w_out[INDEX[name]]
            a = half * (o.shape[-ONE] // TWO) + t * LANES
            copies.append(pltpu.make_async_copy(w_ref.at[half, :, :, pl.ds(STARTS[i], n)], o.at[:, :, :, :, pl.ds(a, LANES)], sem.at[half, i]))
            copies[-ONE].start()
    for half in (ZERO, ONE):
        for (name, t, n), u in zip(ORDER, STARTS):
            k = INDEX[name]
            a = half * (m_in[k].shape[-ONE] // TWO) + t * LANES
            s = len(THREE) + TWO * t
            for s, r, rows in [(SLOT[u], ZERO, 3)] if n == ONE else [(s, ZERO, 8), (s + ONE, 8, ONE)]:
                g = g_ref[half, s, ZERO:rows, :]
                here = (slice(r, r + rows), ZERO, slice(a, a + LANES))
                m_out[k][here] = 0.9 * m_in[k][here] + 0.1 * g
                v_out[k][here] = 0.95 * v_in[k][here] + 0.05 * g * g
    for c in copies:
        c.wait()


def finish(new, rows, m, v, like):
    any_ = pl.BlockSpec(memory_space=pl.ANY)
    vmem = pl.BlockSpec(memory_space=pltpu.VMEM)
    view = lambda t: (NX, NY, t.shape[ZERO] // (PLANE * ROWS), ROWS, t.shape[ONE])
    out = pl.pallas_call(
        _finish,
        in_specs=[vmem] * 16,
        out_specs=[any_] * 7 + [vmem] * 14,
        out_shape=[jax.ShapeDtypeStruct(view(w), w.dtype) for w in like] + [jax.ShapeDtypeStruct(t.shape, t.dtype) for t in (*m, *v)],
        scratch_shapes=[pltpu.SemaphoreType.DMA((TWO, len(ORDER)))],
        compiler_params=pltpu.CompilerParams(vmem_limit_bytes=16 * TWO**20),
        name="finish",
    )(new, rows, *m, *v)
    return [o.reshape(ONE, *w.shape) for o, w in zip(out[:7], like)], out[7:14], out[14:]


def solution(mesh):
    def step(x, dy, *arrays):
        weights, m, v = (arrays[i : i + 7] for i in (ZERO, 7, 14))
        weights = [w[ZERO] for w in weights]
        m, v = ([t.transpose(ONE, ZERO, TWO) for t in s] for s in (m, v))
        kept = front(x[ZERO], *weights[:4])
        new, rows = exchange(kept, dy[ZERO], weights, m, v)
        w, m, v = finish(new, rows, m, v, weights)
        return (*w, *(t.transpose(ONE, ZERO, TWO) for t in (*m, *v)))

    states, all_of, cut = P(("rep", "dp"), None, None), P(None, None, None), P(None, "dp", None)
    return jax.shard_map(
        step,
        mesh=mesh,
        in_specs=(states, states) + (all_of,) * 7 + (cut,) * 14,
        out_specs=(P("rep", None, None),) * 7 + (P("rep", "dp", None),) * 14,
        check_vma=False,
    )
```

```python
import jax
import jax.numpy as jnp
import numpy as np
from jax import lax
from jax.experimental import pallas as pl
from jax.experimental.pallas import tpu as pltpu
from jax.sharding import PartitionSpec as P

HIDDEN = -2e30
LOG2E = 1.4426950408889634
HEAD = 128
THETA = 10000
ZERO, ONE, TWO = range(3)
NAMES = ("wq", "wk", "wv", "wo", "w_gate", "w_up", "w_down")
T, D, HEADS, KV, GROUP = 1024, 768, 6, TWO, 3
STEP = 256
SCALE = HEAD**-0.5
E = SCALE * LOG2E
HALF = HEAD // TWO
bf16, f32 = jnp.bfloat16, jnp.float32


def dot(a, b, ca=ONE, cb=ZERO):
    return lax.dot_general(a, b, (((ca,), (cb,)), ((), ())), preferred_element_type=f32)


def rotary():
    angle = np.arange(T, dtype=np.float32)[:, None] * np.float32(THETA) ** (-np.arange(HALF, dtype=np.float32) / np.float32(HALF))
    return np.concatenate([np.cos(angle), np.sin(angle)], axis=ONE).astype(np.float32)


def cos_sin(table):
    swapped = pltpu.roll(table, HALF, ONE)
    first = lax.broadcasted_iota(jnp.int32, table.shape, ONE) < HALF
    return jnp.where(first, table, swapped), jnp.where(first, -swapped, table)


def norm_scale(wide):
    return lax.rsqrt(jnp.mean(wide * wide, axis=ONE, keepdims=True) + 1e-6)


def causal(n):
    key = lax.broadcasted_iota(jnp.int32, (n, STEP), ZERO)
    return lax.broadcasted_iota(jnp.int32, (n, STEP), ONE) + (n - STEP) >= key


NX, NY, NZ = 4, 4, 8
PLANE = NX * NY
COLUMN = TWO * NZ
ROWS = 3 * COLUMN
LANES = 128
FF = 2304
TILES = FF // STEP
COUNT = 6881280
_run = lambda name, tiles: [(name, t, ONE) for t in range(tiles)]
ORDER = [*_run("w_gate", 9), ("w_down", ZERO, 3), ("w_down", TWO, 3), *_run("wq", 3), *_run("w_up", 9), ("w_down", ONE, 3), *_run("wo", 3), *_run("wk", ONE), *_run("wv", ONE)]
STARTS = [sum(n for _, _, n in ORDER[:i]) for i in range(len(ORDER))]
UNITS = sum(n for _, _, n in ORDER)
START = {(name, t): u for (name, t, _), u in zip(ORDER, STARTS)}
SPLIT = START["w_up", ZERO]
COLOURS = ((ZERO, SPLIT), (SPLIT, UNITS - SPLIT))
INDEX = {name: i for i, name in enumerate(NAMES)}
MESH = pl.DeviceIdType.MESH
THREE = [u for (_, _, n), u in zip(ORDER, STARTS) if n == ONE]
SLOT = {u: s for s, u in enumerate(THREE)}
SLOTS = len(THREE) + 4 * 3
ROW_SLOTS = len(THREE) + TWO * 3


class Flow:
    def __init__(self, number, name, t, n, late, base, slot):
        self.number, self.u, self.n, self.late, self.base, self.slot = number, START[name, t], n, late, base, slot
        self.colour = int(self.u >= SPLIT)


_flow = [("w_gate", ZERO), ("w_gate", 3), ("w_gate", 6), ("w_up", ZERO), ("w_up", 3), ("w_up", 6), ("w_down", ZERO), ("w_down", ONE), ("w_down", TWO), ("wo", ZERO)]
FLOWS = [Flow(i, name, t, 3, ZERO, START[name, t] - 3 * (START[name, t] >= SPLIT), s) for i, ((name, t), s) in enumerate(zip(_flow, (ZERO, ZERO, ZERO, 3, 3, 3, 6, 9, ZERO, 3)))]
FLOWS += [Flow(len(FLOWS), "wq", ZERO, 3, ONE, ZERO, 6), Flow(len(FLOWS) + ONE, "wk", ZERO, TWO, ONE, 3, 9)]
GATES, UPS, (DOWN0, DOWN1, DOWN2, WO, WQ, WKV) = FLOWS[:3], FLOWS[3:6], FLOWS[6:]
PIECE = (4, ONE)
FILLED = (30, 5)
KEYS = 512
GIVE = 12


def _mark(name):
    pass


def _step(*refs):
    it = iter(refs)
    take = lambda n: [next(it) for _ in range(n)]
    x_hbm, dy_hbm, table_hbm, wq_hbm, wk_hbm, wv_hbm, wo_hbm, wg_hbm, wu_hbm, wd_hbm = take(10)
    weights, m_hbm, v_hbm = take(7), take(7), take(7)
    out_w, out_g = take(TWO)
    table_ref, wo_ref, dy_ref, at_ref, q_ref, k_ref, v_ref, kt_ref, vt_ref, ot_ref, lse_ref, h_ref, b_ref, bt_ref = take(14)
    wg_s, wu_s, wd_s, dg_s, du_s, act_s, db_s, dh_s, do_s, delta_s = take(10)
    give, relay, fin, relay2, fin2, col0, col1, zr0, zr1, gc0, gc1, old, three_in, nine_in, packed, moments, m_nat, v_nat, m_down, v_down, norms, rows_out = take(22)
    s_in, s_w, s_old, s_give, r_give, s_hop, r_relay, r_fin, s_zr, r_zr, s_za, r_za, s_norm, r_norm, s_mv, r_mv, s_ag, r_small, r_big, s_core, r_core, s_rows, r_rows = take(23)
    x_ref, wq_ref, wk_ref, wv_ref, o_s = act_s.at[:T, :D], act_s.at[T : T + D, :D], act_s.at[:D, D:], act_s.at[D : TWO * D, D:], dh_s
    dq_s, p_s, ds_s = dh_s, act_s.at[:T, :D], act_s.at[T : TWO * T, :D]
    dk_s, dv_s, dkv_s = db_s.at[:, :HEAD], db_s.at[:, HEAD : TWO * HEAD], (dg_s, du_s)

    me = lax.axis_index("dp")
    core, j, here, y, x = lax.rem(me, TWO), lax.rem(me, COLUMN), lax.div(me, COLUMN), lax.rem(lax.div(me, COLUMN), NY), lax.div(me, COLUMN * NY)
    z, other = lax.div(j, TWO), ONE - core
    turns = [[p, *(lax.rem(p + d, NX) for d in range(ONE, NX))] for p in (x, y)]
    above = [z, *(lax.rem(z + k, NZ) for k in range(ONE, NZ))]
    column_start = here * COLUMN
    plane = {(a, b): (turns[ZERO][a] * NY + turns[ONE][b]) * COLUMN + z * TWO for a in range(NX) for b in range(NY)}
    along = [[plane[d, ZERO] + core for d in (ONE, 3)], [plane[ZERO, d] + core for d in (ONE, 3)]]
    upward = [column_start + k * TWO + core for k in above]
    partner = column_start + z * TWO + other

    def copy(src, dst, s, r, to):
        return pltpu.make_async_remote_copy(src_ref=src, dst_ref=dst, send_sem=s, recv_sem=r, device_id={"dp": to}, device_id_type=MESH)

    def lanes(half, t, width):
        return pl.ds(pl.multiple_of(half * (width // TWO) + t * LANES, LANES), LANES)

    wide = lambda v: v.astype(f32)
    low = lambda v: v.astype(bf16)

    _mark("start")

    def stream(i, slot):
        out = []
        for k, half in enumerate((core, other)):
            span, to = lanes(half, i, FF), pl.ds(k * LANES, LANES)
            for n, (src, dst) in enumerate(((wg_hbm.at[:, span], wg_s.at[slot, :, to]), (wu_hbm.at[:, span], wu_s.at[slot, :, to]), (wd_hbm.at[span, :], wd_s.at[slot, to, :]))):
                out.append(pltpu.make_async_copy(src, dst, s_w.at[slot, n]))
        return out

    ahead = [pltpu.make_async_copy(x_hbm.at[r, :], x_ref.at[r, :], s_in.at[i]) for i, r in enumerate(pl.ds(k * STEP, STEP) for k in range(T // STEP))]
    for src, dst in ((wq_hbm, wq_ref), (table_hbm, table_ref), (wk_hbm, wk_ref), (wv_hbm, wv_ref), (wo_hbm, wo_ref), (dy_hbm, dy_ref)):
        ahead.append(pltpu.make_async_copy(src, dst, s_in.at[len(ahead)]))
    for c in (ahead[ZERO], *ahead[4:8], *ahead[ONE:4], *ahead[8:]):
        c.start()
    places = {}
    for k, ref in enumerate((m_hbm, v_hbm)):
        lane = ZERO
        for name in NAMES:
            src = ref[INDEX[name]]
            if name == "w_down":
                dst, sem = nine_in.at[k], len(ahead) + ONE
            else:
                dst, sem = three_in.at[k, :, :, pl.ds(lane, src.shape[-ONE])], len(ahead)
                places[name] = lane
                lane += src.shape[-ONE]
            pltpu.make_async_copy(src, dst, s_in.at[sem]).start()
    for c in stream(ZERO, ZERO):
        c.start()
    for (name, t, n), u in zip(ORDER, STARTS):
        w = weights[INDEX[name]]
        pltpu.make_async_copy(w.at[x, y, :, :, lanes(core, t, w.shape[-ONE])], old.at[pl.ds(u, n)], s_old).start()

    barrier = pltpu.get_barrier_semaphore()
    peers = [column_start + k * TWO + c for k in above[ONE:] for c in (ZERO, ONE)]
    peers += [first + c for ab, first in plane.items() if any(ab) for c in (ZERO, ONE)]
    peers += [partner]
    for to in peers:
        pl.semaphore_signal(barrier, inc=ONE, device_id={"dp": to}, device_id_type=MESH)

    _mark("front")
    for i in range(T // STEP):
        r = slice(i * STEP, (i + ONE) * STEP)
        ahead[i].wait()
        if i == ZERO:
            for c in ahead[4:8]:
                c.wait()
        w = wide(x_ref[r, :])
        a = low(w * norm_scale(w))
        at_ref[:, r] = a.T
        cos, sin = cos_sin(table_ref[r, :])

        def turned(t):
            t = t.astype(bf16).astype(f32)
            return (t * cos + pltpu.roll(t, HALF, ONE) * sin).astype(bf16)

        q = dot(a, wq_ref[...])
        for h in range(HEADS):
            q_ref[h, r, :] = turned(q[:, h * HEAD : (h + ONE) * HEAD])
        k, v = dot(a, wk_ref[...]), dot(a, wv_ref[...]).astype(bf16)
        for g in range(KV):
            one = turned(k[:, g * HEAD : (g + ONE) * HEAD])
            k_ref[g, r, :] = one
            kt_ref[g, :, r] = one.T
            v_ref[g, r, :] = v[:, g * HEAD : (g + ONE) * HEAD]
            vt_ref[g, :HEAD, r] = v[:, g * HEAD : (g + ONE) * HEAD].T
    for g in range(KV):
        vt_ref[g, HEAD:, :] = jnp.ones((16, T), bf16)


    _mark("moments")
    packed[...] = jnp.zeros_like(packed)
    for k, ref in enumerate((three_in, nine_in)):
        pltpu.make_async_copy(ref, ref, s_in.at[len(ahead) + k]).wait()
    for half in (ZERO, ONE):
        for (name, t, n), u in zip(ORDER, STARTS):
            a = half * (m_hbm[INDEX[name]].shape[-ONE] // TWO) + t * LANES
            for k in (ZERO, ONE):
                if n == ONE:
                    at = places[name] + a
                    packed[half, SLOT[u], 3 * k : 3 * k + 3, :] = three_in[k, :, ZERO, at : at + LANES]
                else:
                    s = len(THREE) + 4 * t + TWO * k
                    packed[half, s] = nine_in[k, ZERO:8, ZERO, a : a + LANES]
                    packed[half, s + ONE, ZERO:ONE, :] = nine_in[k, 8:9, ZERO, a : a + LANES]
    moments[j] = packed[core]
    for u in range(FILLED[ZERO], PIECE[ZERO] * NZ):
        col0[u] = jnp.zeros((ROWS, LANES), bf16)
    for u in range(FILLED[ONE], PIECE[ONE] * NZ):
        col1[u] = jnp.zeros((ROWS, LANES), bf16)
    _mark("barrier")
    pl.semaphore_wait(barrier, len(peers))

    for r in range(ONE, COLUMN):
        to = lax.rem(j + r, COLUMN)
        copy(packed.at[lax.rem(to, TWO)], moments.at[j], s_mv, r_mv, column_start + to).start()
    their_moments = copy(moments.at[pl.ds(ZERO, COLUMN - ONE)], moments.at[pl.ds(ZERO, COLUMN - ONE)], s_mv, r_mv, partner)

    _mark("f_att")
    for i in range(T // STEP):
        n = (i + ONE) * STEP
        r = slice(i * STEP, n)
        ok = causal(STEP)

        def head(h, _):
            g = h // GROUP
            s = dot(k_ref[g, :n, :], q_ref[h, r, :], ONE, ONE)
            own = jnp.where(ok, s[n - STEP :, :], HIDDEN)
            top = jnp.max(own, axis=ZERO, keepdims=True)
            parts = [own]
            if i:
                top = jnp.maximum(top, jnp.max(s[: n - STEP, :], axis=ZERO, keepdims=True))
                parts = [s[: n - STEP, :], own]
            out = jnp.zeros((HEAD + 16, STEP), f32)
            at = ZERO
            p = jnp.concatenate([jnp.exp2((part - top) * E).astype(bf16) for part in parts], axis=ZERO)
            out = dot(vt_ref[g, :, :n], p)
            total = out[HEAD : HEAD + ONE, :]
            o = (out[:HEAD, :] * (ONE / total)).astype(bf16)
            rows = pl.ds(pl.multiple_of(h * HEAD, HEAD), HEAD)
            ot_ref[rows, r] = o
            o_s[r, rows] = o.T
            lse_ref[h, :, r] = top * E + jnp.log2(total)

        lax.fori_loop(ZERO, HEADS, head, None)

    _mark("f_wo")
    ahead[8].wait()
    for i in range(T // STEP):
        r = slice(i * STEP, (i + ONE) * STEP)
        out = dot(o_s[r, :], wo_ref[...]).astype(bf16)
        h = (x_ref[r, :].astype(f32) + out.astype(f32)).astype(bf16)
        h_ref[r, :] = h
        w = wide(h)
        b = low(w * norm_scale(w))
        b_ref[r, :] = b
        bt_ref[:, r] = b.T

    def d2d(u, n, slot, number):
        return copy(give.at[:, :, pl.ds(slot, n)], out_w.at[core, :, :, pl.ds(u, n)], s_give.at[slot], r_give.at[number], partner)

    def send_half(flow):
        d2d(flow.u, flow.n, flow.slot, flow.number).start()

    def half_sent(flow):
        d2d(flow.u, flow.n, flow.slot, flow.number).wait_send()

    def block(flow, k, a):
        units = pl.ds(flow.u, flow.n)
        return out_w.at[core, k, a, units] if flow.colour == ZERO else out_w.at[core, a, k, units]

    FIRST, LAST = pl.ds(ZERO, TWO), pl.ds(TWO, TWO)

    def hop(flow, i):
        axis, back = (flow.colour, ONE - flow.colour)[i // 6], i % TWO
        k = turns[axis][((TWO, TWO), (ONE, 3), (ONE, 3))[i % 6 // TWO][back]]
        s, r, to = s_hop.at[i // 6], (r_relay.at[i // 6, flow.number, back] if i % 6 < TWO else r_fin.at[i // 6, flow.number]), along[axis][back]
        u, n = flow.u, flow.n
        if i < 6:
            part = (FIRST, LAST, LAST, FIRST, FIRST, LAST)[i]
            dst = relay.at[back, :, pl.ds(u, n)] if i < TWO else fin.at[back, part, pl.ds(u, n)]
            return copy(block(flow, k, part), dst, s, r, to)
        half = n // TWO
        lo, hi = pl.ds(u, half), pl.ds(u + half, n - half)
        part = (lo, hi, hi, lo, lo, hi)[i - 6]
        return copy(fin.at[ZERO, k, part], (relay2 if i < 8 else fin2).at[back, part], s, r, to)

    def arrived(ref, sem):
        copy(ref, ref, s_rows, sem, partner).wait_recv()

    def gone(ref, sem):
        copy(ref, ref, sem, r_rows, partner).wait_send()

    cols, zrs, gcs = (col0, col1), (zr0, zr1), (gc0, gc1)

    def stage(flow, k):
        u, n = flow.u, flow.n
        units = slice(u, u + n)
        first, second = turns[flow.colour], turns[ONE - flow.colour]
        if k == ZERO:
            d2d(u, n, ZERO, flow.number).wait_recv()

            def add(i, _):
                a, b = lax.div(i, NY), lax.rem(i, NY)
                out_w[core, a, b, units] = low(wide(out_w[core, a, b, units]) + wide(out_w[other, a, b, units]))

            lax.fori_loop(ZERO, PLANE, add, None)
            for i in range(4):
                hop(flow, i).start()
        elif k == ONE:
            for d in (ZERO, ONE):
                hop(flow, d).wait_recv()
                for a in range(TWO):
                    dst = block(flow, first[ONE + TWO * d], TWO * d + a)
                    dst[...] = low(wide(dst[...]) + wide(relay[d, a, units]))
                hop(flow, 4 + d).start()
        elif k == TWO:
            arrived(fin.at[:, :, pl.ds(u, n)], r_fin.at[ZERO, flow.number])

            def total(a, _):
                fin[ZERO, a, units] = low(wide(block(flow, first[ZERO], a)[...]) + wide(fin[ZERO, a, units]) + wide(fin[ONE, a, units]))

            lax.fori_loop(ZERO, 4, total, None)
            for i in range(4):
                hop(flow, 6 + i).start()
        elif k == 3:
            half = n // TWO
            for d, part in enumerate((slice(u, u + half), slice(u + half, u + n))):
                hop(flow, 6 + d).wait_recv()
                a = second[ONE + TWO * d]
                fin[ZERO, a, part] = low(wide(fin[ZERO, a, part]) + wide(relay2[d, part]))
                hop(flow, 10 + d).start()
        else:
            arrived(fin2.at[:, pl.ds(u, n)], r_fin.at[ONE, flow.number])
            cols[flow.late][flow.base : flow.base + n] = low(wide(fin[ZERO, second[ZERO], units]) + wide(fin2[ZERO, units]) + wide(fin2[ONE, units]))

    def scatter(late, k):
        n = PIECE[late]
        return copy(cols[late].at[pl.ds(above[k] * n, n)], zrs[late].at[k - ONE], s_zr.at[late], r_zr.at[late], upward[k])

    def gather(late, k):
        own = pl.ds(z * PIECE[late], PIECE[late])
        return copy(gcs[late].at[own], gcs[late].at[own], s_za.at[late], r_za.at[late], upward[k])

    OTHERS = range(ONE, NZ)

    def column(late, step):
        if step == ZERO:
            for k in OTHERS:
                scatter(late, k).start()
        elif step == ONE:
            arrived(zrs[late], r_zr.at[late])
            n = PIECE[late]
            for i in range(n):
                total = wide(cols[late][z * n + i])
                for k in range(NZ - ONE):
                    total += wide(zrs[late][k, i])
                gcs[late][z * n + i] = low(total)
            for k in OTHERS:
                gather(late, k).start()
        else:
            arrived(gcs[late].at[pl.ds(ZERO, len(OTHERS) * PIECE[late])], r_za.at[late])

    def spread_moments():
        their_moments.wait_recv()
        for name, n in (("w_gate", 9), ("wq", 3), ("w_up", 9), ("wo", 5)):
            u = START[name, ZERO]

            def move(i, _):
                for d in range(COLUMN):
                    m_nat[u + i, 3 * d : 3 * d + 3, :] = moments[d, SLOT[u] + i, ZERO:3, :]
                    v_nat[u + i, 3 * d : 3 * d + 3, :] = moments[d, SLOT[u] + i, 3:6, :]

            lax.fori_loop(ZERO, n, move, None)

        def move_down(t, _):
            for d in range(COLUMN):
                for k, nat in enumerate((m_down, v_down)):
                    s = len(THREE) + 4 * t + TWO * k
                    nat[t, 9 * d : 9 * d + 8, :] = moments[d, s]
                    nat[t, 9 * d + 8 : 9 * d + 9, :] = moments[d, s + ONE, ZERO:ONE, :]

        lax.fori_loop(ZERO, 3, move_down, None)

    def keep(r, u, slot):
        for k in range(PLANE):
            rows = slice(k * ROWS, (k + ONE) * ROWS)
            out_w[core, k // NY, k % NY, u] = low(r[rows, :LANES])
            give[k // NY, k % NY, slot] = low(r[rows, LANES:])

    def pair(ref, t):
        n = ref.shape[ONE]
        return jnp.concatenate([ref[:, lanes(core, t, n)], ref[:, lanes(other, t, n)]], axis=ONE)

    during = {}

    def when(i, *stages):
        during[i] = stages

    when(3, (GATES[ZERO], ZERO), (UPS[ZERO], ZERO))
    when(4, (GATES[ZERO], ONE), (UPS[ZERO], ONE))
    when(5, (GATES[ZERO], TWO), (UPS[ZERO], TWO))
    when(6, (GATES[ZERO], 3), (UPS[ZERO], 3), (GATES[ONE], ZERO), (UPS[ONE], ZERO))
    when(7, (GATES[ZERO], 4), (UPS[ZERO], 4), (GATES[ONE], ONE), (UPS[ONE], ONE))
    when(8, (GATES[ONE], TWO), (UPS[ONE], TWO))

    ahead[9].wait()
    db_s[...] = jnp.zeros_like(db_s)
    _mark("mlp")

    def step(i, _):
        slot = lax.rem(i, TWO)
        for k, ref in enumerate((wg_s, wu_s, wd_s)):
            pltpu.make_async_copy(ref.at[slot], ref.at[slot], s_w.at[slot, k]).wait()

        @pl.when(i + ONE < TILES)
        def _():
            for c in stream(i + ONE, ONE - slot):
                c.start()

        turn = lax.rem(i, 3)

        @pl.when(i >= 3)
        def _():
            for k in (ZERO, 3):
                d2d(ZERO, ONE, k + turn, ZERO).wait_send()

        wg, wu, wd = wg_s[slot], wu_s[slot], wd_s[slot]
        own_rows, other_rows = lanes(core, i, FF), lanes(other, i, FF)
        for c in range(TWO):
            r = slice(c * (T // TWO), (c + ONE) * (T // TWO))
            g, u = dot(b_ref[r, :], wg), dot(b_ref[r, :], wu)
            da = wide(low(dot(dy_ref[r, :], wd, ONE, ONE)))
            s = ONE / (ONE + jnp.exp(-g))
            silu = g * s
            act = low(silu * u).T
            act_s[own_rows, r] = act[:LANES]
            act_s[other_rows, r] = act[LANES:]
            du_s[r, :] = low(da * silu)
            dg_s[r, :] = low(da * u * (s + silu * (ONE - s)))
        for k, stages in during.items():

            @pl.when(i == k)
            def _(stages=stages):
                for flow, n in stages:
                    stage(flow, n)

        for ref, first, k in ((dg_s, START["w_gate", ZERO], ZERO), (du_s, START["w_up", ZERO], 3)):
            keep(dot(bt_ref[...], ref[...]), first + i, k + turn)
            d2d(first + i, ONE, k + turn, k + lax.div(i, 3)).start()
        db_s[...] += dot(dg_s[...], wg, ONE, ONE) + dot(du_s[...], wu, ONE, ONE)

    lax.fori_loop(ZERO, TILES, step, None)

    def down(flow, t, reused):
        for k in reused:
            d2d(ZERO, ONE, k, ZERO).wait_send()
        dy = pair(dy_ref, t)
        for a in range(NX):
            n = FF // NX
            r = dot(act_s[a * n : (a + ONE) * n, :], dy)
            for k in range(NY):
                for i in range(3):
                    rows = slice((3 * k + i) * ROWS, (3 * k + i + ONE) * ROWS)
                    out_w[core, a, k, flow.u + i] = low(r[rows, :LANES])
                    give[a, k, flow.slot + i] = low(r[rows, LANES:])
        send_half(flow)

    _mark("down0")
    down(DOWN0, ZERO, [])
    stage(GATES[ONE], 3)
    stage(UPS[ONE], 3)
    stage(GATES[TWO], ZERO)
    stage(UPS[TWO], ZERO)
    _mark("down1")
    down(DOWN1, ONE, [])
    stage(GATES[ONE], 4)
    stage(UPS[ONE], 4)
    _mark("down2")
    down(DOWN2, TWO, range(3))
    stage(GATES[TWO], ONE)
    stage(UPS[TWO], ONE)
    stage(DOWN0, ZERO)

    _mark("norm")
    for i in range(T // STEP):
        r = slice(i * STEP, (i + ONE) * STEP)
        w, db = wide(h_ref[r, :]), db_s[r, :]
        s = norm_scale(w)
        dh = low(wide(dy_ref[r, :]) + s * (db - w * (s * s * jnp.mean(db * w, axis=ONE, keepdims=True))))
        dh_s[r, :] = dh
        do = low(dot(dh, wo_ref[...], ONE, ONE))
        do_s[r, :] = do
        for h in range(HEADS):
            rows = slice(h * HEAD, (h + ONE) * HEAD)
            delta_s[h, :, r] = jnp.sum(wide(do[:, rows].T) * wide(ot_ref[rows, r]), axis=ZERO, keepdims=True)
        if i == ONE:
            stage(DOWN1, ZERO)
    stage(GATES[TWO], TWO)
    stage(UPS[TWO], TWO)

    _mark("wo")
    for k in range(3):
        d2d(ZERO, ONE, 3 + k, ZERO).wait_send()
    lax.fori_loop(ZERO, 3, lambda i, _: keep(dot(ot_ref[...], pair(dh_s, i)), WO.u + i, WO.slot + i), None)
    send_half(WO)
    stage(DOWN0, ONE)
    stage(DOWN2, ZERO)
    stage(DOWN1, ONE)

    _mark("att")
    later = {
        (ZERO, ZERO): [(GATES[TWO], 3), (UPS[TWO], 3), (WO, ZERO)],
        (ZERO, ONE): [(DOWN0, TWO)],
        (ZERO, TWO): [(DOWN2, ONE), (DOWN1, TWO), (GATES[TWO], 4), (UPS[TWO], 4)],
        (ZERO, 3): [(WO, ONE), (DOWN0, 3), (DOWN1, 3)],
        (ONE, ZERO): [(DOWN2, TWO)],
        (ONE, ONE): [(WO, TWO), (DOWN0, 4), (DOWN1, 4)],
        (ONE, TWO): [(DOWN2, 3), (WO, 3)],
        (ONE, 3): [(DOWN2, 4), (WO, 4)],
    }

    def group(g, _):
        for i in range(T // STEP):
            n = (i + ONE) * STEP
            r = slice(i * STEP, n)
            ok = causal(STEP)
            qs, dos = [], []
            for k in range(GROUP):
                h = g * GROUP + k
                q, do = q_ref[h, r, :], do_s[r, pl.ds(pl.multiple_of(h * HEAD, HEAD), HEAD)]
                qs.append(q)
                dos.append(do)
                to = slice(k * STEP, (k + ONE) * STEP)
                for a in range(ZERO, n, KEYS):
                    keys = slice(a, min(a + KEYS, n))
                    p = jnp.exp2(dot(k_ref[g, keys, :], q, ONE, ONE) * E - lse_ref[h, :, r])
                    if a + KEYS >= n:
                        own = jnp.where(ok, p[n - STEP - a :, :], 0.0)
                        p = own if n - STEP == a else jnp.concatenate([p[: n - STEP - a, :], own], axis=ZERO)
                    p_s[keys, to] = low(p)
                    ds_s[keys, to] = low(p * (dot(v_ref[g, keys, :], do, ONE, ONE) - delta_s[h, :, r]))
            dv = dot(p_s[:n, :], jnp.concatenate(dos, axis=ZERO))
            dk = dot(ds_s[:n, :], jnp.concatenate(qs, axis=ZERO))
            dq = dot(kt_ref[g, :, :n], ds_s[:n, :])
            cos, sin = cos_sin(table_ref[r, :])
            for k in range(GROUP):
                t = dq[:, k * STEP : (k + ONE) * STEP].T * SCALE
                dq_s[r, pl.ds(pl.multiple_of((g * GROUP + k) * HEAD, HEAD), HEAD)] = low(t * cos - pltpu.roll(t, HALF, ONE) * sin)
            if i == ZERO:
                dv_s[:n], dk_s[:n] = dv, dk
            else:
                dv_s[: n - STEP] += dv[: n - STEP]
                dk_s[: n - STEP] += dk[: n - STEP]
                dv_s[r], dk_s[r] = dv[n - STEP :], dk[n - STEP :]
            for which in (ZERO, ONE):
                if later[which, i]:

                    @pl.when(g == which)
                    def _():
                        for flow, m in later[which, i]:
                            stage(flow, m)

        span = pl.ds(pl.multiple_of(g * HEAD, HEAD), HEAD)
        for i in range(T // STEP):
            r = slice(i * STEP, (i + ONE) * STEP)
            cos, sin = cos_sin(table_ref[r, :])
            t = dk_s[r, :] * SCALE
            dkv_s[ZERO][r, span] = low(t * cos - pltpu.roll(t, HALF, ONE) * sin)
            dkv_s[ONE][r, span] = low(dv_s[r, :])

    lax.fori_loop(ZERO, KV, group, None)

    _mark("qkv")
    half_sent(DOWN0)
    half_sent(DOWN1)
    lax.fori_loop(ZERO, 3, lambda i, _: keep(dot(at_ref[...], pair(dq_s, i)), WQ.u + i, WQ.slot + i), None)
    send_half(WQ)
    for i in (ZERO, ONE):
        keep(dot(at_ref[...], pair(dkv_s[i], ZERO)), WKV.u + i, WKV.slot + i)
    send_half(WKV)

    _mark("tail")
    column(ZERO, ZERO)
    stage(WQ, ZERO)
    stage(WKV, ZERO)
    spread_moments()
    stage(WKV, ONE)
    stage(WQ, ONE)
    _mark("tail_z0")
    column(ZERO, ONE)
    _mark("tail_2")
    stage(WKV, TWO)
    stage(WQ, TWO)
    _mark("tail_3")
    stage(WKV, 3)
    stage(WQ, 3)
    _mark("tail_4")
    stage(WKV, 4)
    stage(WQ, 4)
    column(ONE, ZERO)
    _mark("tail_z1")
    column(ZERO, TWO)
    _mark("tail_z2")
    column(ONE, ONE)
    _mark("tail_z3")
    column(ONE, TWO)

    for flow in (DOWN2, WO, WQ, WKV):
        half_sent(flow)
    gone(out_w.at[core, pl.ds(ZERO, 3)], s_hop.at[ZERO])
    gone(out_w.at[core, ZERO, pl.ds(ZERO, 3)], s_hop.at[ONE])
    for late in (ZERO, ONE):
        gone(zrs[late], s_zr.at[late])
        gone(gcs[late].at[pl.ds(ZERO, len(OTHERS) * PIECE[late])], s_za.at[late])
    their_moments.wait_send()

    _mark("norms")
    squares = jnp.zeros((8, LANES), f32)
    for late in (ZERO, ONE):

        def more(i, total):
            g = wide(gcs[late][i])
            return total + (g * g).reshape(ROWS // 8, 8, LANES).sum(ZERO)

        squares = lax.fori_loop(ZERO, FILLED[late], more, squares)
    mine = norms.at[here * TWO + core]
    mine[...] = squares
    for ab, first in plane.items():
        for c in (core, other):
            if any(ab) or c is other:
                copy(mine, mine, s_norm, r_norm, first + c).start()
    pltpu.make_async_copy(old, old, s_old).wait()
    all_norms = copy(norms.at[pl.ds(ZERO, TWO * PLANE - ONE)], norms.at[pl.ds(ZERO, TWO * PLANE - ONE)], s_norm, r_norm, partner)
    all_norms.wait_recv()
    total = norms[...].sum(axis=ZERO)
    total = jnp.sum(jnp.sum(total, axis=ZERO, keepdims=True), axis=ONE, keepdims=True)
    factor = jnp.minimum(1.0, 0.5 * lax.rsqrt(total * (1.0 / COUNT) + 1e-30))

    _mark("adam")

    def stepped(w, m, v, g):
        g = g * factor
        m = 0.9 * m + 0.1 * g
        v = 0.95 * v + 0.05 * g * g
        return low(w - 0.02 * (m * lax.rsqrt(v + 1e-8) + 0.1 * w))

    for name, t, n in (("w_gate", ZERO, 9), ("w_up", ZERO, 9), ("w_down", ZERO, 3), ("w_down", ONE, 3), ("w_down", TWO, 3), ("wq", ZERO, 3), ("wo", ZERO, 3), ("wk", ZERO, TWO)):
        u = START[name, t]
        late = name in ("wq", "wk")
        first = (3 if u >= SPLIT else ZERO) if late else u - 3 * (u >= SPLIT)

        def unit(i, _):
            if name == "w_down":
                rows = pl.ds(pl.multiple_of(i * ROWS, ROWS), ROWS)
                m, v = m_down[t, rows, :], v_down[t, rows, :]
            else:
                m, v = m_nat[u + i], v_nat[u + i]
            out_w[core, x, y, u + i] = stepped(wide(old[u + i]), m, v, wide(gcs[late][first + i]))

        lax.fori_loop(ZERO, n, unit, None)

    _mark("ag0")

    def slot(colour, ps, pb, h=None):
        u, n = COLOURS[colour]
        if h is not None:
            u, n = (u, n // TWO) if h == ZERO else (u + n // TWO, n - n // TWO)
        units = pl.ds(u, n)
        return out_w.at[core, pb, ps, units] if colour == ZERO else out_w.at[core, ps, pb, units]

    def to_partner(colour, ps, pb):
        v = slot(colour, ps, pb)
        copy(v, v, s_core, r_core, partner).start()

    def send(colour, big, rel, ps, pb, h, d, kind):
        v = slot(colour, ps, pb, h)
        copy(v, v, s_ag.at[big], r_big.at[colour, rel, kind] if big else r_small.at[colour, kind], along[colour if big else ONE - colour][d]).start()

    def came(colour, big, rel, kind):
        units = pl.ds(*COLOURS[colour])
        arrived(out_w.at[core, pl.ds(ZERO, TWO), ZERO, units] if kind == ZERO else out_w.at[core, ZERO, ZERO, units], r_big.at[colour, rel, kind] if big else r_small.at[colour, kind])

    def spot(colour):
        return turns[ONE - colour], turns[colour]

    def big_own(colour, rel):
        ps, pb = spot(colour)
        for d in (ZERO, ONE):
            send(colour, ONE, rel, ps[rel], pb[ZERO], None, d, ZERO)

    def big_forward(colour, rel):
        ps, pb = spot(colour)
        came(colour, ONE, rel, ZERO)
        for d in (ZERO, ONE):
            send(colour, ONE, rel, ps[rel], pb[3 - TWO * d], d, d, ONE)
        for d in (ZERO, ONE):
            to_partner(colour, ps[rel], pb[3 - TWO * d])

    def big_far(colour, rel):
        ps, pb = spot(colour)
        came(colour, ONE, rel, ONE)
        to_partner(colour, ps[rel], pb[TWO])

    for colour in (ZERO, ONE):
        ps, pb = spot(colour)
        for d in (ZERO, ONE):
            send(colour, ZERO, ZERO, ps[ZERO], pb[ZERO], None, d, ZERO)
    for colour in (ZERO, ONE):
        big_own(colour, ZERO)
        ps, pb = spot(colour)
        to_partner(colour, ps[ZERO], pb[ZERO])
    for colour in (ZERO, ONE):
        ps, pb = spot(colour)
        came(colour, ZERO, ZERO, ZERO)
        for d in (ZERO, ONE):
            send(colour, ZERO, ZERO, ps[3 - TWO * d], pb[ZERO], d, d, ONE)
        for rel in (3, ONE):
            big_own(colour, rel)
            to_partner(colour, ps[rel], pb[ZERO])

    _mark("rows")

    def picker(height, each, of):
        row, col = lax.broadcasted_iota(jnp.int32, (height, of), ZERO), lax.broadcasted_iota(jnp.int32, (height, of), ONE)
        half = height // TWO
        ours = (row < each) & (col == each * j + row)
        theirs = (row >= half) & (row < half + each) & (col == each * (j + ONE - TWO * core) + row - half)
        return (ours | theirs).astype(f32).astype(bf16)

    three, nine = picker(16, 3, ROWS), picker(32, 9, 3 * ROWS)
    for (name, t, n), u in zip(ORDER, STARTS):
        late = name in ("wq", "wk", "wv")
        a = ((u - START["wk", ZERO] + 3 if u >= SPLIT else u - START["wq", ZERO]) if late else u - 3 * (u >= SPLIT))
        if n == ONE:
            rows = dot(three, gcs[late][a]) * factor
            out_g[core, SLOT[u]], rows_out[SLOT[u]] = rows[:8], rows[8:]
        else:
            rows = dot(nine, gcs[late][a : a + 3].reshape(3 * ROWS, LANES)) * factor
            s = len(THREE) + TWO * t
            for k in (ZERO, ONE):
                out_g[core, s + k], rows_out[s + k] = rows[8 * k : 8 * k + 8], rows[16 + 8 * k : 24 + 8 * k]
    own_rows = copy(rows_out, out_g.at[core], s_rows, r_rows, partner)
    own_rows.start()

    _mark("ag2")
    for colour in (ZERO, ONE):
        ps, pb = spot(colour)
        big_forward(colour, ZERO)
        came(colour, ZERO, ZERO, ONE)
        big_own(colour, TWO)
        to_partner(colour, ps[TWO], pb[ZERO])
    _mark("ag3")
    for colour in (ZERO, ONE):
        big_forward(colour, 3)
        big_forward(colour, ONE)
        big_far(colour, ZERO)
    _mark("ag4")
    for colour in (ZERO, ONE):
        big_forward(colour, TWO)
        big_far(colour, 3)
        big_far(colour, ONE)
    _mark("ag5")
    for colour in (ZERO, ONE):
        big_far(colour, TWO)
    own_rows.wait()
    arrived(out_w.at[other], r_core)
    gone(out_w.at[core], s_core)
    gone(out_w.at[core, ZERO, pl.ds(ZERO, 3)], s_ag.at[ZERO])
    gone(out_w.at[core, pl.ds(ZERO, 3)], s_ag.at[ONE])
    all_norms.wait_send()
    _mark("end")


def layer_step(x, dy, weights, m, v):
    view = lambda t: t.reshape(NX, NY, t.shape[ZERO] // (PLANE * ROWS), ROWS, t.shape[ONE])
    any_ = pl.BlockSpec(memory_space=pl.ANY)
    vmem = pl.BlockSpec(memory_space=pltpu.VMEM)
    low, wide = lambda *s: pltpu.VMEM(s, bf16), lambda *s: pltpu.VMEM(s, f32)
    unit = lambda *lead: low(*lead, ROWS, LANES)
    dma = lambda *shape: pltpu.SemaphoreType.DMA(shape)
    flows = len(FLOWS)
    scratch = [
        wide(T, HEAD), low(D, D), low(T, D), low(D, T), low(HEADS, T, HEAD), low(KV, T, HEAD), low(KV, T, HEAD), low(KV, HEAD, T), low(KV, HEAD + 16, T),
        low(D, T), wide(HEADS, ONE, T), low(T, D), low(T, D), low(D, T),
        low(TWO, D, STEP), low(TWO, D, STEP), low(TWO, STEP, D), low(T, STEP), low(T, STEP),
        low(FF, T), wide(T, D), low(T, D), low(T, D), wide(HEADS, ONE, T),
        unit(NX, NY, GIVE), unit(TWO, TWO, UNITS), unit(TWO, 4, UNITS), unit(TWO, UNITS), unit(TWO, UNITS),
        *(unit(NZ * p) for p in PIECE), *(unit(NZ - ONE, p) for p in PIECE), *(unit(NZ * p) for p in PIECE),
        unit(UNITS), wide(TWO, 3, ONE, sum(t.shape[-ONE] for t in m[:-ONE])), wide(TWO, 9, ONE, D), wide(TWO, SLOTS, 8, LANES), wide(COLUMN, SLOTS, 8, LANES),
        wide(UNITS, ROWS, LANES), wide(UNITS, ROWS, LANES), wide(3, 3 * ROWS, LANES), wide(3, 3 * ROWS, LANES),
        wide(TWO * PLANE, 8, LANES), wide(ROW_SLOTS, 8, LANES),
        dma(12), dma(TWO, 3), dma(), dma(GIVE), dma(flows), dma(TWO), dma(TWO, flows, TWO), dma(TWO, flows), dma(TWO), dma(TWO), dma(TWO), dma(TWO), dma(), dma(), dma(), dma(),
        dma(TWO), dma(TWO, TWO), dma(TWO, 4, TWO), dma(), dma(), dma(), dma(),
    ]
    return pl.pallas_call(
        _step,
        in_specs=[any_] * 31,
        out_specs=[vmem, vmem],
        out_shape=[pltpu.VMEM((TWO, NX, NY, UNITS, ROWS, LANES), bf16), pltpu.VMEM((TWO, ROW_SLOTS, 8, LANES), f32)],
        scratch_shapes=scratch,
        compiler_params=pltpu.CompilerParams(collective_id=ZERO, has_side_effects=True, vmem_limit_bytes=50 * TWO**20),
        name="step",
    )(x, dy, jnp.asarray(rotary()), *weights, *map(view, weights), *m, *v)


def _finish(*refs):
    w_ref, g_ref, m_in, v_in = refs[ZERO], refs[ONE], refs[TWO:9], refs[9:16]
    w_out, m_out, v_out, sem = refs[16:23], refs[23:30], refs[30:37], refs[37]
    copies = []
    for half in (ZERO, ONE):
        for i, (name, t, n) in enumerate(ORDER):
            o = w_out[INDEX[name]]
            a = half * (o.shape[-ONE] // TWO) + t * LANES
            copies.append(pltpu.make_async_copy(w_ref.at[half, :, :, pl.ds(STARTS[i], n)], o.at[:, :, :, :, pl.ds(a, LANES)], sem.at[half, i]))
            copies[-ONE].start()
    for half in (ZERO, ONE):
        for (name, t, n), u in zip(ORDER, STARTS):
            k = INDEX[name]
            a = half * (m_in[k].shape[-ONE] // TWO) + t * LANES
            s = len(THREE) + TWO * t
            for s, r, rows in [(SLOT[u], ZERO, 3)] if n == ONE else [(s, ZERO, 8), (s + ONE, 8, ONE)]:
                g = g_ref[half, s, ZERO:rows, :]
                here = (slice(r, r + rows), ZERO, slice(a, a + LANES))
                m_out[k][here] = 0.9 * m_in[k][here] + 0.1 * g
                v_out[k][here] = 0.95 * v_in[k][here] + 0.05 * g * g
    for c in copies:
        c.wait()


def finish(new, rows, m, v, like):
    any_ = pl.BlockSpec(memory_space=pl.ANY)
    vmem = pl.BlockSpec(memory_space=pltpu.VMEM)
    view = lambda t: (NX, NY, t.shape[ZERO] // (PLANE * ROWS), ROWS, t.shape[ONE])
    out = pl.pallas_call(
        _finish,
        in_specs=[vmem] * 16,
        out_specs=[any_] * 7 + [vmem] * 14,
        out_shape=[jax.ShapeDtypeStruct(view(w), w.dtype) for w in like] + [jax.ShapeDtypeStruct(t.shape, t.dtype) for t in (*m, *v)],
        scratch_shapes=[pltpu.SemaphoreType.DMA((TWO, len(ORDER)))],
        compiler_params=pltpu.CompilerParams(vmem_limit_bytes=16 * TWO**20),
        name="finish",
    )(new, rows, *m, *v)
    return [o.reshape(ONE, *w.shape) for o, w in zip(out[:7], like)], out[7:14], out[14:]


def solution(mesh):
    def step(x, dy, *arrays):
        weights, m, v = (arrays[i : i + 7] for i in (ZERO, 7, 14))
        weights = [w[ZERO] for w in weights]
        m, v = ([t.transpose(ONE, ZERO, TWO) for t in s] for s in (m, v))
        new, rows = layer_step(x[ZERO], dy[ZERO], weights, m, v)
        w, m, v = finish(new, rows, m, v, weights)
        return (*w, *(t.transpose(ONE, ZERO, TWO) for t in (*m, *v)))

    states, all_of, cut = P(("rep", "dp"), None, None), P(None, None, None), P(None, "dp", None)
    return jax.shard_map(
        step,
        mesh=mesh,
        in_specs=(states, states) + (all_of,) * 7 + (cut,) * 14,
        out_specs=(P("rep", None, None),) * 7 + (P("rep", "dp", None),) * 14,
        check_vma=False,
    )
```

```python
import functools

import jax
import jax.numpy as jnp
import numpy as np
from jax import lax
from jax.experimental import pallas as pl
from jax.experimental.pallas import tpu as pltpu
from jax.sharding import PartitionSpec as P

HIDDEN = -2e30
LOG2E = 1.4426950408889634
HEAD = 128
THETA = 10000
ZERO, ONE, TWO = range(3)
NAMES = ("wq", "wk", "wv", "wo", "w_gate", "w_up", "w_down")
T, D, HEADS, KV, GROUP = 1024, 768, 6, TWO, 3
STEP = 256
SCALE = HEAD**-0.5
E = SCALE * LOG2E
HALF = HEAD // TWO
bf16, f32 = jnp.bfloat16, jnp.float32


def dot(a, b, ca=ONE, cb=ZERO):
    return lax.dot_general(a, b, (((ca,), (cb,)), ((), ())), preferred_element_type=f32)


def rotary():
    angle = np.arange(T, dtype=np.float32)[:, None] * np.float32(THETA) ** (-np.arange(HALF, dtype=np.float32) / np.float32(HALF))
    return np.concatenate([np.cos(angle), np.sin(angle)], axis=ONE).astype(np.float32)


def cos_sin(table):
    swapped = pltpu.roll(table, HALF, ONE)
    first = lax.broadcasted_iota(jnp.int32, table.shape, ONE) < HALF
    return jnp.where(first, table, swapped), jnp.where(first, -swapped, table)


def norm_scale(wide):
    return lax.rsqrt(jnp.mean(wide * wide, axis=ONE, keepdims=True) + 1e-6)


def causal(n):
    key = lax.broadcasted_iota(jnp.int32, (n, STEP), ZERO)
    return lax.broadcasted_iota(jnp.int32, (n, STEP), ONE) + (n - STEP) >= key


NX, NY, NZ = 4, 4, 8
PLANE = NX * NY
COLUMN = TWO * NZ
ROWS = 3 * COLUMN
LANES = 128
FF = 2304
TILES = FF // STEP
COUNT = 6881280
_run = lambda name, tiles: [(name, t, ONE) for t in range(tiles)]
ORDER = [("w_down", ZERO, 3), ("w_down", TWO, 3), *_run("w_gate", 9), *_run("wq", 3), *_run("w_up", 9), *_run("wo", 3), *_run("wk", ONE), *_run("wv", ONE), ("w_down", ONE, 3)]
STARTS = [sum(n for _, _, n in ORDER[:i]) for i in range(len(ORDER))]
UNITS = sum(n for _, _, n in ORDER)
START = {(name, t): u for (name, t, _), u in zip(ORDER, STARTS)}
SPLIT = START["w_up", ZERO]
UPRIGHT = 14
COLOURS = ((ZERO, UPRIGHT), (UPRIGHT + NZ, UNITS - UPRIGHT - NZ))
INDEX = {name: i for i, name in enumerate(NAMES)}
MESH = pl.DeviceIdType.MESH
THREE = [u for (_, _, n), u in zip(ORDER, STARTS) if n == ONE]
SLOT = {u: s for s, u in enumerate(THREE)}
SLOTS = len(THREE) + 4 * 3
ROW_SLOTS = len(THREE) + TWO * 3


class Flow:
    def __init__(self, number, name, t, n, batch, base, slot):
        self.number, self.u, self.n, self.batch, self.base, self.slot = number, START[name, t], n, batch, base, slot
        self.colour = int(self.u >= SPLIT)


FLOWS = []
for _batch, _flows in enumerate((
    (("w_gate", ZERO, 3, ZERO), ("w_gate", 3, 3, ZERO), ("w_gate", 6, 3, ZERO), ("w_up", ZERO, 3, 3), ("w_up", 3, 3, 3), ("w_up", 6, 3, 3)),
    (("w_down", ZERO, 3, 6), ("w_down", ONE, 3, 9), ("w_down", TWO, 3, ZERO), ("wo", ZERO, 3, 3)),
    (("wq", ZERO, 3, 6), ("wk", ZERO, TWO, 9)),
)):
    _base = ZERO
    for _name, _t, _n, _slot in _flows:
        FLOWS.append(Flow(len(FLOWS), _name, _t, _n, _batch, _base, _slot))
        _base += _n
GATES, UPS, (DOWN0, DOWN1, DOWN2, WO, WQ, WKV) = FLOWS[:3], FLOWS[3:6], FLOWS[6:]
BATCHES = range(3)
FILLED = [sum(f.n for f in FLOWS if f.batch == k) for k in BATCHES]
PIECE = [-(-n // NZ) for n in FILLED]
PLACE = {f.u + i: (f.batch, f.base + i) for f in FLOWS for i in range(f.n)}
KEYS = 512
GIVE = 12


def _mark(name):
    pass


def _step(*refs):
    it = iter(refs)
    take = lambda n: [next(it) for _ in range(n)]
    x_hbm, dy_hbm, table_hbm, wq_hbm, wk_hbm, wv_hbm, wo_hbm, wg_hbm, wu_hbm, wd_hbm = take(10)
    weights, m_hbm, v_hbm = take(7), take(7), take(7)
    out_w, out_g = take(TWO)
    table_ref, wo_ref, dy_ref, at_ref, q_ref, k_ref, v_ref, kt_ref, vt_ref, ot_ref, lse_ref, h_ref, b_ref, bt_ref = take(14)
    wg_s, wu_s, wd_s, dg_s, du_s, act_s, db_s, dh_s, do_s, delta_s = take(10)
    give, relay, fin, relay2, fin2 = take(5)
    cols, zrs, gcs = take(3), take(3), take(3)
    old, three_in, nine_in, packed, moments, m_nat, v_nat, m_down, v_down, norms, rows_out = take(11)
    s_in, s_w, s_old, s_give, r_give, s_hop, r_relay, r_fin, s_zr, r_zr, s_za, r_za, s_norm, r_norm, s_mv, r_mv, s_ag, r_small, r_big, s_up, r_up, s_core, r_core, s_rows, r_rows = take(25)
    x_ref, wq_ref, wk_ref, wv_ref, o_s = act_s.at[:T, :D], act_s.at[T : T + D, :D], act_s.at[:D, D:], act_s.at[D : TWO * D, D:], dh_s
    dq_s, p_s, ds_s = dh_s, act_s.at[:T, :D], act_s.at[T : TWO * T, :D]
    dk_s, dv_s, dkv_s = db_s.at[:, :HEAD], db_s.at[:, HEAD : TWO * HEAD], (dg_s, du_s)

    me = lax.axis_index("dp")
    core, j, here, y, x = lax.rem(me, TWO), lax.rem(me, COLUMN), lax.div(me, COLUMN), lax.rem(lax.div(me, COLUMN), NY), lax.div(me, COLUMN * NY)
    z, other = lax.div(j, TWO), ONE - core
    turns = [[p, *(lax.rem(p + d, NX) for d in range(ONE, NX))] for p in (x, y)]
    above = [z, *(lax.rem(z + k, NZ) for k in range(ONE, NZ))]
    column_start = here * COLUMN
    plane = {(a, b): (turns[ZERO][a] * NY + turns[ONE][b]) * COLUMN + z * TWO for a in range(NX) for b in range(NY)}
    along = [[plane[d, ZERO] + core for d in (ONE, 3)], [plane[ZERO, d] + core for d in (ONE, 3)]]
    upward = [column_start + k * TWO + core for k in above]
    partner = column_start + z * TWO + other

    def copy(src, dst, s, r, to):
        return pltpu.make_async_remote_copy(src_ref=src, dst_ref=dst, send_sem=s, recv_sem=r, device_id={"dp": to}, device_id_type=MESH)

    def lanes(half, t, width):
        return pl.ds(pl.multiple_of(half * (width // TWO) + t * LANES, LANES), LANES)

    wide = lambda v: v.astype(f32)
    low = lambda v: v.astype(bf16)

    _mark("start")

    def stream(i, slot):
        out = []
        for k, half in enumerate((core, other)):
            span, to = lanes(half, i, FF), pl.ds(k * LANES, LANES)
            for n, (src, dst) in enumerate(((wg_hbm.at[:, span], wg_s.at[slot, :, to]), (wu_hbm.at[:, span], wu_s.at[slot, :, to]), (wd_hbm.at[span, :], wd_s.at[slot, to, :]))):
                out.append(pltpu.make_async_copy(src, dst, s_w.at[slot, n]))
        return out

    ahead = [pltpu.make_async_copy(x_hbm.at[r, :], x_ref.at[r, :], s_in.at[i]) for i, r in enumerate(pl.ds(k * STEP, STEP) for k in range(T // STEP))]
    for src, dst in ((wq_hbm, wq_ref), (table_hbm, table_ref), (wk_hbm, wk_ref), (wv_hbm, wv_ref), (wo_hbm, wo_ref), (dy_hbm, dy_ref)):
        ahead.append(pltpu.make_async_copy(src, dst, s_in.at[len(ahead)]))
    for c in (ahead[ZERO], *ahead[4:8], *ahead[ONE:4], *ahead[8:]):
        c.start()
    places = {}
    for k, ref in enumerate((m_hbm, v_hbm)):
        lane = ZERO
        for name in NAMES:
            src = ref[INDEX[name]]
            if name == "w_down":
                dst, sem = nine_in.at[k], len(ahead) + ONE
            else:
                dst, sem = three_in.at[k, :, :, pl.ds(lane, src.shape[-ONE])], len(ahead)
                places[name] = lane
                lane += src.shape[-ONE]
            pltpu.make_async_copy(src, dst, s_in.at[sem]).start()
    for c in stream(ZERO, ZERO):
        c.start()
    for (name, t, n), u in zip(ORDER, STARTS):
        w = weights[INDEX[name]]
        pltpu.make_async_copy(w.at[x, y, :, :, lanes(core, t, w.shape[-ONE])], old.at[pl.ds(u, n)], s_old).start()

    barrier = pltpu.get_barrier_semaphore()
    peers = [column_start + k * TWO + c for k in above[ONE:] for c in (ZERO, ONE)]
    peers += [first + c for ab, first in plane.items() if any(ab) for c in (ZERO, ONE)]
    peers += [partner]
    for to in peers:
        pl.semaphore_signal(barrier, inc=ONE, device_id={"dp": to}, device_id_type=MESH)

    _mark("front")
    for i in range(T // STEP):
        r = slice(i * STEP, (i + ONE) * STEP)
        ahead[i].wait()
        if i == ZERO:
            for c in ahead[4:8]:
                c.wait()
        w = wide(x_ref[r, :])
        a = low(w * norm_scale(w))
        at_ref[:, r] = a.T
        cos, sin = cos_sin(table_ref[r, :])

        def turned(t):
            t = t.astype(bf16).astype(f32)
            return (t * cos + pltpu.roll(t, HALF, ONE) * sin).astype(bf16)

        q = dot(a, wq_ref[...])
        for h in range(HEADS):
            q_ref[h, r, :] = turned(q[:, h * HEAD : (h + ONE) * HEAD])
        k, v = dot(a, wk_ref[...]), dot(a, wv_ref[...]).astype(bf16)
        for g in range(KV):
            one = turned(k[:, g * HEAD : (g + ONE) * HEAD])
            k_ref[g, r, :] = one
            kt_ref[g, :, r] = one.T
            v_ref[g, r, :] = v[:, g * HEAD : (g + ONE) * HEAD]
            vt_ref[g, :HEAD, r] = v[:, g * HEAD : (g + ONE) * HEAD].T
    for g in range(KV):
        vt_ref[g, HEAD:, :] = jnp.ones((16, T), bf16)


    _mark("moments")
    packed[...] = jnp.zeros_like(packed)
    for k, ref in enumerate((three_in, nine_in)):
        pltpu.make_async_copy(ref, ref, s_in.at[len(ahead) + k]).wait()
    for half in (ZERO, ONE):
        for (name, t, n), u in zip(ORDER, STARTS):
            a = half * (m_hbm[INDEX[name]].shape[-ONE] // TWO) + t * LANES
            for k in (ZERO, ONE):
                if n == ONE:
                    at = places[name] + a
                    packed[half, SLOT[u], 3 * k : 3 * k + 3, :] = three_in[k, :, ZERO, at : at + LANES]
                else:
                    s = len(THREE) + 4 * t + TWO * k
                    packed[half, s] = nine_in[k, ZERO:8, ZERO, a : a + LANES]
                    packed[half, s + ONE, ZERO:ONE, :] = nine_in[k, 8:9, ZERO, a : a + LANES]
    moments[j] = packed[core]
    for k in BATCHES:
        for u in range(FILLED[k], PIECE[k] * NZ):
            cols[k][u] = jnp.zeros((ROWS, LANES), bf16)
    _mark("barrier")
    pl.semaphore_wait(barrier, len(peers))

    for r in range(ONE, COLUMN):
        to = lax.rem(j + r, COLUMN)
        copy(packed.at[lax.rem(to, TWO)], moments.at[j], s_mv, r_mv, column_start + to).start()
    their_moments = copy(moments.at[pl.ds(ZERO, COLUMN - ONE)], moments.at[pl.ds(ZERO, COLUMN - ONE)], s_mv, r_mv, partner)

    _mark("f_att")
    for i in range(T // STEP):
        n = (i + ONE) * STEP
        r = slice(i * STEP, n)
        ok = causal(STEP)

        def heads(g, _):
            tops = []
            for k in range(GROUP):
                q = q_ref[g * GROUP + k, r, :]
                scores = [dot(k_ref[g, a : min(a + KEYS, n), :], q, ONE, ONE) for a in range(ZERO, n, KEYS)]
                last = scores[-ONE]
                own = jnp.where(ok, last[last.shape[ZERO] - STEP :, :], HIDDEN)
                scores[-ONE] = own if last.shape[ZERO] == STEP else jnp.concatenate([last[: last.shape[ZERO] - STEP, :], own], axis=ZERO)
                top = functools.reduce(jnp.maximum, [jnp.max(t, axis=ZERO, keepdims=True) for t in scores])
                for a, t in zip(range(ZERO, n, KEYS), scores):
                    do_s[a : a + t.shape[ZERO], k * STEP : (k + ONE) * STEP] = low(jnp.exp2((t - top) * E))
                tops.append(top)
            out = dot(vt_ref[g, :, :n], do_s[:n, :])
            for k, top in enumerate(tops):
                h, own = g * GROUP + k, slice(k * STEP, (k + ONE) * STEP)
                total = out[HEAD : HEAD + ONE, own]
                o = low(out[:HEAD, own] * (ONE / total))
                rows = pl.ds(pl.multiple_of(h * HEAD, HEAD), HEAD)
                ot_ref[rows, r] = o
                o_s[r, rows] = o.T
                lse_ref[h, :, r] = top * E + jnp.log2(total)

        lax.fori_loop(ZERO, KV, heads, None)

    _mark("f_wo")
    ahead[8].wait()
    for i in range(T // STEP):
        r = slice(i * STEP, (i + ONE) * STEP)
        out = dot(o_s[r, :], wo_ref[...]).astype(bf16)
        h = (x_ref[r, :].astype(f32) + out.astype(f32)).astype(bf16)
        h_ref[r, :] = h
        w = wide(h)
        b = low(w * norm_scale(w))
        b_ref[r, :] = b
        bt_ref[:, r] = b.T

    def d2d(u, n, slot, number):
        return copy(give.at[:, :, pl.ds(slot, n)], out_w.at[core, :, :, pl.ds(u, n)], s_give.at[slot], r_give.at[number], partner)

    def send_half(flow):
        d2d(flow.u, flow.n, flow.slot, flow.number).start()

    def half_sent(flow):
        d2d(flow.u, flow.n, flow.slot, flow.number).wait_send()

    def block(flow, k, a):
        units = pl.ds(flow.u, flow.n)
        return out_w.at[core, k, a, units] if flow.colour == ZERO else out_w.at[core, a, k, units]

    FIRST, LAST = pl.ds(ZERO, TWO), pl.ds(TWO, TWO)

    def hop(flow, i):
        axis, back = (flow.colour, ONE - flow.colour)[i // 6], i % TWO
        k = turns[axis][((TWO, TWO), (ONE, 3), (ONE, 3))[i % 6 // TWO][back]]
        s, r, to = s_hop.at[i // 6], (r_relay.at[i // 6, flow.number, back] if i % 6 < TWO else r_fin.at[i // 6, flow.number]), along[axis][back]
        u, n = flow.u, flow.n
        if i < 6:
            part = (FIRST, LAST, LAST, FIRST, FIRST, LAST)[i]
            dst = relay.at[back, :, pl.ds(u, n)] if i < TWO else fin.at[back, part, pl.ds(u, n)]
            return copy(block(flow, k, part), dst, s, r, to)
        half = n // TWO
        lo, hi = pl.ds(u, half), pl.ds(u + half, n - half)
        part = (lo, hi, hi, lo, lo, hi)[i - 6]
        return copy(fin.at[ZERO, k, part], (relay2 if i < 8 else fin2).at[back, part], s, r, to)

    def arrived(ref, sem):
        copy(ref, ref, s_rows, sem, partner).wait_recv()

    def gone(ref, sem):
        copy(ref, ref, sem, r_rows, partner).wait_send()

    def stage(flow, k):
        u, n = flow.u, flow.n
        units = slice(u, u + n)
        first, second = turns[flow.colour], turns[ONE - flow.colour]
        if k == ZERO:
            d2d(u, n, ZERO, flow.number).wait_recv()

            def add(i, _):
                a, b = lax.div(i, NY), lax.rem(i, NY)
                out_w[core, a, b, units] = low(wide(out_w[core, a, b, units]) + wide(out_w[other, a, b, units]))

            lax.fori_loop(ZERO, PLANE, add, None)
            for i in range(4):
                hop(flow, i).start()
        elif k == ONE:
            for d in (ZERO, ONE):
                hop(flow, d).wait_recv()
                for a in range(TWO):
                    dst = block(flow, first[ONE + TWO * d], TWO * d + a)
                    dst[...] = low(wide(dst[...]) + wide(relay[d, a, units]))
                hop(flow, 4 + d).start()
        elif k == TWO:
            arrived(fin.at[:, :, pl.ds(u, n)], r_fin.at[ZERO, flow.number])

            def total(a, _):
                fin[ZERO, a, units] = low(wide(block(flow, first[ZERO], a)[...]) + wide(fin[ZERO, a, units]) + wide(fin[ONE, a, units]))

            lax.fori_loop(ZERO, 4, total, None)
            for i in range(4):
                hop(flow, 6 + i).start()
        elif k == 3:
            half = n // TWO
            for d, part in enumerate((slice(u, u + half), slice(u + half, u + n))):
                hop(flow, 6 + d).wait_recv()
                a = second[ONE + TWO * d]
                fin[ZERO, a, part] = low(wide(fin[ZERO, a, part]) + wide(relay2[d, part]))
                hop(flow, 10 + d).start()
        else:
            arrived(fin2.at[:, pl.ds(u, n)], r_fin.at[ONE, flow.number])
            cols[flow.batch][flow.base : flow.base + n] = low(wide(fin[ZERO, second[ZERO], units]) + wide(fin2[ZERO, units]) + wide(fin2[ONE, units]))

    def scatter(batch, k):
        n = PIECE[batch]
        return copy(cols[batch].at[pl.ds(above[k] * n, n)], zrs[batch].at[k - ONE], s_zr.at[batch], r_zr.at[batch], upward[k])

    def gather(batch, k):
        own = pl.ds(z * PIECE[batch], PIECE[batch])
        return copy(gcs[batch].at[own], gcs[batch].at[own], s_za.at[batch], r_za.at[batch], upward[k])

    OTHERS = range(ONE, NZ)

    def column(batch, step):
        if step == ZERO:
            for k in OTHERS:
                scatter(batch, k).start()
        elif step == ONE:
            arrived(zrs[batch], r_zr.at[batch])
            n = PIECE[batch]
            for i in range(n):
                total = wide(cols[batch][z * n + i])
                for k in range(NZ - ONE):
                    total += wide(zrs[batch][k, i])
                gcs[batch][z * n + i] = low(total)
            for k in OTHERS:
                gather(batch, k).start()
        else:
            arrived(gcs[batch].at[pl.ds(ZERO, len(OTHERS) * PIECE[batch])], r_za.at[batch])

    def spread_moments():
        their_moments.wait_recv()
        for name, n in (("w_gate", 9), ("wq", 3), ("w_up", 9), ("wo", 5)):
            u = START[name, ZERO]

            def move(i, _):
                for d in range(COLUMN):
                    m_nat[u + i, 3 * d : 3 * d + 3, :] = moments[d, SLOT[u] + i, ZERO:3, :]
                    v_nat[u + i, 3 * d : 3 * d + 3, :] = moments[d, SLOT[u] + i, 3:6, :]

            lax.fori_loop(ZERO, n, move, None)

        def move_down(t, _):
            for d in range(COLUMN):
                for k, nat in enumerate((m_down, v_down)):
                    s = len(THREE) + 4 * t + TWO * k
                    nat[t, 9 * d : 9 * d + 8, :] = moments[d, s]
                    nat[t, 9 * d + 8 : 9 * d + 9, :] = moments[d, s + ONE, ZERO:ONE, :]

        lax.fori_loop(ZERO, 3, move_down, None)

    def keep(r, u, slot):
        for k in range(PLANE):
            rows = slice(k * ROWS, (k + ONE) * ROWS)
            out_w[core, k // NY, k % NY, u] = low(r[rows, :LANES])
            give[k // NY, k % NY, slot] = low(r[rows, LANES:])

    def pair(ref, t):
        n = ref.shape[ONE]
        return jnp.concatenate([ref[:, lanes(core, t, n)], ref[:, lanes(other, t, n)]], axis=ONE)

    during = {}

    def when(i, *stages):
        during[i] = stages

    when(3, (GATES[ZERO], ZERO), (UPS[ZERO], ZERO))
    when(4, (GATES[ZERO], ONE), (UPS[ZERO], ONE))
    when(5, (GATES[ZERO], TWO), (UPS[ZERO], TWO))
    when(6, (GATES[ZERO], 3), (UPS[ZERO], 3), (GATES[ONE], ZERO), (UPS[ONE], ZERO))
    when(7, (GATES[ZERO], 4), (UPS[ZERO], 4), (GATES[ONE], ONE), (UPS[ONE], ONE))
    when(8, (GATES[ONE], TWO), (UPS[ONE], TWO))

    ahead[9].wait()
    db_s[...] = jnp.zeros_like(db_s)
    _mark("mlp")

    def step(i, _):
        slot = lax.rem(i, TWO)
        for k, ref in enumerate((wg_s, wu_s, wd_s)):
            pltpu.make_async_copy(ref.at[slot], ref.at[slot], s_w.at[slot, k]).wait()

        @pl.when(i + ONE < TILES)
        def _():
            for c in stream(i + ONE, ONE - slot):
                c.start()

        turn = lax.rem(i, 3)

        @pl.when(i >= 3)
        def _():
            for k in (ZERO, 3):
                d2d(ZERO, ONE, k + turn, ZERO).wait_send()

        wg, wu, wd = wg_s[slot], wu_s[slot], wd_s[slot]
        own_rows, other_rows = lanes(core, i, FF), lanes(other, i, FF)
        for c in range(TWO):
            r = slice(c * (T // TWO), (c + ONE) * (T // TWO))
            g, u = dot(b_ref[r, :], wg), dot(b_ref[r, :], wu)
            da = wide(low(dot(dy_ref[r, :], wd, ONE, ONE)))
            s = ONE / (ONE + jnp.exp(-g))
            silu = g * s
            act = low(silu * u).T
            act_s[own_rows, r] = act[:LANES]
            act_s[other_rows, r] = act[LANES:]
            du_s[r, :] = low(da * silu)
            dg_s[r, :] = low(da * u * (s + silu * (ONE - s)))
        for k, stages in during.items():

            @pl.when(i == k)
            def _(stages=stages):
                for flow, n in stages:
                    stage(flow, n)

        for ref, first, k in ((dg_s, START["w_gate", ZERO], ZERO), (du_s, START["w_up", ZERO], 3)):
            keep(dot(bt_ref[...], ref[...]), first + i, k + turn)
        db_s[...] += dot(dg_s[...], wg, ONE, ONE) + dot(du_s[...], wu, ONE, ONE)
        for first, k in ((START["w_gate", ZERO], ZERO), (START["w_up", ZERO], 3)):
            d2d(first + i, ONE, k + turn, k + lax.div(i, 3)).start()

    lax.fori_loop(ZERO, TILES, step, None)

    def down(flow, t, reused):
        for k in reused:
            d2d(ZERO, ONE, k, ZERO).wait_send()
        dy = pair(dy_ref, t)
        for a in range(NX):
            n = FF // NX
            r = dot(act_s[a * n : (a + ONE) * n, :], dy)
            for k in range(NY):
                for i in range(3):
                    rows = slice((3 * k + i) * ROWS, (3 * k + i + ONE) * ROWS)
                    out_w[core, a, k, flow.u + i] = low(r[rows, :LANES])
                    give[a, k, flow.slot + i] = low(r[rows, LANES:])
        send_half(flow)

    _mark("down0")
    down(DOWN0, ZERO, [])
    stage(GATES[ONE], 3)
    stage(UPS[ONE], 3)
    stage(GATES[TWO], ZERO)
    stage(UPS[TWO], ZERO)
    _mark("down1")
    down(DOWN1, ONE, [])
    stage(GATES[ONE], 4)
    stage(UPS[ONE], 4)
    _mark("down2")
    down(DOWN2, TWO, range(3))
    stage(GATES[TWO], ONE)
    stage(UPS[TWO], ONE)
    stage(DOWN0, ZERO)

    _mark("norm")
    for i in range(T // STEP):
        r = slice(i * STEP, (i + ONE) * STEP)
        w, db = wide(h_ref[r, :]), db_s[r, :]
        s = norm_scale(w)
        dh = low(wide(dy_ref[r, :]) + s * (db - w * (s * s * jnp.mean(db * w, axis=ONE, keepdims=True))))
        dh_s[r, :] = dh
        do = low(dot(dh, wo_ref[...], ONE, ONE))
        do_s[r, :] = do
        for h in range(HEADS):
            rows = slice(h * HEAD, (h + ONE) * HEAD)
            delta_s[h, :, r] = jnp.sum(wide(do[:, rows].T) * wide(ot_ref[rows, r]), axis=ZERO, keepdims=True)
        if i == ONE:
            stage(DOWN1, ZERO)
    stage(GATES[TWO], TWO)
    stage(UPS[TWO], TWO)

    _mark("wo")
    for k in range(3):
        d2d(ZERO, ONE, 3 + k, ZERO).wait_send()
    lax.fori_loop(ZERO, 3, lambda i, _: keep(dot(ot_ref[...], pair(dh_s, i)), WO.u + i, WO.slot + i), None)
    send_half(WO)
    stage(DOWN0, ONE)
    stage(DOWN1, ONE)

    _mark("att")
    later = {
        (ZERO, ZERO): [(GATES[TWO], 3), (UPS[TWO], 3), (DOWN2, ZERO)],
        (ZERO, ONE): [(WO, ZERO)],
        (ZERO, TWO): [(DOWN0, TWO), (DOWN1, TWO), (GATES[TWO], 4), (UPS[TWO], 4), (None, ZERO)],
        (ZERO, 3): [(DOWN2, ONE), (WO, ONE), (DOWN0, 3), (DOWN1, 3)],
        (ONE, ZERO): [],
        (ONE, ONE): [(DOWN0, 4), (DOWN1, 4)],
        (ONE, TWO): [(DOWN2, TWO), (WO, TWO)],
        (ONE, 3): [(DOWN2, 3), (WO, 3)],
    }

    def group(g, _):
        for i in range(T // STEP):
            n = (i + ONE) * STEP
            r = slice(i * STEP, n)
            ok = causal(STEP)
            qs, dos = [], []
            for k in range(GROUP):
                h = g * GROUP + k
                q, do = q_ref[h, r, :], do_s[r, pl.ds(pl.multiple_of(h * HEAD, HEAD), HEAD)]
                qs.append(q)
                dos.append(do)
                to = slice(k * STEP, (k + ONE) * STEP)
                for a in range(ZERO, n, KEYS):
                    keys = slice(a, min(a + KEYS, n))
                    p = jnp.exp2(dot(k_ref[g, keys, :], q, ONE, ONE) * E - lse_ref[h, :, r])
                    if a + KEYS >= n:
                        own = jnp.where(ok, p[n - STEP - a :, :], 0.0)
                        p = own if n - STEP == a else jnp.concatenate([p[: n - STEP - a, :], own], axis=ZERO)
                    p_s[keys, to] = low(p)
                    ds_s[keys, to] = low(p * (dot(v_ref[g, keys, :], do, ONE, ONE) - delta_s[h, :, r]))
            dv = dot(p_s[:n, :], jnp.concatenate(dos, axis=ZERO))
            dk = dot(ds_s[:n, :], jnp.concatenate(qs, axis=ZERO))
            dq = dot(kt_ref[g, :, :n], ds_s[:n, :])
            cos, sin = cos_sin(table_ref[r, :])
            for k in range(GROUP):
                t = dq[:, k * STEP : (k + ONE) * STEP].T * SCALE
                dq_s[r, pl.ds(pl.multiple_of((g * GROUP + k) * HEAD, HEAD), HEAD)] = low(t * cos - pltpu.roll(t, HALF, ONE) * sin)
            if i == ZERO:
                dv_s[:n], dk_s[:n] = dv, dk
            else:
                dv_s[: n - STEP] += dv[: n - STEP]
                dk_s[: n - STEP] += dk[: n - STEP]
                dv_s[r], dk_s[r] = dv[n - STEP :], dk[n - STEP :]
            for which in (ZERO, ONE):
                if later[which, i]:

                    @pl.when(g == which)
                    def _():
                        for flow, m in later[which, i]:
                            if flow:
                                stage(flow, m)
                            else:
                                column(ZERO, m)

        span = pl.ds(pl.multiple_of(g * HEAD, HEAD), HEAD)
        for i in range(T // STEP):
            r = slice(i * STEP, (i + ONE) * STEP)
            cos, sin = cos_sin(table_ref[r, :])
            t = dk_s[r, :] * SCALE
            dkv_s[ZERO][r, span] = low(t * cos - pltpu.roll(t, HALF, ONE) * sin)
            dkv_s[ONE][r, span] = low(dv_s[r, :])

    lax.fori_loop(ZERO, KV, group, None)

    _mark("qkv")
    half_sent(DOWN0)
    half_sent(DOWN1)
    lax.fori_loop(ZERO, 3, lambda i, _: keep(dot(at_ref[...], pair(dq_s, i)), WQ.u + i, WQ.slot + i), None)
    send_half(WQ)
    for i in (ZERO, ONE):
        keep(dot(at_ref[...], pair(dkv_s[i], ZERO)), WKV.u + i, WKV.slot + i)
    send_half(WKV)

    _mark("tail")
    stage(DOWN2, 4)
    stage(WO, 4)
    column(ONE, ZERO)
    stage(WQ, ZERO)
    column(ZERO, ONE)
    stage(WKV, ZERO)
    _mark("tail_m")
    spread_moments()
    _mark("tail_1")
    stage(WQ, ONE)
    stage(WKV, ONE)
    column(ONE, ONE)
    _mark("tail_2")
    stage(WQ, TWO)
    stage(WKV, TWO)
    _mark("tail_3")
    stage(WQ, 3)
    stage(WKV, 3)
    _mark("tail_4")
    stage(WQ, 4)
    stage(WKV, 4)
    column(TWO, ZERO)
    _mark("tail_z0")
    column(ZERO, TWO)
    gone(out_w.at[core, pl.ds(ZERO, 3)], s_hop.at[ZERO])
    gone(out_w.at[core, ZERO, pl.ds(ZERO, 3)], s_hop.at[ONE])
    _mark("tail_z1")
    column(TWO, ONE)
    _mark("tail_z2")
    column(ONE, TWO)

    def squares(batch, total):
        def more(i, total):
            g = wide(gcs[batch][i])
            return total + (g * g).reshape(ROWS // 8, 8, LANES).sum(ZERO)

        return lax.fori_loop(ZERO, FILLED[batch], more, total)

    first_squares = squares(ONE, squares(ZERO, jnp.zeros((8, LANES), f32)))
    _mark("tail_z3")
    column(TWO, TWO)
    for flow in (DOWN2, WO, WQ, WKV):
        half_sent(flow)
    for batch in BATCHES:
        gone(zrs[batch], s_zr.at[batch])
        gone(gcs[batch].at[pl.ds(ZERO, len(OTHERS) * PIECE[batch])], s_za.at[batch])
    their_moments.wait_send()

    _mark("norms")
    mine = norms.at[here * TWO + core]
    mine[...] = squares(TWO, first_squares)
    for ab, first in plane.items():
        for c in (core, other):
            if any(ab) or c is other:
                copy(mine, mine, s_norm, r_norm, first + c).start()
    pltpu.make_async_copy(old, old, s_old).wait()
    all_norms = copy(norms.at[pl.ds(ZERO, TWO * PLANE - ONE)], norms.at[pl.ds(ZERO, TWO * PLANE - ONE)], s_norm, r_norm, partner)
    all_norms.wait_recv()
    total = norms[...].sum(axis=ZERO)
    total = jnp.sum(jnp.sum(total, axis=ZERO, keepdims=True), axis=ONE, keepdims=True)
    factor = jnp.minimum(1.0, 0.5 * lax.rsqrt(total * (1.0 / COUNT) + 1e-30))

    _mark("adam")

    def stepped(w, m, v, g):
        g = g * factor
        m = 0.9 * m + 0.1 * g
        v = 0.95 * v + 0.05 * g * g
        return low(w - 0.02 * (m * lax.rsqrt(v + 1e-8) + 0.1 * w))

    def new_units(name, t, n):
        u = START[name, t]
        batch, first = PLACE[u]

        def unit(i, _):
            if name == "w_down":
                rows = pl.ds(pl.multiple_of(i * ROWS, ROWS), ROWS)
                m, v = m_down[t, rows, :], v_down[t, rows, :]
            else:
                m, v = m_nat[u + i], v_nat[u + i]
            out_w[core, x, y, u + i] = stepped(wide(old[u + i]), m, v, wide(gcs[batch][first + i]))

        lax.fori_loop(ZERO, n, unit, None)

    for k, (name, t) in enumerate((name, t) for (name, t, n), u in zip(ORDER, STARTS) if UPRIGHT <= u < UPRIGHT + NZ):

        @pl.when(z == k)
        def _(name=name, t=t):
            new_units(name, t, ONE)

    def upright(k, part=pl.ds(ZERO, NX)):
        return out_w.at[core, part, :, pl.ds(UPRIGHT + above[k], ONE)]

    mine = out_w.at[core, x, y, pl.ds(UPRIGHT + z, ONE)]
    for ab, first in plane.items():
        if any(ab):
            copy(mine, mine, s_up.at[ZERO], r_up.at[ZERO], first + core).start()
    for name, t, n in (("w_gate", ZERO, 8), ("w_down", ZERO, 3), ("w_down", TWO, 3), ("w_up", 4, 5), ("w_down", ONE, 3), ("wo", ZERO, 3), ("wk", ZERO, TWO)):
        new_units(name, t, n)

    _mark("ag0")

    def slot(colour, ps, pb, h=None):
        u, n = COLOURS[colour]
        if h is not None:
            u, n = (u, n // TWO) if h == ZERO else (u + n // TWO, n - n // TWO)
        units = pl.ds(u, n)
        return out_w.at[core, pb, ps, units] if colour == ZERO else out_w.at[core, ps, pb, units]

    def give_partner(v):
        copy(v, v, s_core, r_core, partner).start()

    def to_partner(colour, ps, pb):
        give_partner(slot(colour, ps, pb))

    def send(colour, big, rel, ps, pb, h, d, kind):
        v = slot(colour, ps, pb, h)
        copy(v, v, s_ag.at[big], r_big.at[colour, rel, kind] if big else r_small.at[colour, kind], along[colour if big else ONE - colour][d]).start()

    def came(colour, big, rel, kind):
        units = pl.ds(*COLOURS[colour])
        arrived(out_w.at[core, pl.ds(ZERO, TWO), ZERO, units] if kind == ZERO else out_w.at[core, ZERO, ZERO, units], r_big.at[colour, rel, kind] if big else r_small.at[colour, kind])

    def spot(colour):
        return turns[ONE - colour], turns[colour]

    def big_own(colour, rel):
        ps, pb = spot(colour)
        for d in (ZERO, ONE):
            send(colour, ONE, rel, ps[rel], pb[ZERO], None, d, ZERO)

    def big_forward(colour, rel):
        ps, pb = spot(colour)
        came(colour, ONE, rel, ZERO)
        for d in (ZERO, ONE):
            send(colour, ONE, rel, ps[rel], pb[3 - TWO * d], d, d, ONE)
        for d in (ZERO, ONE):
            to_partner(colour, ps[rel], pb[3 - TWO * d])

    def big_far(colour, rel):
        ps, pb = spot(colour)
        came(colour, ONE, rel, ONE)
        to_partner(colour, ps[rel], pb[TWO])

    def rise(k):
        arrived(out_w.at[core, pl.ds(ZERO, 3), ZERO, pl.ds(ZERO, 5)] if k == ZERO else out_w.at[core, :, :, pl.ds(ZERO, TWO if k < 4 else ONE)], r_up.at[k])
        came_from = sorted({-k % NZ, k}, reverse=True)
        if k < 4:
            for d in (ZERO, ONE):
                v = upright(came_from[min(d, k)], pl.ds(ZERO, NX) if k < 3 else (FIRST, LAST)[d])
                copy(v, v, s_up.at[ONE], r_up.at[k + ONE], upward[(ONE, NZ - ONE)[d]]).start()
        for c in came_from:
            give_partner(upright(c))

    def small_own(colour):
        ps, pb = spot(colour)
        for d in (ZERO, ONE):
            send(colour, ZERO, ZERO, ps[ZERO], pb[ZERO], None, d, ZERO)

    def small_forward(colour):
        ps, pb = spot(colour)
        came(colour, ZERO, ZERO, ZERO)
        for d in (ZERO, ONE):
            send(colour, ZERO, ZERO, ps[3 - TWO * d], pb[ZERO], d, d, ONE)
        for rel in (3, ONE):
            big_own(colour, rel)
            to_partner(colour, ps[rel], pb[ZERO])

    def small_far(colour):
        ps, pb = spot(colour)
        came(colour, ZERO, ZERO, ONE)
        big_own(colour, TWO)
        to_partner(colour, ps[TWO], pb[ZERO])

    small_own(ZERO)
    small_own(ONE)
    for colour in (ZERO, ONE):
        ps, pb = spot(colour)
        big_own(colour, ZERO)
        to_partner(colour, ps[ZERO], pb[ZERO])

    _mark("rows")

    def picker(height, each, of):
        row, col = lax.broadcasted_iota(jnp.int32, (height, of), ZERO), lax.broadcasted_iota(jnp.int32, (height, of), ONE)
        half = height // TWO
        ours = (row < each) & (col == each * j + row)
        theirs = (row >= half) & (row < half + each) & (col == each * (j + ONE - TWO * core) + row - half)
        return (ours | theirs).astype(f32).astype(bf16)

    three, nine = picker(16, 3, ROWS), picker(32, 9, 3 * ROWS)
    for (name, t, n), u in zip(ORDER, STARTS):
        batch, a = PLACE[u]
        if n == ONE:
            rows = dot(three, gcs[batch][a]) * factor
            out_g[core, SLOT[u]], rows_out[SLOT[u]] = rows[:8], rows[8:]
        else:
            rows = dot(nine, gcs[batch][a : a + 3].reshape(3 * ROWS, LANES)) * factor
            s = len(THREE) + TWO * t
            for k in (ZERO, ONE):
                out_g[core, s + k], rows_out[s + k] = rows[8 * k : 8 * k + 8], rows[16 + 8 * k : 24 + 8 * k]
    own_rows = copy(rows_out, out_g.at[core], s_rows, r_rows, partner)
    own_rows.start()

    _mark("ag1")
    small_forward(ZERO)
    small_forward(ONE)
    rise(ZERO)
    _mark("ag2")
    big_forward(ZERO, ZERO)
    big_forward(ONE, ZERO)
    rise(ONE)
    small_far(ZERO)
    small_far(ONE)
    _mark("ag3")
    big_forward(ZERO, 3)
    big_forward(ONE, 3)
    rise(TWO)
    big_forward(ZERO, ONE)
    big_forward(ONE, ONE)
    big_far(ZERO, ZERO)
    big_far(ONE, ZERO)
    rise(3)
    _mark("ag4")
    big_forward(ZERO, TWO)
    big_forward(ONE, TWO)
    for rel in (3, ONE):
        big_far(ZERO, rel)
        big_far(ONE, rel)
    rise(4)
    _mark("ag5")
    big_far(ZERO, TWO)
    big_far(ONE, TWO)
    own_rows.wait()
    arrived(out_w.at[other], r_core)
    gone(out_w.at[core], s_core)
    shared = pl.ds(ZERO, UNITS - NZ)
    gone(out_w.at[core, ZERO, pl.ds(ZERO, 3), shared], s_ag.at[ZERO])
    gone(out_w.at[core, pl.ds(ZERO, 3), :, shared], s_ag.at[ONE])
    gone(out_w.at[core, pl.ds(ZERO, 3), ZERO, pl.ds(ZERO, 5)], s_up.at[ZERO])
    gone(out_w.at[core, :, :, pl.ds(ZERO, 7)], s_up.at[ONE])
    all_norms.wait_send()
    _mark("end")


def layer_step(x, dy, weights, m, v):
    view = lambda t: t.reshape(NX, NY, t.shape[ZERO] // (PLANE * ROWS), ROWS, t.shape[ONE])
    any_ = pl.BlockSpec(memory_space=pl.ANY)
    vmem = pl.BlockSpec(memory_space=pltpu.VMEM)
    low, wide = lambda *s: pltpu.VMEM(s, bf16), lambda *s: pltpu.VMEM(s, f32)
    unit = lambda *lead: low(*lead, ROWS, LANES)
    dma = lambda *shape: pltpu.SemaphoreType.DMA(shape)
    flows = len(FLOWS)
    scratch = [
        wide(T, HEAD), low(D, D), low(T, D), low(D, T), low(HEADS, T, HEAD), low(KV, T, HEAD), low(KV, T, HEAD), low(KV, HEAD, T), low(KV, HEAD + 16, T),
        low(D, T), wide(HEADS, ONE, T), low(T, D), low(T, D), low(D, T),
        low(TWO, D, STEP), low(TWO, D, STEP), low(TWO, STEP, D), low(T, STEP), low(T, STEP),
        low(FF, T), wide(T, D), low(T, D), low(T, D), wide(HEADS, ONE, T),
        unit(NX, NY, GIVE), unit(TWO, TWO, UNITS), unit(TWO, 4, UNITS), unit(TWO, UNITS), unit(TWO, UNITS),
        *(unit(NZ * p) for p in PIECE), *(unit(NZ - ONE, p) for p in PIECE), *(unit(NZ * p) for p in PIECE),
        unit(UNITS), wide(TWO, 3, ONE, sum(t.shape[-ONE] for t in m[:-ONE])), wide(TWO, 9, ONE, D), wide(TWO, SLOTS, 8, LANES), wide(COLUMN, SLOTS, 8, LANES),
        wide(UNITS, ROWS, LANES), wide(UNITS, ROWS, LANES), wide(3, 3 * ROWS, LANES), wide(3, 3 * ROWS, LANES),
        wide(TWO * PLANE, 8, LANES), wide(ROW_SLOTS, 8, LANES),
        dma(12), dma(TWO, 3), dma(), dma(GIVE), dma(flows), dma(TWO), dma(TWO, flows, TWO), dma(TWO, flows), *[dma(len(BATCHES))] * 4, dma(), dma(), dma(), dma(),
        dma(TWO), dma(TWO, TWO), dma(TWO, 4, TWO), dma(TWO), dma(5), dma(), dma(), dma(), dma(),
    ]
    return pl.pallas_call(
        _step,
        in_specs=[any_] * 31,
        out_specs=[vmem, vmem],
        out_shape=[pltpu.VMEM((TWO, NX, NY, UNITS, ROWS, LANES), bf16), pltpu.VMEM((TWO, ROW_SLOTS, 8, LANES), f32)],
        scratch_shapes=scratch,
        compiler_params=pltpu.CompilerParams(collective_id=ZERO, has_side_effects=True, vmem_limit_bytes=50 * TWO**20),
        name="step",
    )(x, dy, jnp.asarray(rotary()), *weights, *map(view, weights), *m, *v)


def _finish(*refs):
    w_ref, g_ref, m_in, v_in = refs[ZERO], refs[ONE], refs[TWO:9], refs[9:16]
    w_out, m_out, v_out, sem = refs[16:23], refs[23:30], refs[30:37], refs[37]
    copies = []
    for half in (ZERO, ONE):
        for i, (name, t, n) in enumerate(ORDER):
            o = w_out[INDEX[name]]
            a = half * (o.shape[-ONE] // TWO) + t * LANES
            copies.append(pltpu.make_async_copy(w_ref.at[half, :, :, pl.ds(STARTS[i], n)], o.at[:, :, :, :, pl.ds(a, LANES)], sem.at[half, i]))
            copies[-ONE].start()
    for half in (ZERO, ONE):
        for (name, t, n), u in zip(ORDER, STARTS):
            k = INDEX[name]
            a = half * (m_in[k].shape[-ONE] // TWO) + t * LANES
            s = len(THREE) + TWO * t
            for s, r, rows in [(SLOT[u], ZERO, 3)] if n == ONE else [(s, ZERO, 8), (s + ONE, 8, ONE)]:
                g = g_ref[half, s, ZERO:rows, :]
                here = (slice(r, r + rows), ZERO, slice(a, a + LANES))
                m_out[k][here] = 0.9 * m_in[k][here] + 0.1 * g
                v_out[k][here] = 0.95 * v_in[k][here] + 0.05 * g * g
    for c in copies:
        c.wait()


def finish(new, rows, m, v, like):
    any_ = pl.BlockSpec(memory_space=pl.ANY)
    vmem = pl.BlockSpec(memory_space=pltpu.VMEM)
    view = lambda t: (NX, NY, t.shape[ZERO] // (PLANE * ROWS), ROWS, t.shape[ONE])
    out = pl.pallas_call(
        _finish,
        in_specs=[vmem] * 16,
        out_specs=[any_] * 7 + [vmem] * 14,
        out_shape=[jax.ShapeDtypeStruct(view(w), w.dtype) for w in like] + [jax.ShapeDtypeStruct(t.shape, t.dtype) for t in (*m, *v)],
        scratch_shapes=[pltpu.SemaphoreType.DMA((TWO, len(ORDER)))],
        compiler_params=pltpu.CompilerParams(vmem_limit_bytes=16 * TWO**20),
        name="finish",
    )(new, rows, *m, *v)
    return [o.reshape(ONE, *w.shape) for o, w in zip(out[:7], like)], out[7:14], out[14:]


def solution(mesh):
    def step(x, dy, *arrays):
        weights, m, v = (arrays[i : i + 7] for i in (ZERO, 7, 14))
        weights = [w[ZERO] for w in weights]
        m, v = ([t.transpose(ONE, ZERO, TWO) for t in s] for s in (m, v))
        new, rows = layer_step(x[ZERO], dy[ZERO], weights, m, v)
        w, m, v = finish(new, rows, m, v, weights)
        return (*w, *(t.transpose(ONE, ZERO, TWO) for t in (*m, *v)))

    states, all_of, cut = P(("rep", "dp"), None, None), P(None, None, None), P(None, "dp", None)
    return jax.shard_map(
        step,
        mesh=mesh,
        in_specs=(states, states) + (all_of,) * 7 + (cut,) * 14,
        out_specs=(P("rep", None, None),) * 7 + (P("rep", "dp", None),) * 14,
        check_vma=False,
    )
```

```python
import functools

import jax
import jax.numpy as jnp
import numpy as np
from jax import lax
from jax.experimental import pallas as pl
from jax.experimental.pallas import tpu as pltpu
from jax.sharding import PartitionSpec as P

HIDDEN = -2e30
LOG2E = 1.4426950408889634
HEAD = 128
THETA = 10000
ZERO, ONE, TWO = range(3)
NAMES = ("wq", "wk", "wv", "wo", "w_gate", "w_up", "w_down")
T, D, HEADS, KV, GROUP = 1024, 768, 6, TWO, 3
STEP = 256
SCALE = HEAD**-0.5
E = SCALE * LOG2E
HALF = HEAD // TWO
FINE = 32
bf16, f32 = jnp.bfloat16, jnp.float32


def dot(a, b, ca=ONE, cb=ZERO):
    return lax.dot_general(a, b, (((ca,), (cb,)), ((), ())), preferred_element_type=f32)


def rotary():
    rate = float(THETA) ** (-np.arange(HALF) / HALF)
    (c, s), (d, e) = ([fn(np.arange(FINE)[:, None] * step * rate) for fn in (np.cos, np.sin)] for step in (FINE, ONE))
    return np.concatenate([np.concatenate(pair, axis=ONE) for pair in ((c, s), (s, c), (d, d), (-e, e))]).astype(np.float32)


def cos_sin(table):
    swapped = pltpu.roll(table, HALF, ONE)
    first = lax.broadcasted_iota(jnp.int32, table.shape, ONE) < HALF
    return jnp.where(first, table, swapped), jnp.where(first, -swapped, table)


def norm_scale(wide):
    return lax.rsqrt(jnp.mean(wide * wide, axis=ONE, keepdims=True) + 1e-6)


def causal(n):
    key = lax.broadcasted_iota(jnp.int32, (n, STEP), ZERO)
    return lax.broadcasted_iota(jnp.int32, (n, STEP), ONE) + (n - STEP) >= key


NX, NY, NZ = 4, 4, 8
PLANE = NX * NY
COLUMN = TWO * NZ
ROWS = 3 * COLUMN
LANES = 128
FF = 2304
TILES = FF // STEP
COUNT = 6881280
_run = lambda name, tiles: [(name, t, ONE) for t in range(tiles)]
ORDER = [("w_down", ZERO, 3), ("w_down", TWO, 3), *_run("w_gate", 9), *_run("wq", 3), *_run("w_up", 9), *_run("wo", 3), *_run("wk", ONE), *_run("wv", ONE), ("w_down", ONE, 3)]
STARTS = [sum(n for _, _, n in ORDER[:i]) for i in range(len(ORDER))]
UNITS = sum(n for _, _, n in ORDER)
START = {(name, t): u for (name, t, _), u in zip(ORDER, STARTS)}
SPLIT = START["w_up", ZERO]
UPRIGHT = 14
COLOURS = ((ZERO, UPRIGHT), (UPRIGHT + NZ, UNITS - UPRIGHT - NZ))
INDEX = {name: i for i, name in enumerate(NAMES)}
MESH = pl.DeviceIdType.MESH
THREE = [u for (_, _, n), u in zip(ORDER, STARTS) if n == ONE]
SLOT = {u: s for s, u in enumerate(THREE)}
SLOTS = len(THREE) + 4 * 3
ROW_SLOTS = len(THREE) + TWO * 3


class Flow:
    def __init__(self, number, name, t, n, batch, base, slot):
        self.number, self.u, self.n, self.batch, self.base, self.slot = number, START[name, t], n, batch, base, slot
        self.colour = int(self.u >= SPLIT)


FLOWS, _filled = [], [ZERO] * 4
for _name, _t, _n, _batch, _slot in (
    *(("w_gate", t, 3, t // 6, ZERO) for t in (ZERO, 3, 6)),
    *(("w_up", t, 3, t // 6, 3) for t in (ZERO, 3, 6)),
    ("w_down", ZERO, 3, ONE, 6), ("w_down", ONE, 3, ONE, 9), ("w_down", TWO, 3, TWO, ZERO), ("wo", ZERO, 3, TWO, 3), ("wq", ZERO, 3, 3, 6), ("wk", ZERO, TWO, 3, 9),
):
    FLOWS.append(Flow(len(FLOWS), _name, _t, _n, _batch, _filled[_batch], _slot))
    _filled[_batch] += _n
GATES, UPS, (DOWN0, DOWN1, DOWN2, WO, WQ, WKV) = FLOWS[:3], FLOWS[3:6], FLOWS[6:]
FILLED = tuple(_filled)
BATCHES = range(len(FILLED))
PIECE = [-(-n // NZ) for n in FILLED]
PLACE = {f.u + i: (f.batch, f.base + i) for f in FLOWS for i in range(f.n)}
RUNS = []
for (_name, _t, _n), _u in zip(ORDER, STARTS):
    if UPRIGHT <= _u < UPRIGHT + NZ:
        continue
    _name0, _t0, _n0 = RUNS[-ONE] if RUNS else ("", ZERO, ZERO)
    if _n == ONE and _name == _name0 and _t == _t0 + _n0 and PLACE[_u][ZERO] == PLACE[_u - ONE][ZERO]:
        RUNS[-ONE] = (_name0, _t0, _n0 + ONE)
    else:
        RUNS.append((_name, _t, _n))
KEYS = 512
GIVE = 12


def _mark(name):
    pass


def _step(*refs):
    it = iter(refs)
    take = lambda n: [next(it) for _ in range(n)]
    x_hbm, dy_hbm, table_hbm, wq_hbm, wk_hbm, wv_hbm, wo_hbm, wg_hbm, wu_hbm, wd_hbm = take(10)
    weights, m_hbm, v_hbm = take(7), take(7), take(7)
    out_w, three_out, nine_out = take(3)
    rot_ref, table_ref, wo_ref, dy_ref, at_ref, q_ref, k_ref, v_ref, kt_ref, vt_ref, ot_ref, lse_ref, h_ref, b_ref, bt_ref = take(15)
    wg_s, wu_s, wd_s, dg_s, du_s, act_s, db_s, dh_s, do_s, delta_s = take(10)
    give, relay, fin, relay2, fin2 = take(5)
    cols, zrs, gcs = (take(len(BATCHES)) for _ in range(3))
    old, three_in, nine_in, packed, moments, m_nat, v_nat, m_down, v_down, norms, rows_out, out_g = take(12)
    s_in, s_w, s_old, s_give, r_give, s_hop, r_relay, r_fin, s_zr, r_zr, s_za, r_za, s_norm, r_norm, s_mv, r_mv, s_ag, r_small, r_big, s_up, r_up, s_core, r_core, s_rows, r_rows = take(25)
    x_ref, wq_ref, wk_ref, wv_ref, o_s = act_s.at[:T, :D], act_s.at[T : T + D, :D], act_s.at[:D, D:], act_s.at[D : TWO * D, D:], dh_s
    dq_s, p_s, ds_s = dh_s, act_s.at[:T, :D], act_s.at[T : TWO * T, :D]
    dk_s, dv_s, dkv_s = db_s.at[:, :HEAD], db_s.at[:, HEAD : TWO * HEAD], (dg_s, du_s)

    me = lax.axis_index("dp")
    core, j, here, y, x = lax.rem(me, TWO), lax.rem(me, COLUMN), lax.div(me, COLUMN), lax.rem(lax.div(me, COLUMN), NY), lax.div(me, COLUMN * NY)
    z, other = lax.div(j, TWO), ONE - core
    turns = [[p, *(lax.rem(p + d, NX) for d in range(ONE, NX))] for p in (x, y)]
    above = [z, *(lax.rem(z + k, NZ) for k in range(ONE, NZ))]
    column_start = here * COLUMN
    plane = {(a, b): (turns[ZERO][a] * NY + turns[ONE][b]) * COLUMN + z * TWO for a in range(NX) for b in range(NY)}
    along = [[plane[d, ZERO] + core for d in (ONE, 3)], [plane[ZERO, d] + core for d in (ONE, 3)]]
    upward = [column_start + k * TWO + core for k in above]
    partner = column_start + z * TWO + other

    def copy(src, dst, s, r, to):
        return pltpu.make_async_remote_copy(src_ref=src, dst_ref=dst, send_sem=s, recv_sem=r, device_id={"dp": to}, device_id_type=MESH)

    def lanes(half, t, width):
        return pl.ds(pl.multiple_of(half * (width // TWO) + t * LANES, LANES), LANES)

    wide = lambda v: v.astype(f32)
    low = lambda v: v.astype(bf16)

    _mark("start")

    def stream(i, slot):
        out = []
        for k, half in enumerate((core, other)):
            span, to = lanes(half, i, FF), pl.ds(k * LANES, LANES)
            for n, (src, dst) in enumerate(((wg_hbm.at[:, span], wg_s.at[slot, :, to]), (wu_hbm.at[:, span], wu_s.at[slot, :, to]), (wd_hbm.at[span, :], wd_s.at[slot, to, :]))):
                out.append(pltpu.make_async_copy(src, dst, s_w.at[slot, n]))
        return out

    ahead = [pltpu.make_async_copy(x_hbm.at[r, :], x_ref.at[r, :], s_in.at[i]) for i, r in enumerate(pl.ds(k * STEP, STEP) for k in range(T // STEP))]
    for src, dst in ((wq_hbm, wq_ref), (table_hbm, rot_ref), (wk_hbm, wk_ref), (wv_hbm, wv_ref), (wo_hbm, wo_ref), (dy_hbm, dy_ref)):
        ahead.append(pltpu.make_async_copy(src, dst, s_in.at[len(ahead)]))
    for c in (ahead[5], ahead[ZERO], ahead[4], *ahead[6:8], *ahead[ONE:4], *ahead[8:]):
        c.start()
    places = {}
    for k, ref in enumerate((m_hbm, v_hbm)):
        lane = ZERO
        for name in NAMES:
            src = ref[INDEX[name]]
            if name == "w_down":
                dst, sem = nine_in.at[k], len(ahead) + ONE
            else:
                dst, sem = three_in.at[k, :, :, pl.ds(lane, src.shape[-ONE])], len(ahead)
                places[name] = lane
                lane += src.shape[-ONE]
            pltpu.make_async_copy(src, dst, s_in.at[sem]).start()
    for c in stream(ZERO, ZERO):
        c.start()
    for (name, t, n), u in zip(ORDER, STARTS):
        w = weights[INDEX[name]]
        pltpu.make_async_copy(w.at[x, y, :, :, lanes(core, t, w.shape[-ONE])], old.at[pl.ds(u, n)], s_old).start()

    barrier = pltpu.get_barrier_semaphore()
    peers = [column_start + k * TWO + c for k in above[ONE:] for c in (ZERO, ONE)]
    peers += [first + c for ab, first in plane.items() if any(ab) for c in (ZERO, ONE)]
    peers += [partner]
    for to in peers:
        pl.semaphore_signal(barrier, inc=ONE, device_id={"dp": to}, device_id_type=MESH)

    _mark("front")
    ahead[5].wait()

    def angles(i, _):
        table_ref[pl.ds(pl.multiple_of(i * FINE, FINE), FINE), :] = (
            rot_ref[pl.ds(i, ONE), :] * rot_ref[TWO * FINE : 3 * FINE, :] + rot_ref[pl.ds(FINE + i, ONE), :] * rot_ref[3 * FINE :, :]
        )

    lax.fori_loop(ZERO, FINE, angles, None)
    for i in range(T // STEP):
        r = slice(i * STEP, (i + ONE) * STEP)
        ahead[i].wait()
        if i == ZERO:
            for c in (ahead[4], *ahead[6:8]):
                c.wait()
        w = wide(x_ref[r, :])
        a = low(w * norm_scale(w))
        at_ref[:, r] = a.T
        cos, sin = cos_sin(table_ref[r, :])

        def turned(t):
            t = t.astype(bf16).astype(f32)
            return (t * cos + pltpu.roll(t, HALF, ONE) * sin).astype(bf16)

        q = dot(a, wq_ref[...])
        for h in range(HEADS):
            q_ref[h, r, :] = turned(q[:, h * HEAD : (h + ONE) * HEAD])
        k, v = dot(a, wk_ref[...]), dot(a, wv_ref[...]).astype(bf16)
        for g in range(KV):
            one = turned(k[:, g * HEAD : (g + ONE) * HEAD])
            k_ref[g, r, :] = one
            kt_ref[g, :, r] = one.T
            v_ref[g, r, :] = v[:, g * HEAD : (g + ONE) * HEAD]
            vt_ref[g, :HEAD, r] = v[:, g * HEAD : (g + ONE) * HEAD].T
    for g in range(KV):
        vt_ref[g, HEAD:, :] = jnp.ones((16, T), bf16)


    _mark("moments")
    packed[...] = jnp.zeros_like(packed)
    for k, ref in enumerate((three_in, nine_in)):
        pltpu.make_async_copy(ref, ref, s_in.at[len(ahead) + k]).wait()
    for half in (ZERO, ONE):
        for (name, t, n), u in zip(ORDER, STARTS):
            a = half * (m_hbm[INDEX[name]].shape[-ONE] // TWO) + t * LANES
            for k in (ZERO, ONE):
                if n == ONE:
                    at = places[name] + a
                    packed[half, SLOT[u], 3 * k : 3 * k + 3, :] = three_in[k, :, ZERO, at : at + LANES]
                else:
                    s = len(THREE) + 4 * t + TWO * k
                    packed[half, s] = nine_in[k, ZERO:8, ZERO, a : a + LANES]
                    packed[half, s + ONE, ZERO:ONE, :] = nine_in[k, 8:9, ZERO, a : a + LANES]
    moments[j] = packed[core]
    for k in BATCHES:
        for u in range(FILLED[k], PIECE[k] * NZ):
            cols[k][u] = jnp.zeros((ROWS, LANES), bf16)
    _mark("barrier")
    pl.semaphore_wait(barrier, len(peers))

    for r in range(ONE, COLUMN):
        to = lax.rem(j + r, COLUMN)
        copy(packed.at[lax.rem(to, TWO)], moments.at[j], s_mv, r_mv, column_start + to).start()
    their_moments = copy(moments.at[pl.ds(ZERO, COLUMN - ONE)], moments.at[pl.ds(ZERO, COLUMN - ONE)], s_mv, r_mv, partner)

    weights_s = (do_s, b_ref)
    _mark("f_att")
    for i in range(T // STEP):
        n = (i + ONE) * STEP
        r = slice(i * STEP, n)
        ok = causal(STEP)

        def heads(g):
            tops = []
            for k in range(GROUP):
                q = q_ref[g * GROUP + k, r, :]
                scores = [dot(k_ref[g, a : min(a + KEYS, n), :], q, ONE, ONE) for a in range(ZERO, n, KEYS)]
                last = scores[-ONE]
                own = jnp.where(ok, last[last.shape[ZERO] - STEP :, :], HIDDEN)
                scores[-ONE] = own if last.shape[ZERO] == STEP else jnp.concatenate([last[: last.shape[ZERO] - STEP, :], own], axis=ZERO)
                top = functools.reduce(jnp.maximum, [jnp.max(t, axis=ZERO, keepdims=True) for t in scores])
                for a, t in zip(range(ZERO, n, KEYS), scores):
                    weights_s[g][a : a + t.shape[ZERO], k * STEP : (k + ONE) * STEP] = low(jnp.exp2((t - top) * E))
                tops.append(top)
            out = dot(vt_ref[g, :, :n], weights_s[g][:n, :])
            for k, top in enumerate(tops):
                h, own = g * GROUP + k, slice(k * STEP, (k + ONE) * STEP)
                total = out[HEAD : HEAD + ONE, own]
                o = low(out[:HEAD, own] * (ONE / total))
                rows = slice(h * HEAD, (h + ONE) * HEAD)
                ot_ref[rows, r] = o
                o_s[r, rows] = o.T
                lse_ref[h, :, r] = top * E + jnp.log2(total)

        for g in range(KV):
            heads(g)

    _mark("f_wo")
    ahead[8].wait()
    for i in range(T // STEP):
        r = slice(i * STEP, (i + ONE) * STEP)
        out = dot(o_s[r, :], wo_ref[...]).astype(bf16)
        h = (x_ref[r, :].astype(f32) + out.astype(f32)).astype(bf16)
        h_ref[r, :] = h
        w = wide(h)
        b = low(w * norm_scale(w))
        b_ref[r, :] = b
        bt_ref[:, r] = b.T

    def d2d(u, n, slot, number):
        return copy(give.at[:, :, pl.ds(slot, n)], out_w.at[core, :, :, pl.ds(u, n)], s_give.at[slot], r_give.at[number], partner)

    def send_half(flow):
        d2d(flow.u, flow.n, flow.slot, flow.number).start()

    def half_sent(flow):
        d2d(flow.u, flow.n, flow.slot, flow.number).wait_send()

    def block(flow, k, a):
        units = pl.ds(flow.u, flow.n)
        return out_w.at[core, k, a, units] if flow.colour == ZERO else out_w.at[core, a, k, units]

    FIRST, LAST = pl.ds(ZERO, TWO), pl.ds(TWO, TWO)

    def hop(flow, i):
        axis, back = (flow.colour, ONE - flow.colour)[i // 6], i % TWO
        k = turns[axis][((TWO, TWO), (ONE, 3), (ONE, 3))[i % 6 // TWO][back]]
        s, r, to = s_hop.at[i // 6], (r_relay.at[i // 6, flow.number, back] if i % 6 < TWO else r_fin.at[i // 6, flow.number]), along[axis][back]
        u, n = flow.u, flow.n
        if i < 6:
            part = (FIRST, LAST, LAST, FIRST, FIRST, LAST)[i]
            dst = relay.at[back, :, pl.ds(u, n)] if i < TWO else fin.at[back, part, pl.ds(u, n)]
            return copy(block(flow, k, part), dst, s, r, to)
        half = n // TWO
        lo, hi = pl.ds(u, half), pl.ds(u + half, n - half)
        part = (lo, hi, hi, lo, lo, hi)[i - 6]
        return copy(fin.at[ZERO, k, part], (relay2 if i < 8 else fin2).at[back, part], s, r, to)

    def arrived(ref, sem):
        copy(ref, ref, s_rows, sem, partner).wait_recv()

    def gone(ref, sem):
        copy(ref, ref, sem, r_rows, partner).wait_send()

    def stage(flow, k, apart=False):
        u, n = flow.u, flow.n
        units = slice(u, u + n)
        first, second = turns[flow.colour], turns[ONE - flow.colour]
        if k == ZERO:
            d2d(u, n, ZERO, flow.number).wait_recv()

            def add(i, _):
                a, b = lax.div(i, NY), lax.rem(i, NY)
                out_w[core, a, b, units] = low(wide(out_w[core, a, b, units]) + wide(out_w[other, a, b, units]))

            lax.fori_loop(ZERO, PLANE, add, None)
            for i in range(TWO if apart else 4):
                hop(flow, i).start()
        elif k == ONE:
            for d in (ZERO, ONE):
                hop(flow, d).wait_recv()
                for a in range(TWO):
                    dst = block(flow, first[ONE + TWO * d], TWO * d + a)
                    dst[...] = low(wide(dst[...]) + wide(relay[d, a, units]))
                hop(flow, 4 + d).start()
        elif k == TWO:
            arrived(fin.at[:, :, pl.ds(u, n)], r_fin.at[ZERO, flow.number])

            def total(a, _):
                fin[ZERO, a, units] = low(wide(block(flow, first[ZERO], a)[...]) + wide(fin[ZERO, a, units]) + wide(fin[ONE, a, units]))

            lax.fori_loop(ZERO, 4, total, None)
            for i in range(4):
                hop(flow, 6 + i).start()
        elif k == 3:
            half = n // TWO
            for d, part in enumerate((slice(u, u + half), slice(u + half, u + n))):
                hop(flow, 6 + d).wait_recv()
                a = second[ONE + TWO * d]
                fin[ZERO, a, part] = low(wide(fin[ZERO, a, part]) + wide(relay2[d, part]))
                hop(flow, 10 + d).start()
        else:
            arrived(fin2.at[:, pl.ds(u, n)], r_fin.at[ONE, flow.number])
            cols[flow.batch][flow.base : flow.base + n] = low(wide(fin[ZERO, second[ZERO], units]) + wide(fin2[ZERO, units]) + wide(fin2[ONE, units]))

    def scatter(batch, k):
        n = PIECE[batch]
        return copy(cols[batch].at[pl.ds(above[k] * n, n)], zrs[batch].at[k - ONE], s_zr.at[batch], r_zr.at[batch], upward[k])

    def gather(batch, k):
        own = pl.ds(z * PIECE[batch], PIECE[batch])
        return copy(gcs[batch].at[own], gcs[batch].at[own], s_za.at[batch], r_za.at[batch], upward[k])

    OTHERS = range(ONE, NZ)

    def column(batch, step):
        if step == ZERO:
            for k in OTHERS:
                scatter(batch, k).start()
        elif step == ONE:
            arrived(zrs[batch], r_zr.at[batch])
            n = PIECE[batch]
            for i in range(n):
                total = wide(cols[batch][z * n + i])
                for k in range(NZ - ONE):
                    total += wide(zrs[batch][k, i])
                gcs[batch][z * n + i] = low(total)
            for k in OTHERS:
                gather(batch, k).start()
        else:
            arrived(gcs[batch].at[pl.ds(ZERO, len(OTHERS) * PIECE[batch])], r_za.at[batch])

    def spread_moments():
        their_moments.wait_recv()
        for name, n in (("w_gate", 9), ("wq", 3), ("w_up", 9), ("wo", 5)):
            u = START[name, ZERO]

            def move(i, _):
                for d in range(COLUMN):
                    m_nat[u + i, 3 * d : 3 * d + 3, :] = moments[d, SLOT[u] + i, ZERO:3, :]
                    v_nat[u + i, 3 * d : 3 * d + 3, :] = moments[d, SLOT[u] + i, 3:6, :]

            lax.fori_loop(ZERO, n, move, None)

        def move_down(t, _):
            for d in range(COLUMN):
                for k, nat in enumerate((m_down, v_down)):
                    s = len(THREE) + 4 * t + TWO * k
                    nat[t, 9 * d : 9 * d + 8, :] = moments[d, s]
                    nat[t, 9 * d + 8 : 9 * d + 9, :] = moments[d, s + ONE, ZERO:ONE, :]

        lax.fori_loop(ZERO, 3, move_down, None)

    def keep(r, u, slot):
        for k in range(PLANE):
            rows = slice(k * ROWS, (k + ONE) * ROWS)
            out_w[core, k // NY, k % NY, u] = low(r[rows, :LANES])
            give[k // NY, k % NY, slot] = low(r[rows, LANES:])

    def pair(ref, t):
        n = ref.shape[ONE]
        return jnp.concatenate([ref[:, lanes(core, t, n)], ref[:, lanes(other, t, n)]], axis=ONE)

    during = {}

    def when(i, *stages):
        during[i] = stages

    when(3, (GATES[ZERO], ZERO), (UPS[ZERO], ZERO))
    when(5, (GATES[ZERO], ONE), (UPS[ZERO], ONE))
    when(6, (GATES[ONE], ZERO), (UPS[ONE], ZERO))
    when(7, (GATES[ZERO], TWO), (UPS[ZERO], TWO))
    when(8, (GATES[ONE], ONE), (UPS[ONE], ONE), (GATES[ZERO], 3), (UPS[ZERO], 3))

    ahead[9].wait()
    db_s[...] = jnp.zeros_like(db_s)
    _mark("mlp")

    def step(i, _):
        slot = lax.rem(i, TWO)
        for k, ref in enumerate((wg_s, wu_s, wd_s)):
            pltpu.make_async_copy(ref.at[slot], ref.at[slot], s_w.at[slot, k]).wait()

        @pl.when(i + ONE < TILES)
        def _():
            for c in stream(i + ONE, ONE - slot):
                c.start()

        turn = lax.rem(i, 3)

        @pl.when(i >= 3)
        def _():
            for k in (ZERO, 3):
                d2d(ZERO, ONE, k + turn, ZERO).wait_send()

        wg, wu, wd = wg_s[slot], wu_s[slot], wd_s[slot]
        own_rows, other_rows = lanes(core, i, FF), lanes(other, i, FF)
        for c in range(TWO):
            r = slice(c * (T // TWO), (c + ONE) * (T // TWO))
            g, u = dot(b_ref[r, :], wg), dot(b_ref[r, :], wu)
            da = wide(low(dot(dy_ref[r, :], wd, ONE, ONE)))
            s = ONE / (ONE + jnp.exp(-g))
            silu = g * s
            act = low(silu * u).T
            act_s[own_rows, r] = act[:LANES]
            act_s[other_rows, r] = act[LANES:]
            du_s[r, :] = low(da * silu)
            dg_s[r, :] = low(da * u * (s + silu * (ONE - s)))
        for k, stages in during.items():

            @pl.when(i == k)
            def _(stages=stages):
                for flow, n in stages:
                    stage(flow, n)

        for ref, first, k in ((dg_s, START["w_gate", ZERO], ZERO), (du_s, START["w_up", ZERO], 3)):
            keep(dot(bt_ref[...], ref[...]), first + i, k + turn)
        db_s[...] += dot(dg_s[...], wg, ONE, ONE) + dot(du_s[...], wu, ONE, ONE)
        for first, k in ((START["w_gate", ZERO], ZERO), (START["w_up", ZERO], 3)):
            d2d(first + i, ONE, k + turn, k + lax.div(i, 3)).start()

    lax.fori_loop(ZERO, TILES, step, None)

    def down(flow, t, reused):
        for k in reused:
            d2d(ZERO, ONE, k, ZERO).wait_send()
        dy = pair(dy_ref, t)
        n = FF // NX

        for a in range(NX):
            r = dot(act_s[a * n : (a + ONE) * n, :], dy)
            for k in range(NY):
                for i in range(3):
                    rows = slice((3 * k + i) * ROWS, (3 * k + i + ONE) * ROWS)
                    out_w[core, a, k, flow.u + i] = low(r[rows, :LANES])
                    give[a, k, flow.slot + i] = low(r[rows, LANES:])
        send_half(flow)

    _mark("down0")
    down(DOWN0, ZERO, [])
    stage(GATES[ZERO], 4)
    stage(UPS[ZERO], 4)
    stage(GATES[TWO], ZERO)
    stage(UPS[TWO], ZERO)
    _mark("down1")
    down(DOWN1, ONE, [])
    stage(GATES[ONE], TWO)
    stage(UPS[ONE], TWO)
    _mark("down2")
    down(DOWN2, TWO, range(3))
    stage(DOWN0, ZERO)

    _mark("norm")
    for i in range(T // STEP):
        r = slice(i * STEP, (i + ONE) * STEP)
        w, db = wide(h_ref[r, :]), db_s[r, :]
        s = norm_scale(w)
        dh = low(wide(dy_ref[r, :]) + s * (db - w * (s * s * jnp.mean(db * w, axis=ONE, keepdims=True))))
        dh_s[r, :] = dh
        do = low(dot(dh, wo_ref[...], ONE, ONE))
        do_s[r, :] = do
        for h in range(HEADS):
            rows = slice(h * HEAD, (h + ONE) * HEAD)
            delta_s[h, :, r] = jnp.sum(wide(do[:, rows].T) * wide(ot_ref[rows, r]), axis=ZERO, keepdims=True)
        if i == ONE:
            stage(GATES[ONE], 3)
            stage(UPS[ONE], 3)
            stage(DOWN1, ZERO)
    stage(GATES[TWO], ONE)
    stage(UPS[TWO], ONE)

    _mark("wo")
    for k in range(3):
        d2d(ZERO, ONE, 3 + k, ZERO).wait_send()
    lax.fori_loop(ZERO, 3, lambda i, _: keep(dot(ot_ref[...], pair(dh_s, i)), WO.u + i, WO.slot + i), None)
    send_half(WO)
    stage(GATES[ONE], 4)
    stage(UPS[ONE], 4)
    column(ZERO, ZERO)
    stage(DOWN0, ONE)
    stage(DOWN2, ZERO)

    _mark("att")
    later = {
        (ZERO, ZERO): [],
        (ZERO, ONE): [(GATES[TWO], TWO), (UPS[TWO], TWO), (DOWN1, ONE), (WO, ZERO)],
        (ZERO, TWO): [],
        (ZERO, 3): [(GATES[TWO], 3), (UPS[TWO], 3), (DOWN0, TWO), (DOWN2, ONE)],
        (ONE, ZERO): [(DOWN1, TWO), (WO, ONE)],
        (ONE, ONE): [(ZERO, ONE), (GATES[TWO], 4), (UPS[TWO], 4), (DOWN0, 3)],
        (ONE, TWO): [(DOWN1, 3), (DOWN2, TWO)],
        (ONE, 3): [(DOWN0, 4), (DOWN1, 4), (ONE, ZERO), (WO, TWO)],
    }

    def group(g, _):
        for i in range(T // STEP):
            n = (i + ONE) * STEP
            r = slice(i * STEP, n)
            ok = causal(STEP)
            qs, dos = [], []
            for k in range(GROUP):
                h = g * GROUP + k
                q, do = q_ref[h, r, :], do_s[r, pl.ds(pl.multiple_of(h * HEAD, HEAD), HEAD)]
                qs.append(q)
                dos.append(do)
                to = slice(k * STEP, (k + ONE) * STEP)
                for a in range(ZERO, n, KEYS):
                    keys = slice(a, min(a + KEYS, n))
                    p = jnp.exp2(dot(k_ref[g, keys, :], q, ONE, ONE) * E - lse_ref[h, :, r])
                    if a + KEYS >= n:
                        own = jnp.where(ok, p[n - STEP - a :, :], 0.0)
                        p = own if n - STEP == a else jnp.concatenate([p[: n - STEP - a, :], own], axis=ZERO)
                    p_s[keys, to] = low(p)
                    ds_s[keys, to] = low(p * (dot(v_ref[g, keys, :], do, ONE, ONE) - delta_s[h, :, r]))
            dv = dot(p_s[:n, :], jnp.concatenate(dos, axis=ZERO))
            dk = dot(ds_s[:n, :], jnp.concatenate(qs, axis=ZERO))
            dq = dot(kt_ref[g, :, :n], ds_s[:n, :])
            cos, sin = cos_sin(table_ref[r, :])
            for k in range(GROUP):
                t = dq[:, k * STEP : (k + ONE) * STEP].T * SCALE
                dq_s[r, pl.ds(pl.multiple_of((g * GROUP + k) * HEAD, HEAD), HEAD)] = low(t * cos - pltpu.roll(t, HALF, ONE) * sin)
            if i == ZERO:
                dv_s[:n], dk_s[:n] = dv, dk
            else:
                dv_s[: n - STEP] += dv[: n - STEP]
                dk_s[: n - STEP] += dk[: n - STEP]
                dv_s[r], dk_s[r] = dv[n - STEP :], dk[n - STEP :]
            for which in (ZERO, ONE):
                if later[which, i]:

                    @pl.when(g == which)
                    def _():
                        for flow, m in later[which, i]:
                            if isinstance(flow, Flow):
                                stage(flow, m)
                            else:
                                column(flow, m)

        span = pl.ds(pl.multiple_of(g * HEAD, HEAD), HEAD)
        for i in range(T // STEP):
            r = slice(i * STEP, (i + ONE) * STEP)
            cos, sin = cos_sin(table_ref[r, :])
            t = dk_s[r, :] * SCALE
            dkv_s[ZERO][r, span] = low(t * cos - pltpu.roll(t, HALF, ONE) * sin)
            dkv_s[ONE][r, span] = low(dv_s[r, :])

    lax.fori_loop(ZERO, KV, group, None)

    _mark("qkv")
    half_sent(DOWN0)
    half_sent(DOWN1)
    lax.fori_loop(ZERO, 3, lambda i, _: keep(dot(at_ref[...], pair(dq_s, i)), WQ.u + i, WQ.slot + i), None)
    send_half(WQ)
    for i in (ZERO, ONE):
        keep(dot(at_ref[...], pair(dkv_s[i], ZERO)), WKV.u + i, WKV.slot + i)
    send_half(WKV)

    _mark("tail")
    stage(DOWN2, 3)
    stage(WO, 3)
    spread_moments()
    stage(WQ, ZERO, True)
    stage(WKV, ZERO, True)
    for flow in (WQ, WKV):
        hop(flow, TWO).start()
        hop(flow, 3).start()
    _mark("tail_1")
    stage(WQ, ONE)
    stage(WKV, ONE)
    stage(DOWN2, 4)
    stage(WO, 4)
    column(TWO, ZERO)
    column(ONE, ONE)
    _mark("tail_2")
    stage(WQ, TWO)
    stage(WKV, TWO)
    _mark("tail_3")
    stage(WQ, 3)
    stage(WKV, 3)
    column(TWO, ONE)
    _mark("tail_4")
    stage(WQ, 4)
    stage(WKV, 4)
    column(3, ZERO)
    _mark("tail_z0")
    column(ZERO, TWO)
    gone(out_w.at[core, pl.ds(ZERO, 3)], s_hop.at[ZERO])
    gone(out_w.at[core, ZERO, pl.ds(ZERO, 3)], s_hop.at[ONE])
    _mark("tail_z1")
    column(3, ONE)
    _mark("tail_z2")
    column(ONE, TWO)
    column(TWO, TWO)

    def squares(batch, total):
        def more(i, total):
            g = wide(gcs[batch][i])
            return total + (g * g).reshape(ROWS // 8, 8, LANES).sum(ZERO)

        return lax.fori_loop(ZERO, FILLED[batch], more, total)

    first_squares = functools.reduce(lambda total, batch: squares(batch, total), BATCHES[:-ONE], jnp.zeros((8, LANES), f32))
    _mark("tail_z3")
    column(3, TWO)
    for flow in (DOWN2, WO, WQ, WKV):
        half_sent(flow)
    for batch in BATCHES:
        gone(zrs[batch], s_zr.at[batch])
        gone(gcs[batch].at[pl.ds(ZERO, len(OTHERS) * PIECE[batch])], s_za.at[batch])
    their_moments.wait_send()

    _mark("norms")
    mine = norms.at[here * TWO + core]
    mine[...] = squares(BATCHES[-ONE], first_squares)
    for ab, first in plane.items():
        for c in (core, other):
            if any(ab) or c is other:
                copy(mine, mine, s_norm, r_norm, first + c).start()
    pltpu.make_async_copy(old, old, s_old).wait()
    all_norms = copy(norms.at[pl.ds(ZERO, TWO * PLANE - ONE)], norms.at[pl.ds(ZERO, TWO * PLANE - ONE)], s_norm, r_norm, partner)
    all_norms.wait_recv()
    total = norms[...].sum(axis=ZERO)
    total = jnp.sum(jnp.sum(total, axis=ZERO, keepdims=True), axis=ONE, keepdims=True)
    factor = jnp.minimum(1.0, 0.5 * lax.rsqrt(total * (1.0 / COUNT) + 1e-30))

    _mark("adam")

    def stepped(w, m, v, g):
        g = g * factor
        m = 0.9 * m + 0.1 * g
        v = 0.95 * v + 0.05 * g * g
        return low(w - 0.02 * (m * lax.rsqrt(v + 1e-8) + 0.1 * w))

    def new_units(name, t, n):
        u = START[name, t]
        batch, first = PLACE[u]

        def unit(i, _):
            if name == "w_down":
                rows = pl.ds(pl.multiple_of(i * ROWS, ROWS), ROWS)
                m, v = m_down[t, rows, :], v_down[t, rows, :]
            else:
                m, v = m_nat[u + i], v_nat[u + i]
            out_w[core, x, y, u + i] = stepped(wide(old[u + i]), m, v, wide(gcs[batch][first + i]))

        lax.fori_loop(ZERO, n, unit, None)

    for k, (name, t) in enumerate((name, t) for (name, t, n), u in zip(ORDER, STARTS) if UPRIGHT <= u < UPRIGHT + NZ):

        @pl.when(z == k)
        def _(name=name, t=t):
            new_units(name, t, ONE)

    def upright(k, part=pl.ds(ZERO, NX)):
        return out_w.at[core, part, :, pl.ds(UPRIGHT + above[k], ONE)]

    mine = out_w.at[core, x, y, pl.ds(UPRIGHT + z, ONE)]
    for ab, first in plane.items():
        if any(ab):
            copy(mine, mine, s_up.at[ZERO], r_up.at[ZERO], first + core).start()
    for name, t, n in RUNS:
        new_units(name, t, n)

    _mark("ag0")

    def slot(colour, ps, pb, h=None):
        u, n = COLOURS[colour]
        if h is not None:
            u, n = (u, n // TWO) if h == ZERO else (u + n // TWO, n - n // TWO)
        units = pl.ds(u, n)
        return out_w.at[core, pb, ps, units] if colour == ZERO else out_w.at[core, ps, pb, units]

    def give_partner(v):
        copy(v, v, s_core, r_core, partner).start()

    def to_partner(colour, ps, pb):
        give_partner(slot(colour, ps, pb))

    def send(colour, big, rel, ps, pb, h, d, kind):
        v = slot(colour, ps, pb, h)
        copy(v, v, s_ag.at[big], r_big.at[colour, rel, kind] if big else r_small.at[colour, kind], along[colour if big else ONE - colour][d]).start()

    def came(colour, big, rel, kind):
        units = pl.ds(*COLOURS[colour])
        arrived(out_w.at[core, pl.ds(ZERO, TWO), ZERO, units] if kind == ZERO else out_w.at[core, ZERO, ZERO, units], r_big.at[colour, rel, kind] if big else r_small.at[colour, kind])

    def spot(colour):
        return turns[ONE - colour], turns[colour]

    def big_own(colour, rel):
        ps, pb = spot(colour)
        for d in (ZERO, ONE):
            send(colour, ONE, rel, ps[rel], pb[ZERO], None, d, ZERO)

    def big_forward(colour, rel):
        ps, pb = spot(colour)
        came(colour, ONE, rel, ZERO)
        for d in (ZERO, ONE):
            send(colour, ONE, rel, ps[rel], pb[3 - TWO * d], d, d, ONE)
        for d in (ZERO, ONE):
            to_partner(colour, ps[rel], pb[3 - TWO * d])

    def big_far(colour, rel):
        ps, pb = spot(colour)
        came(colour, ONE, rel, ONE)
        to_partner(colour, ps[rel], pb[TWO])

    def rise(k):
        arrived(out_w.at[core, pl.ds(ZERO, 3), ZERO, pl.ds(ZERO, 5)] if k == ZERO else out_w.at[core, :, :, pl.ds(ZERO, TWO if k < 4 else ONE)], r_up.at[k])
        came_from = sorted({-k % NZ, k}, reverse=True)
        if k < 4:
            for d in (ZERO, ONE):
                v = upright(came_from[min(d, k)], pl.ds(ZERO, NX) if k < 3 else (FIRST, LAST)[d])
                copy(v, v, s_up.at[ONE], r_up.at[k + ONE], upward[(ONE, NZ - ONE)[d]]).start()
        for c in came_from:
            give_partner(upright(c))

    def small_own(colour):
        ps, pb = spot(colour)
        for d in (ZERO, ONE):
            send(colour, ZERO, ZERO, ps[ZERO], pb[ZERO], None, d, ZERO)

    def small_forward(colour):
        ps, pb = spot(colour)
        came(colour, ZERO, ZERO, ZERO)
        for d in (ZERO, ONE):
            send(colour, ZERO, ZERO, ps[3 - TWO * d], pb[ZERO], d, d, ONE)
        for rel in (3, ONE):
            big_own(colour, rel)
            to_partner(colour, ps[rel], pb[ZERO])

    def small_far(colour):
        ps, pb = spot(colour)
        came(colour, ZERO, ZERO, ONE)
        big_own(colour, TWO)
        to_partner(colour, ps[TWO], pb[ZERO])

    small_own(ZERO)
    small_own(ONE)
    for colour in (ZERO, ONE):
        ps, pb = spot(colour)
        big_own(colour, ZERO)
        to_partner(colour, ps[ZERO], pb[ZERO])

    _mark("rows")

    def picker(height, each, of):
        row, col = lax.broadcasted_iota(jnp.int32, (height, of), ZERO), lax.broadcasted_iota(jnp.int32, (height, of), ONE)
        half = height // TWO
        ours = (row < each) & (col == each * j + row)
        theirs = (row >= half) & (row < half + each) & (col == each * (j + ONE - TWO * core) + row - half)
        return (ours | theirs).astype(f32).astype(bf16)

    three, nine = picker(16, 3, ROWS), picker(32, 9, 3 * ROWS)
    for (name, t, n), u in zip(ORDER, STARTS):
        batch, a = PLACE[u]
        if n == ONE:
            rows = dot(three, gcs[batch][a]) * factor
            out_g[core, SLOT[u]], rows_out[SLOT[u]] = rows[:8], rows[8:]
        else:
            rows = dot(nine, gcs[batch][a : a + 3].reshape(3 * ROWS, LANES)) * factor
            s = len(THREE) + TWO * t
            for k in (ZERO, ONE):
                out_g[core, s + k], rows_out[s + k] = rows[8 * k : 8 * k + 8], rows[16 + 8 * k : 24 + 8 * k]
    own_rows = copy(rows_out, out_g.at[core], s_rows, r_rows, partner)
    own_rows.start()

    _mark("ag1")
    small_forward(ZERO)
    small_forward(ONE)
    rise(ZERO)
    _mark("ag2")
    big_forward(ZERO, ZERO)
    big_forward(ONE, ZERO)
    rise(ONE)
    small_far(ZERO)
    small_far(ONE)
    _mark("ag3")
    big_forward(ZERO, 3)
    big_forward(ONE, 3)
    rise(TWO)
    big_forward(ZERO, ONE)
    big_forward(ONE, ONE)
    big_far(ZERO, ZERO)
    big_far(ONE, ZERO)
    rise(3)
    own_rows.wait()
    for half in (ZERO, ONE):
        for (name, t, n), u in zip(ORDER, STARTS):
            a, s = half * (m_hbm[INDEX[name]].shape[-ONE] // TWO) + t * LANES, len(THREE) + TWO * t
            for s, r, rows in [(SLOT[u], ZERO, 3)] if n == ONE else [(s, ZERO, 8), (s + ONE, 8, ONE)]:
                old_ref, new_ref, at = (three_in, three_out, places[name] + a) if n == ONE else (nine_in, nine_out, a)
                g = out_g[half, s, ZERO:rows, :]
                here = (slice(r, r + rows), ZERO, slice(at, at + LANES))
                new_ref[(ZERO, *here)] = 0.9 * old_ref[(ZERO, *here)] + 0.1 * g
                new_ref[(ONE, *here)] = 0.95 * old_ref[(ONE, *here)] + 0.05 * g * g
    _mark("ag4")
    big_forward(ZERO, TWO)
    big_forward(ONE, TWO)
    for rel in (3, ONE):
        big_far(ZERO, rel)
        big_far(ONE, rel)
    rise(4)
    _mark("ag5")
    big_far(ZERO, TWO)
    big_far(ONE, TWO)
    arrived(out_w.at[other], r_core)
    gone(out_w.at[core], s_core)
    shared = pl.ds(ZERO, UNITS - NZ)
    gone(out_w.at[core, ZERO, pl.ds(ZERO, 3), shared], s_ag.at[ZERO])
    gone(out_w.at[core, pl.ds(ZERO, 3), :, shared], s_ag.at[ONE])
    gone(out_w.at[core, pl.ds(ZERO, 3), ZERO, pl.ds(ZERO, 5)], s_up.at[ZERO])
    gone(out_w.at[core, :, :, pl.ds(ZERO, 7)], s_up.at[ONE])
    all_norms.wait_send()
    _mark("end")


def layer_step(x, dy, weights, m, v):
    view = lambda t: t.reshape(NX, NY, t.shape[ZERO] // (PLANE * ROWS), ROWS, t.shape[ONE])
    any_ = pl.BlockSpec(memory_space=pl.ANY)
    vmem = pl.BlockSpec(memory_space=pltpu.VMEM)
    low, wide = lambda *s: pltpu.VMEM(s, bf16), lambda *s: pltpu.VMEM(s, f32)
    unit = lambda *lead: low(*lead, ROWS, LANES)
    dma = lambda *shape: pltpu.SemaphoreType.DMA(shape)
    flows = len(FLOWS)
    moments = wide(TWO, 3, ONE, sum(t.shape[-ONE] for t in m[:-ONE])), wide(TWO, 9, ONE, D)
    scratch = [
        wide(4 * FINE, HEAD), wide(T, HEAD), low(D, D), low(T, D), low(D, T), low(HEADS, T, HEAD), low(KV, T, HEAD), low(KV, T, HEAD), low(KV, HEAD, T), low(KV, HEAD + 16, T),
        low(D, T), wide(HEADS, ONE, T), low(T, D), low(T, D), low(D, T),
        low(TWO, D, STEP), low(TWO, D, STEP), low(TWO, STEP, D), low(T, STEP), low(T, STEP),
        low(FF, T), wide(T, D), low(T, D), low(T, D), wide(HEADS, ONE, T),
        unit(NX, NY, GIVE), unit(TWO, TWO, UNITS), unit(TWO, 4, UNITS), unit(TWO, UNITS), unit(TWO, UNITS),
        *(unit(NZ * p) for p in PIECE), *(unit(NZ - ONE, p) for p in PIECE), *(unit(NZ * p) for p in PIECE),
        unit(UNITS), *moments, wide(TWO, SLOTS, 8, LANES), wide(COLUMN, SLOTS, 8, LANES),
        wide(UNITS, ROWS, LANES), wide(UNITS, ROWS, LANES), wide(3, 3 * ROWS, LANES), wide(3, 3 * ROWS, LANES),
        wide(TWO * PLANE, 8, LANES), wide(ROW_SLOTS, 8, LANES), wide(TWO, ROW_SLOTS, 8, LANES),
        dma(12), dma(TWO, 3), dma(), dma(GIVE), dma(flows), dma(TWO), dma(TWO, flows, TWO), dma(TWO, flows), *[dma(len(BATCHES))] * 4, dma(), dma(), dma(), dma(),
        dma(TWO), dma(TWO, TWO), dma(TWO, 4, TWO), dma(TWO), dma(5), dma(), dma(), dma(), dma(),
    ]
    return pl.pallas_call(
        _step,
        in_specs=[any_] * 31,
        out_specs=[vmem] * 3,
        out_shape=[unit(TWO, NX, NY, UNITS), *moments],
        scratch_shapes=scratch,
        compiler_params=pltpu.CompilerParams(collective_id=ZERO, has_side_effects=True, vmem_limit_bytes=50 * TWO**20),
        name="step",
    )(x, dy, jnp.asarray(rotary()), *weights, *map(view, weights), *m, *v)


def _finish(w_ref, three_ref, nine_ref, *refs):
    w_out, moments_out, sem = refs[:7], (refs[7:14], refs[14:21]), refs[21]
    copies = []
    for half in (ZERO, ONE):
        for i, (name, t, n) in enumerate(ORDER):
            o = w_out[INDEX[name]]
            a = half * (o.shape[-ONE] // TWO) + t * LANES
            copies.append(pltpu.make_async_copy(w_ref.at[half, :, :, pl.ds(STARTS[i], n)], o.at[:, :, :, :, pl.ds(a, LANES)], sem.at[ZERO]))
    for k in (ZERO, ONE):
        lane = ZERO
        for name, o in zip(NAMES, moments_out[k]):
            if name == "w_down":
                copies.append(pltpu.make_async_copy(nine_ref.at[k], o, sem.at[TWO]))
            else:
                copies.append(pltpu.make_async_copy(three_ref.at[k, :, :, pl.ds(lane, o.shape[-ONE])], o, sem.at[ONE]))
                lane += o.shape[-ONE]
    for c in copies:
        c.start()
    for k, ref in enumerate((w_ref, three_ref, nine_ref)):
        pltpu.make_async_copy(ref, ref, sem.at[k]).wait()


def finish(new, m, v, like):
    any_ = pl.BlockSpec(memory_space=pl.ANY)
    vmem = pl.BlockSpec(memory_space=pltpu.VMEM)
    view = lambda t: (NX, NY, t.shape[ZERO] // (PLANE * ROWS), ROWS, t.shape[ONE])
    out = pl.pallas_call(
        _finish,
        in_specs=[vmem] * 3,
        out_specs=[any_] * 21,
        out_shape=[jax.ShapeDtypeStruct(view(w), w.dtype) for w in like] + [jax.ShapeDtypeStruct(t.shape, t.dtype) for t in (*m, *v)],
        scratch_shapes=[pltpu.SemaphoreType.DMA((3,))],
        compiler_params=pltpu.CompilerParams(vmem_limit_bytes=16 * TWO**20),
        name="finish",
    )(*new)
    return [o.reshape(ONE, *w.shape) for o, w in zip(out[:7], like)], out[7:14], out[14:]


def solution(mesh):
    def step(x, dy, *arrays):
        weights, m, v = (arrays[i : i + 7] for i in (ZERO, 7, 14))
        weights = [w[ZERO] for w in weights]
        m, v = ([t.transpose(ONE, ZERO, TWO) for t in s] for s in (m, v))
        w, m, v = finish(layer_step(x[ZERO], dy[ZERO], weights, m, v), m, v, weights)
        return (*w, *(t.transpose(ONE, ZERO, TWO) for t in (*m, *v)))

    states, all_of, cut = P(("rep", "dp"), None, None), P(None, None, None), P(None, "dp", None)
    return jax.shard_map(
        step,
        mesh=mesh,
        in_specs=(states, states) + (all_of,) * 7 + (cut,) * 14,
        out_specs=(P("rep", None, None),) * 7 + (P("rep", "dp", None),) * 14,
        check_vma=False,
    )
```

```python
import functools

import jax
import jax.numpy as jnp
import numpy as np
from jax import lax
from jax.experimental import pallas as pl
from jax.experimental.pallas import tpu as pltpu
from jax.sharding import PartitionSpec as P

HIDDEN = -2e30
LOG2E = 1.4426950408889634
HEAD = 128
THETA = 10000
ZERO, ONE, TWO = range(3)
NAMES = ("wq", "wk", "wv", "wo", "w_gate", "w_up", "w_down")
T, D, HEADS, KV, GROUP = 1024, 768, 6, TWO, 3
STEP = 256
SCALE = HEAD**-0.5
E = SCALE * LOG2E
HALF = HEAD // TWO
FINE = 32
bf16, f32 = jnp.bfloat16, jnp.float32


def dot(a, b, ca=ONE, cb=ZERO):
    return lax.dot_general(a, b, (((ca,), (cb,)), ((), ())), preferred_element_type=f32)


def rotary():
    rate = float(THETA) ** (-np.arange(HALF) / HALF)
    (c, s), (d, e) = ([fn(np.arange(FINE)[:, None] * step * rate) for fn in (np.cos, np.sin)] for step in (FINE, ONE))
    return np.concatenate([np.concatenate(pair, axis=ONE) for pair in ((c, s), (s, c), (d, d), (-e, e))]).astype(np.float32)


def cos_sin(table):
    swapped = pltpu.roll(table, HALF, ONE)
    first = lax.broadcasted_iota(jnp.int32, table.shape, ONE) < HALF
    return jnp.where(first, table, swapped), jnp.where(first, -swapped, table)


def norm_scale(wide):
    return lax.rsqrt(jnp.mean(wide * wide, axis=ONE, keepdims=True) + 1e-6)


def causal(n):
    key = lax.broadcasted_iota(jnp.int32, (n, STEP), ZERO)
    return lax.broadcasted_iota(jnp.int32, (n, STEP), ONE) + (n - STEP) >= key


NX, NY, NZ = 4, 4, 8
PLANE = NX * NY
COLUMN = TWO * NZ
ROWS = 3 * COLUMN
LANES = 128
FF = 2304
TILES = FF // STEP
COUNT = 6881280
_run = lambda name, tiles: [(name, t, ONE) for t in range(tiles)]
ORDER = [("w_down", ZERO, 3), ("w_down", TWO, 3), *_run("w_gate", 9), *_run("wq", 3), *_run("w_up", 9), *_run("wo", 3), *_run("wk", ONE), *_run("wv", ONE), ("w_down", ONE, 3)]
STARTS = [sum(n for _, _, n in ORDER[:i]) for i in range(len(ORDER))]
UNITS = sum(n for _, _, n in ORDER)
START = {(name, t): u for (name, t, _), u in zip(ORDER, STARTS)}
SPLIT = START["w_up", ZERO]
UPRIGHT = 14
COLOURS = ((ZERO, UPRIGHT), (UPRIGHT + NZ, UNITS - UPRIGHT - NZ))
INDEX = {name: i for i, name in enumerate(NAMES)}
MESH = pl.DeviceIdType.MESH
THREE = [u for (_, _, n), u in zip(ORDER, STARTS) if n == ONE]
SLOT = {u: s for s, u in enumerate(THREE)}
SLOTS = len(THREE) + 4 * 3
ROW_SLOTS = len(THREE) + TWO * 3


class Flow:
    def __init__(self, number, name, t, n, batch, base, slot):
        self.number, self.u, self.n, self.batch, self.base, self.slot = number, START[name, t], n, batch, base, slot
        self.colour = int(self.u >= SPLIT)


FLOWS, _filled = [], [ZERO] * 4
for _name, _t, _n, _batch, _slot in (
    *(("w_gate", t, 3, t // 6, ZERO) for t in (ZERO, 3, 6)),
    *(("w_up", t, 3, t // 6, 3) for t in (ZERO, 3, 6)),
    ("w_down", ZERO, 3, ONE, 6), ("w_down", ONE, 3, ONE, 9), ("w_down", TWO, 3, TWO, ZERO), ("wo", ZERO, 3, TWO, 3), ("wq", ZERO, 3, 3, 6), ("wk", ZERO, TWO, 3, 9),
):
    FLOWS.append(Flow(len(FLOWS), _name, _t, _n, _batch, _filled[_batch], _slot))
    _filled[_batch] += _n
GATES, UPS, (DOWN0, DOWN1, DOWN2, WO, WQ, WKV) = FLOWS[:3], FLOWS[3:6], FLOWS[6:]
FILLED = tuple(_filled)
BATCHES = range(len(FILLED))
PART = 3
PIECE = [-(-n * PART // NZ) for n in FILLED]
PLACE = {f.u + i: (f.batch, f.base + i) for f in FLOWS for i in range(f.n)}
RUNS = []
for (_name, _t, _n), _u in zip(ORDER, STARTS):
    if UPRIGHT <= _u < UPRIGHT + NZ:
        continue
    _name0, _t0, _n0 = RUNS[-ONE] if RUNS else ("", ZERO, ZERO)
    if _n == ONE and _name == _name0 and _t == _t0 + _n0 and PLACE[_u][ZERO] == PLACE[_u - ONE][ZERO]:
        RUNS[-ONE] = (_name0, _t0, _n0 + ONE)
    else:
        RUNS.append((_name, _t, _n))
KEYS = 512
GIVE = 12


def _mark(name):
    pass


def _step(*refs):
    it = iter(refs)
    take = lambda n: [next(it) for _ in range(n)]
    x_hbm, dy_hbm, table_hbm, wq_hbm, wk_hbm, wv_hbm, wo_hbm, wg_hbm, wu_hbm, wd_hbm = take(10)
    weights, m_hbm, v_hbm = take(7), take(7), take(7)
    out_w, three_out, nine_out = take(3)
    rot_ref, table_ref, wo_ref, dy_ref, at_ref, q_ref, k_ref, v_ref, kt_ref, vt_ref, ot_ref, lse_ref, h_ref, b_ref, bt_ref = take(15)
    wg_s, wu_s, wd_s, dg_s, du_s, act_s, db_s, dh_s, do_s, delta_s = take(10)
    give, relay, fin, relay2, fin2 = take(5)
    cols, zrs, gcs = (take(len(BATCHES)) for _ in range(3))
    old, three_in, nine_in, packed, moments, m_nat, v_nat, m_down, v_down, norms, rows_out, out_g = take(12)
    s_in, s_w, s_old, s_give, r_give, s_hop, r_relay, r_fin, s_zr, r_zr, s_za, r_za, s_norm, r_norm, s_mv, r_mv, s_ag, r_small, r_big, s_up, r_up, s_core, r_core, s_rows, r_rows = take(25)
    x_ref, wq_ref, wk_ref, wv_ref, o_s = act_s.at[:T, :D], act_s.at[T : T + D, :D], act_s.at[:D, D:], act_s.at[D : TWO * D, D:], dh_s
    dq_s, p_s, ds_s = dh_s, act_s.at[:T, :D], act_s.at[T : TWO * T, :D]
    dk_s, dv_s, dkv_s = db_s.at[:, :HEAD], db_s.at[:, HEAD : TWO * HEAD], (dg_s, du_s)

    me = lax.axis_index("dp")
    core, j, here, y, x = lax.rem(me, TWO), lax.rem(me, COLUMN), lax.div(me, COLUMN), lax.rem(lax.div(me, COLUMN), NY), lax.div(me, COLUMN * NY)
    z, other = lax.div(j, TWO), ONE - core
    turns = [[p, *(lax.rem(p + d, NX) for d in range(ONE, NX))] for p in (x, y)]
    above = [z, *(lax.rem(z + k, NZ) for k in range(ONE, NZ))]
    column_start = here * COLUMN
    plane = {(a, b): (turns[ZERO][a] * NY + turns[ONE][b]) * COLUMN + z * TWO for a in range(NX) for b in range(NY)}
    along = [[plane[d, ZERO] + core for d in (ONE, 3)], [plane[ZERO, d] + core for d in (ONE, 3)]]
    upward = [column_start + k * TWO + core for k in above]
    partner = column_start + z * TWO + other

    def copy(src, dst, s, r, to):
        return pltpu.make_async_remote_copy(src_ref=src, dst_ref=dst, send_sem=s, recv_sem=r, device_id={"dp": to}, device_id_type=MESH)

    def lanes(half, t, width):
        return pl.ds(pl.multiple_of(half * (width // TWO) + t * LANES, LANES), LANES)

    wide = lambda v: v.astype(f32)
    low = lambda v: v.astype(bf16)

    _mark("start")

    def stream(i, slot):
        out = []
        for k, half in enumerate((core, other)):
            span, to = lanes(half, i, FF), pl.ds(k * LANES, LANES)
            for n, (src, dst) in enumerate(((wg_hbm.at[:, span], wg_s.at[slot, :, to]), (wu_hbm.at[:, span], wu_s.at[slot, :, to]), (wd_hbm.at[span, :], wd_s.at[slot, to, :]))):
                out.append(pltpu.make_async_copy(src, dst, s_w.at[slot, n]))
        return out

    ahead = [pltpu.make_async_copy(x_hbm.at[r, :], x_ref.at[r, :], s_in.at[i]) for i, r in enumerate(pl.ds(k * STEP, STEP) for k in range(T // STEP))]
    for src, dst in ((wq_hbm, wq_ref), (table_hbm, rot_ref), (wk_hbm, wk_ref), (wv_hbm, wv_ref), (wo_hbm, wo_ref), (dy_hbm, dy_ref)):
        ahead.append(pltpu.make_async_copy(src, dst, s_in.at[len(ahead)]))
    for c in (ahead[5], ahead[ZERO], ahead[4], *ahead[6:8], *ahead[ONE:4], *ahead[8:]):
        c.start()
    places = {}
    for k, ref in enumerate((m_hbm, v_hbm)):
        lane = ZERO
        for name in NAMES:
            src = ref[INDEX[name]]
            if name == "w_down":
                dst, sem = nine_in.at[k], len(ahead) + ONE
            else:
                dst, sem = three_in.at[k, :, :, pl.ds(lane, src.shape[-ONE])], len(ahead)
                places[name] = lane
                lane += src.shape[-ONE]
            pltpu.make_async_copy(src, dst, s_in.at[sem]).start()
    for c in stream(ZERO, ZERO):
        c.start()
    for (name, t, n), u in zip(ORDER, STARTS):
        w = weights[INDEX[name]]
        pltpu.make_async_copy(w.at[x, y, :, :, lanes(core, t, w.shape[-ONE])], old.at[pl.ds(u, n)], s_old).start()

    barrier = pltpu.get_barrier_semaphore()
    peers = [column_start + k * TWO + c for k in above[ONE:] for c in (ZERO, ONE)]
    peers += [first + c for ab, first in plane.items() if any(ab) for c in (ZERO, ONE)]
    peers += [partner]
    for to in peers:
        pl.semaphore_signal(barrier, inc=ONE, device_id={"dp": to}, device_id_type=MESH)

    _mark("front")
    ahead[5].wait()

    def angles(i, _):
        table_ref[pl.ds(pl.multiple_of(i * FINE, FINE), FINE), :] = (
            rot_ref[pl.ds(i, ONE), :] * rot_ref[TWO * FINE : 3 * FINE, :] + rot_ref[pl.ds(FINE + i, ONE), :] * rot_ref[3 * FINE :, :]
        )

    lax.fori_loop(ZERO, FINE, angles, None)
    for i in range(T // STEP):
        r = slice(i * STEP, (i + ONE) * STEP)
        ahead[i].wait()
        if i == ZERO:
            for c in (ahead[4], *ahead[6:8]):
                c.wait()
        w = wide(x_ref[r, :])
        a = low(w * norm_scale(w))
        at_ref[:, r] = a.T
        cos, sin = cos_sin(table_ref[r, :])

        def turned(t):
            t = t.astype(bf16).astype(f32)
            return (t * cos + pltpu.roll(t, HALF, ONE) * sin).astype(bf16)

        q = dot(a, wq_ref[...])
        for h in range(HEADS):
            q_ref[h, r, :] = turned(q[:, h * HEAD : (h + ONE) * HEAD])
        k, v = dot(a, wk_ref[...]), dot(a, wv_ref[...]).astype(bf16)
        for g in range(KV):
            one = turned(k[:, g * HEAD : (g + ONE) * HEAD])
            k_ref[g, r, :] = one
            kt_ref[g, :, r] = one.T
            v_ref[g, r, :] = v[:, g * HEAD : (g + ONE) * HEAD]
            vt_ref[g, :HEAD, r] = v[:, g * HEAD : (g + ONE) * HEAD].T
    for g in range(KV):
        vt_ref[g, HEAD:, :] = jnp.ones((16, T), bf16)


    _mark("moments")
    packed[...] = jnp.zeros_like(packed)
    for k, ref in enumerate((three_in, nine_in)):
        pltpu.make_async_copy(ref, ref, s_in.at[len(ahead) + k]).wait()
    for half in (ZERO, ONE):
        for (name, t, n), u in zip(ORDER, STARTS):
            a = half * (m_hbm[INDEX[name]].shape[-ONE] // TWO) + t * LANES
            for k in (ZERO, ONE):
                if n == ONE:
                    at = places[name] + a
                    packed[half, SLOT[u], 3 * k : 3 * k + 3, :] = three_in[k, :, ZERO, at : at + LANES]
                else:
                    s = len(THREE) + 4 * t + TWO * k
                    packed[half, s] = nine_in[k, ZERO:8, ZERO, a : a + LANES]
                    packed[half, s + ONE, ZERO:ONE, :] = nine_in[k, 8:9, ZERO, a : a + LANES]
    moments[j] = packed[core]
    for k in BATCHES:
        for u in range(FILLED[k] * PART, PIECE[k] * NZ):
            cols[k][u] = jnp.zeros((ROWS // PART, LANES), bf16)
    _mark("barrier")
    pl.semaphore_wait(barrier, len(peers))

    for r in range(ONE, COLUMN):
        to = lax.rem(j + r, COLUMN)
        copy(packed.at[lax.rem(to, TWO)], moments.at[j], s_mv, r_mv, column_start + to).start()
    their_moments = copy(moments.at[pl.ds(ZERO, COLUMN - ONE)], moments.at[pl.ds(ZERO, COLUMN - ONE)], s_mv, r_mv, partner)

    weights_s = (do_s, b_ref)
    _mark("f_att")
    for i in range(T // STEP):
        n = (i + ONE) * STEP
        r = slice(i * STEP, n)
        ok = causal(STEP)

        def heads(g):
            tops = []
            for k in range(GROUP):
                q = q_ref[g * GROUP + k, r, :]
                scores = [dot(k_ref[g, a : min(a + KEYS, n), :], q, ONE, ONE) for a in range(ZERO, n, KEYS)]
                last = scores[-ONE]
                own = jnp.where(ok, last[last.shape[ZERO] - STEP :, :], HIDDEN)
                scores[-ONE] = own if last.shape[ZERO] == STEP else jnp.concatenate([last[: last.shape[ZERO] - STEP, :], own], axis=ZERO)
                top = functools.reduce(jnp.maximum, [jnp.max(t, axis=ZERO, keepdims=True) for t in scores])
                for a, t in zip(range(ZERO, n, KEYS), scores):
                    weights_s[g][a : a + t.shape[ZERO], k * STEP : (k + ONE) * STEP] = low(jnp.exp2((t - top) * E))
                tops.append(top)
            out = dot(vt_ref[g, :, :n], weights_s[g][:n, :])
            for k, top in enumerate(tops):
                h, own = g * GROUP + k, slice(k * STEP, (k + ONE) * STEP)
                total = out[HEAD : HEAD + ONE, own]
                o = low(out[:HEAD, own] * (ONE / total))
                rows = slice(h * HEAD, (h + ONE) * HEAD)
                ot_ref[rows, r] = o
                o_s[r, rows] = o.T
                lse_ref[h, :, r] = top * E + jnp.log2(total)

        for g in range(KV):
            heads(g)

    _mark("f_wo")
    ahead[8].wait()
    for i in range(T // STEP):
        r = slice(i * STEP, (i + ONE) * STEP)
        out = dot(o_s[r, :], wo_ref[...]).astype(bf16)
        h = (x_ref[r, :].astype(f32) + out.astype(f32)).astype(bf16)
        h_ref[r, :] = h
        w = wide(h)
        b = low(w * norm_scale(w))
        b_ref[r, :] = b
        bt_ref[:, r] = b.T

    def d2d(u, n, slot, number):
        return copy(give.at[:, :, pl.ds(slot, n)], out_w.at[core, :, :, pl.ds(u, n)], s_give.at[slot], r_give.at[number], partner)

    def send_half(flow):
        d2d(flow.u, flow.n, flow.slot, flow.number).start()

    def half_sent(flow):
        d2d(flow.u, flow.n, flow.slot, flow.number).wait_send()

    def block(flow, k, a):
        units = pl.ds(flow.u, flow.n)
        return out_w.at[core, k, a, units] if flow.colour == ZERO else out_w.at[core, a, k, units]

    FIRST, LAST = pl.ds(ZERO, TWO), pl.ds(TWO, TWO)

    def hop(flow, i):
        axis, back = (flow.colour, ONE - flow.colour)[i // 6], i % TWO
        k = turns[axis][((TWO, TWO), (ONE, 3), (ONE, 3))[i % 6 // TWO][back]]
        s, r, to = s_hop.at[i // 6], (r_relay.at[i // 6, flow.number, back] if i % 6 < TWO else r_fin.at[i // 6, flow.number]), along[axis][back]
        u, n = flow.u, flow.n
        if i < 6:
            part = (FIRST, LAST, LAST, FIRST, FIRST, LAST)[i]
            dst = relay.at[back, :, pl.ds(u, n)] if i < TWO else fin.at[back, part, pl.ds(u, n)]
            return copy(block(flow, k, part), dst, s, r, to)
        half = n // TWO
        lo, hi = pl.ds(u, half), pl.ds(u + half, n - half)
        part = (lo, hi, hi, lo, lo, hi)[i - 6]
        return copy(fin.at[ZERO, k, part], (relay2 if i < 8 else fin2).at[back, part], s, r, to)

    def summed(batch, i):
        return gcs[batch][pl.ds(i * PART, PART)].reshape(ROWS, LANES)

    def arrived(ref, sem):
        copy(ref, ref, s_rows, sem, partner).wait_recv()

    def gone(ref, sem):
        copy(ref, ref, sem, r_rows, partner).wait_send()

    def stage(flow, k, apart=False):
        u, n = flow.u, flow.n
        units = slice(u, u + n)
        first, second = turns[flow.colour], turns[ONE - flow.colour]
        if k == ZERO:
            d2d(u, n, ZERO, flow.number).wait_recv()

            def add(i, _):
                a, b = lax.div(i, NY), lax.rem(i, NY)
                out_w[core, a, b, units] = low(wide(out_w[core, a, b, units]) + wide(out_w[other, a, b, units]))

            lax.fori_loop(ZERO, PLANE, add, None)
            for i in range(TWO if apart else 4):
                hop(flow, i).start()
        elif k == ONE:
            for d in (ZERO, ONE):
                hop(flow, d).wait_recv()
                for a in range(TWO):
                    dst = block(flow, first[ONE + TWO * d], TWO * d + a)
                    dst[...] = low(wide(dst[...]) + wide(relay[d, a, units]))
                hop(flow, 4 + d).start()
        elif k == TWO:
            arrived(fin.at[:, :, pl.ds(u, n)], r_fin.at[ZERO, flow.number])

            def total(a, _):
                fin[ZERO, a, units] = low(wide(block(flow, first[ZERO], a)[...]) + wide(fin[ZERO, a, units]) + wide(fin[ONE, a, units]))

            lax.fori_loop(ZERO, 4, total, None)
            for i in range(4):
                hop(flow, 6 + i).start()
        elif k == 3:
            half = n // TWO
            for d, part in enumerate((slice(u, u + half), slice(u + half, u + n))):
                hop(flow, 6 + d).wait_recv()
                a = second[ONE + TWO * d]
                fin[ZERO, a, part] = low(wide(fin[ZERO, a, part]) + wide(relay2[d, part]))
                hop(flow, 10 + d).start()
        else:
            arrived(fin2.at[:, pl.ds(u, n)], r_fin.at[ONE, flow.number])
            rows = low(wide(fin[ZERO, second[ZERO], units]) + wide(fin2[ZERO, units]) + wide(fin2[ONE, units]))
            cols[flow.batch][flow.base * PART : (flow.base + n) * PART] = rows.reshape(n * PART, ROWS // PART, LANES)

    def scatter(batch, k):
        n = PIECE[batch]
        return copy(cols[batch].at[pl.ds(above[k] * n, n)], zrs[batch].at[k - ONE], s_zr.at[batch], r_zr.at[batch], upward[k])

    def gather(batch, k):
        own = pl.ds(z * PIECE[batch], PIECE[batch])
        return copy(gcs[batch].at[own], gcs[batch].at[own], s_za.at[batch], r_za.at[batch], upward[k])

    OTHERS = range(ONE, NZ)

    def column(batch, step):
        if step == ZERO:
            for k in OTHERS:
                scatter(batch, k).start()
        elif step == ONE:
            arrived(zrs[batch], r_zr.at[batch])
            n = PIECE[batch]
            for i in range(n):
                total = wide(cols[batch][z * n + i])
                for k in range(NZ - ONE):
                    total += wide(zrs[batch][k, i])
                gcs[batch][z * n + i] = low(total)
            for k in OTHERS:
                gather(batch, k).start()
        else:
            arrived(gcs[batch].at[pl.ds(ZERO, len(OTHERS) * PIECE[batch])], r_za.at[batch])

    def spread_moments():
        their_moments.wait_recv()
        for name, n in (("w_gate", 9), ("wq", 3), ("w_up", 9), ("wo", 5)):
            u = START[name, ZERO]

            def move(i, _):
                for d in range(COLUMN):
                    m_nat[u + i, 3 * d : 3 * d + 3, :] = moments[d, SLOT[u] + i, ZERO:3, :]
                    v_nat[u + i, 3 * d : 3 * d + 3, :] = moments[d, SLOT[u] + i, 3:6, :]

            lax.fori_loop(ZERO, n, move, None)

        def move_down(t, _):
            for d in range(COLUMN):
                for k, nat in enumerate((m_down, v_down)):
                    s = len(THREE) + 4 * t + TWO * k
                    nat[t, 9 * d : 9 * d + 8, :] = moments[d, s]
                    nat[t, 9 * d + 8 : 9 * d + 9, :] = moments[d, s + ONE, ZERO:ONE, :]

        lax.fori_loop(ZERO, 3, move_down, None)

    def keep(r, u, slot):
        for k in range(PLANE):
            rows = slice(k * ROWS, (k + ONE) * ROWS)
            out_w[core, k // NY, k % NY, u] = low(r[rows, :LANES])
            give[k // NY, k % NY, slot] = low(r[rows, LANES:])

    def pair(ref, t):
        n = ref.shape[ONE]
        return jnp.concatenate([ref[:, lanes(core, t, n)], ref[:, lanes(other, t, n)]], axis=ONE)

    during = {}

    def when(i, *stages):
        during[i] = stages

    when(3, (GATES[ZERO], ZERO), (UPS[ZERO], ZERO))
    when(5, (GATES[ZERO], ONE), (UPS[ZERO], ONE))
    when(6, (GATES[ONE], ZERO), (UPS[ONE], ZERO))
    when(7, (GATES[ZERO], TWO), (UPS[ZERO], TWO))
    when(8, (GATES[ONE], ONE), (UPS[ONE], ONE), (GATES[ZERO], 3), (UPS[ZERO], 3))

    ahead[9].wait()
    db_s[...] = jnp.zeros_like(db_s)
    _mark("mlp")

    def step(i, _):
        slot = lax.rem(i, TWO)
        for k, ref in enumerate((wg_s, wu_s, wd_s)):
            pltpu.make_async_copy(ref.at[slot], ref.at[slot], s_w.at[slot, k]).wait()

        @pl.when(i + ONE < TILES)
        def _():
            for c in stream(i + ONE, ONE - slot):
                c.start()

        turn = lax.rem(i, 3)

        @pl.when(i >= 3)
        def _():
            for k in (ZERO, 3):
                d2d(ZERO, ONE, k + turn, ZERO).wait_send()

        wg, wu, wd = wg_s[slot], wu_s[slot], wd_s[slot]
        own_rows, other_rows = lanes(core, i, FF), lanes(other, i, FF)
        for c in range(TWO):
            r = slice(c * (T // TWO), (c + ONE) * (T // TWO))
            g, u = dot(b_ref[r, :], wg), dot(b_ref[r, :], wu)
            da = wide(low(dot(dy_ref[r, :], wd, ONE, ONE)))
            s = ONE / (ONE + jnp.exp(-g))
            silu = g * s
            act = low(silu * u).T
            act_s[own_rows, r] = act[:LANES]
            act_s[other_rows, r] = act[LANES:]
            du_s[r, :] = low(da * silu)
            dg_s[r, :] = low(da * u * (s + silu * (ONE - s)))
        for k, stages in during.items():

            @pl.when(i == k)
            def _(stages=stages):
                for flow, n in stages:
                    stage(flow, n)

        for ref, first, k in ((dg_s, START["w_gate", ZERO], ZERO), (du_s, START["w_up", ZERO], 3)):
            keep(dot(bt_ref[...], ref[...]), first + i, k + turn)
        db_s[...] += dot(dg_s[...], wg, ONE, ONE) + dot(du_s[...], wu, ONE, ONE)
        for first, k in ((START["w_gate", ZERO], ZERO), (START["w_up", ZERO], 3)):
            d2d(first + i, ONE, k + turn, k + lax.div(i, 3)).start()

    lax.fori_loop(ZERO, TILES, step, None)

    def down(flow, t, reused):
        for k in reused:
            d2d(ZERO, ONE, k, ZERO).wait_send()
        dy = pair(dy_ref, t)
        n = FF // NX

        for a in range(NX):
            r = dot(act_s[a * n : (a + ONE) * n, :], dy)
            for k in range(NY):
                for i in range(3):
                    rows = slice((3 * k + i) * ROWS, (3 * k + i + ONE) * ROWS)
                    out_w[core, a, k, flow.u + i] = low(r[rows, :LANES])
                    give[a, k, flow.slot + i] = low(r[rows, LANES:])
        send_half(flow)

    _mark("down0")
    down(DOWN0, ZERO, [])
    stage(GATES[TWO], ZERO)
    stage(UPS[TWO], ZERO)
    _mark("down1")
    down(DOWN1, ONE, [])
    stage(GATES[ZERO], 4)
    stage(UPS[ZERO], 4)
    stage(GATES[ONE], TWO)
    stage(UPS[ONE], TWO)
    _mark("down2")
    down(DOWN2, TWO, range(3))
    stage(DOWN0, ZERO)

    _mark("norm")
    for i in range(T // STEP):
        r = slice(i * STEP, (i + ONE) * STEP)
        w, db = wide(h_ref[r, :]), db_s[r, :]
        s = norm_scale(w)
        dh = low(wide(dy_ref[r, :]) + s * (db - w * (s * s * jnp.mean(db * w, axis=ONE, keepdims=True))))
        dh_s[r, :] = dh
        do = low(dot(dh, wo_ref[...], ONE, ONE))
        do_s[r, :] = do
        for h in range(HEADS):
            rows = slice(h * HEAD, (h + ONE) * HEAD)
            delta_s[h, :, r] = jnp.sum(wide(do[:, rows].T) * wide(ot_ref[rows, r]), axis=ZERO, keepdims=True)
        if i == ONE:
            stage(GATES[ONE], 3)
            stage(UPS[ONE], 3)
            stage(DOWN1, ZERO)
    stage(GATES[TWO], ONE)
    stage(UPS[TWO], ONE)

    _mark("wo")
    for k in range(3):
        d2d(ZERO, ONE, 3 + k, ZERO).wait_send()
    for i in range(3):
        keep(dot(ot_ref[...], pair(dh_s, i)), WO.u + i, WO.slot + i)
    send_half(WO)
    stage(GATES[ONE], 4)
    stage(UPS[ONE], 4)
    column(ZERO, ZERO)
    stage(DOWN0, ONE)
    stage(DOWN2, ZERO)

    _mark("att")
    later = {
        (ZERO, ZERO): [],
        (ZERO, ONE): [(GATES[TWO], TWO), (UPS[TWO], TWO), (DOWN1, ONE), (WO, ZERO)],
        (ZERO, TWO): [],
        (ZERO, 3): [(GATES[TWO], 3), (UPS[TWO], 3), (DOWN0, TWO), (DOWN2, ONE)],
        (ONE, ZERO): [(DOWN1, TWO), (WO, ONE)],
        (ONE, ONE): [(ZERO, ONE), (GATES[TWO], 4), (UPS[TWO], 4), (DOWN0, 3)],
        (ONE, TWO): [(DOWN1, 3), (DOWN2, TWO)],
        (ONE, 3): [(DOWN0, 4), (WO, TWO)],
    }

    def group(g, _):
        for i in range(T // STEP):
            n = (i + ONE) * STEP
            r = slice(i * STEP, n)
            ok = causal(STEP)
            qs, dos = [], []
            for k in range(GROUP):
                h = g * GROUP + k
                q, do = q_ref[h, r, :], do_s[r, pl.ds(pl.multiple_of(h * HEAD, HEAD), HEAD)]
                qs.append(q)
                dos.append(do)
                to = slice(k * STEP, (k + ONE) * STEP)
                for a in range(ZERO, n, KEYS):
                    keys = slice(a, min(a + KEYS, n))
                    p = jnp.exp2(dot(k_ref[g, keys, :], q, ONE, ONE) * E - lse_ref[h, :, r])
                    if a + KEYS >= n:
                        own = jnp.where(ok, p[n - STEP - a :, :], 0.0)
                        p = own if n - STEP == a else jnp.concatenate([p[: n - STEP - a, :], own], axis=ZERO)
                    p_s[keys, to] = low(p)
                    ds_s[keys, to] = low(p * (dot(v_ref[g, keys, :], do, ONE, ONE) - delta_s[h, :, r]))
            dv = dot(p_s[:n, :], jnp.concatenate(dos, axis=ZERO))
            dk = dot(ds_s[:n, :], jnp.concatenate(qs, axis=ZERO))
            dq = dot(kt_ref[g, :, :n], ds_s[:n, :])
            cos, sin = cos_sin(table_ref[r, :])
            for k in range(GROUP):
                t = dq[:, k * STEP : (k + ONE) * STEP].T * SCALE
                dq_s[r, pl.ds(pl.multiple_of((g * GROUP + k) * HEAD, HEAD), HEAD)] = low(t * cos - pltpu.roll(t, HALF, ONE) * sin)
            if i == ZERO:
                dv_s[:n], dk_s[:n] = dv, dk
            else:
                dv_s[: n - STEP] += dv[: n - STEP]
                dk_s[: n - STEP] += dk[: n - STEP]
                dv_s[r], dk_s[r] = dv[n - STEP :], dk[n - STEP :]
            for which in (ZERO, ONE):
                if later[which, i]:

                    @pl.when(g == which)
                    def _():
                        for flow, m in later[which, i]:
                            if isinstance(flow, Flow):
                                stage(flow, m)
                            else:
                                column(flow, m)

        span = pl.ds(pl.multiple_of(g * HEAD, HEAD), HEAD)
        for i in range(T // STEP):
            r = slice(i * STEP, (i + ONE) * STEP)
            cos, sin = cos_sin(table_ref[r, :])
            t = dk_s[r, :] * SCALE
            dkv_s[ZERO][r, span] = low(t * cos - pltpu.roll(t, HALF, ONE) * sin)
            dkv_s[ONE][r, span] = low(dv_s[r, :])

    lax.fori_loop(ZERO, KV, group, None)

    _mark("qkv")
    half_sent(DOWN0)
    half_sent(DOWN1)
    for i in range(3):
        keep(dot(at_ref[...], pair(dq_s, i)), WQ.u + i, WQ.slot + i)
    send_half(WQ)
    for i in (ZERO, ONE):
        keep(dot(at_ref[...], pair(dkv_s[i], ZERO)), WKV.u + i, WKV.slot + i)
    send_half(WKV)

    _mark("tail")
    stage(DOWN1, 4)
    column(ONE, ZERO)
    stage(DOWN2, 3)
    stage(WO, 3)
    spread_moments()
    stage(WQ, ZERO, True)
    stage(WKV, ZERO, True)
    for flow in (WQ, WKV):
        hop(flow, TWO).start()
        hop(flow, 3).start()
    _mark("tail_1")
    stage(WQ, ONE)
    stage(WKV, ONE)
    stage(DOWN2, 4)
    stage(WO, 4)
    column(TWO, ZERO)
    column(ONE, ONE)
    _mark("tail_2")
    stage(WQ, TWO)
    stage(WKV, TWO)
    _mark("tail_3")
    stage(WQ, 3)
    stage(WKV, 3)
    column(TWO, ONE)
    _mark("tail_4")
    stage(WQ, 4)
    stage(WKV, 4)
    column(3, ZERO)
    _mark("tail_z0")
    column(ZERO, TWO)
    gone(out_w.at[core, pl.ds(ZERO, 3)], s_hop.at[ZERO])
    gone(out_w.at[core, ZERO, pl.ds(ZERO, 3)], s_hop.at[ONE])
    _mark("tail_z1")
    column(3, ONE)
    _mark("tail_z2")
    column(ONE, TWO)
    column(TWO, TWO)

    def squares(batch, total):
        def more(i, total):
            g = wide(summed(batch, i))
            return total + (g * g).reshape(ROWS // 8, 8, LANES).sum(ZERO)

        return lax.fori_loop(ZERO, FILLED[batch], more, total)

    first_squares = functools.reduce(lambda total, batch: squares(batch, total), BATCHES[:-ONE], jnp.zeros((8, LANES), f32))
    _mark("tail_z3")
    column(3, TWO)
    for flow in (DOWN2, WO, WQ, WKV):
        half_sent(flow)
    for batch in BATCHES:
        gone(zrs[batch], s_zr.at[batch])
        gone(gcs[batch].at[pl.ds(ZERO, len(OTHERS) * PIECE[batch])], s_za.at[batch])
    their_moments.wait_send()

    _mark("norms")
    mine = norms.at[here * TWO + core]
    mine[...] = jnp.sum(squares(BATCHES[-ONE], first_squares), axis=ZERO, keepdims=True)
    for ab, first in plane.items():
        for c in (core, other):
            if any(ab) or c is other:
                copy(mine, mine, s_norm, r_norm, first + c).start()
    pltpu.make_async_copy(old, old, s_old).wait()
    all_norms = copy(norms.at[pl.ds(ZERO, TWO * PLANE - ONE)], norms.at[pl.ds(ZERO, TWO * PLANE - ONE)], s_norm, r_norm, partner)
    all_norms.wait_recv()
    total = norms[...].sum(axis=ZERO)
    total = jnp.sum(total, axis=ONE, keepdims=True)
    factor = jnp.minimum(1.0, 0.5 * lax.rsqrt(total * (1.0 / COUNT) + 1e-30))

    _mark("adam")

    def stepped(w, m, v, g):
        g = g * factor
        m = 0.9 * m + 0.1 * g
        v = 0.95 * v + 0.05 * g * g
        return low(w - 0.02 * (m * lax.rsqrt(v + 1e-8) + 0.1 * w))

    def new_units(name, t, n):
        u = START[name, t]
        batch, first = PLACE[u]

        def unit(i, _):
            if name == "w_down":
                rows = pl.ds(pl.multiple_of(i * ROWS, ROWS), ROWS)
                m, v = m_down[t, rows, :], v_down[t, rows, :]
            else:
                m, v = m_nat[u + i], v_nat[u + i]
            out_w[core, x, y, u + i] = stepped(wide(old[u + i]), m, v, wide(summed(batch, first + i)))

        lax.fori_loop(ZERO, n, unit, None)

    for k, (name, t) in enumerate((name, t) for (name, t, n), u in zip(ORDER, STARTS) if UPRIGHT <= u < UPRIGHT + NZ):

        @pl.when(z == k)
        def _(name=name, t=t):
            new_units(name, t, ONE)

    def upright(k, part=pl.ds(ZERO, NX)):
        return out_w.at[core, part, :, pl.ds(UPRIGHT + above[k], ONE)]

    mine = out_w.at[core, x, y, pl.ds(UPRIGHT + z, ONE)]
    for ab, first in plane.items():
        if any(ab):
            copy(mine, mine, s_up.at[ZERO], r_up.at[ZERO], first + core).start()
    for name, t, n in RUNS:
        new_units(name, t, n)

    _mark("ag0")

    def slot(colour, ps, pb, h=None):
        u, n = COLOURS[colour]
        if h is not None:
            u, n = (u, n // TWO) if h == ZERO else (u + n // TWO, n - n // TWO)
        units = pl.ds(u, n)
        return out_w.at[core, pb, ps, units] if colour == ZERO else out_w.at[core, ps, pb, units]

    def give_partner(v):
        copy(v, v, s_core, r_core, partner).start()

    def to_partner(colour, ps, pb):
        give_partner(slot(colour, ps, pb))

    def send(colour, big, rel, ps, pb, h, d, kind):
        v = slot(colour, ps, pb, h)
        copy(v, v, s_ag.at[big], r_big.at[colour, rel, kind] if big else r_small.at[colour, kind], along[colour if big else ONE - colour][d]).start()

    def came(colour, big, rel, kind):
        units = pl.ds(*COLOURS[colour])
        arrived(out_w.at[core, pl.ds(ZERO, TWO), ZERO, units] if kind == ZERO else out_w.at[core, ZERO, ZERO, units], r_big.at[colour, rel, kind] if big else r_small.at[colour, kind])

    def spot(colour):
        return turns[ONE - colour], turns[colour]

    def big_own(colour, rel):
        ps, pb = spot(colour)
        for d in (ZERO, ONE):
            send(colour, ONE, rel, ps[rel], pb[ZERO], None, d, ZERO)

    def big_forward(colour, rel):
        ps, pb = spot(colour)
        came(colour, ONE, rel, ZERO)
        for d in (ZERO, ONE):
            send(colour, ONE, rel, ps[rel], pb[3 - TWO * d], d, d, ONE)
        for d in (ZERO, ONE):
            to_partner(colour, ps[rel], pb[3 - TWO * d])

    def big_far(colour, rel):
        ps, pb = spot(colour)
        came(colour, ONE, rel, ONE)
        to_partner(colour, ps[rel], pb[TWO])

    def rise(k):
        arrived(out_w.at[core, pl.ds(ZERO, 3), ZERO, pl.ds(ZERO, 5)] if k == ZERO else out_w.at[core, :, :, pl.ds(ZERO, TWO if k < 4 else ONE)], r_up.at[k])
        came_from = sorted({-k % NZ, k}, reverse=True)
        if k < 4:
            for d in (ZERO, ONE):
                v = upright(came_from[min(d, k)], pl.ds(ZERO, NX) if k < 3 else (FIRST, LAST)[d])
                copy(v, v, s_up.at[ONE], r_up.at[k + ONE], upward[(ONE, NZ - ONE)[d]]).start()
        for c in came_from:
            give_partner(upright(c))

    def small_own(colour):
        ps, pb = spot(colour)
        for d in (ZERO, ONE):
            send(colour, ZERO, ZERO, ps[ZERO], pb[ZERO], None, d, ZERO)

    def small_forward(colour):
        ps, pb = spot(colour)
        came(colour, ZERO, ZERO, ZERO)
        for d in (ZERO, ONE):
            send(colour, ZERO, ZERO, ps[3 - TWO * d], pb[ZERO], d, d, ONE)
        for rel in (3, ONE):
            big_own(colour, rel)
            to_partner(colour, ps[rel], pb[ZERO])

    def small_far(colour):
        ps, pb = spot(colour)
        came(colour, ZERO, ZERO, ONE)
        big_own(colour, TWO)
        to_partner(colour, ps[TWO], pb[ZERO])

    small_own(ZERO)
    small_own(ONE)
    for colour in (ZERO, ONE):
        ps, pb = spot(colour)
        big_own(colour, ZERO)
        to_partner(colour, ps[ZERO], pb[ZERO])

    _mark("rows")

    def picker(height, each, of):
        row, col = lax.broadcasted_iota(jnp.int32, (height, of), ZERO), lax.broadcasted_iota(jnp.int32, (height, of), ONE)
        half = height // TWO
        ours = (row < each) & (col == each * j + row)
        theirs = (row >= half) & (row < half + each) & (col == each * (j + ONE - TWO * core) + row - half)
        return (ours | theirs).astype(f32).astype(bf16)

    three, nine = picker(16, 3, ROWS), picker(32, 9, 3 * ROWS)
    for (name, t, n), u in zip(ORDER, STARTS):
        batch, a = PLACE[u]
        if n == ONE:
            rows = dot(three, summed(batch, a)) * factor
            out_g[core, SLOT[u]], rows_out[SLOT[u]] = rows[:8], rows[8:]
        else:
            rows = dot(nine, jnp.concatenate([summed(batch, a + i) for i in range(3)], axis=ZERO)) * factor
            s = len(THREE) + TWO * t
            for k in (ZERO, ONE):
                out_g[core, s + k], rows_out[s + k] = rows[8 * k : 8 * k + 8], rows[16 + 8 * k : 24 + 8 * k]
    own_rows = copy(rows_out, out_g.at[core], s_rows, r_rows, partner)
    own_rows.start()

    _mark("ag1")
    small_forward(ZERO)
    small_forward(ONE)
    rise(ZERO)
    _mark("ag2")
    big_forward(ZERO, ZERO)
    big_forward(ONE, ZERO)
    rise(ONE)
    small_far(ZERO)
    small_far(ONE)
    _mark("ag3")
    big_forward(ZERO, 3)
    big_forward(ONE, 3)
    rise(TWO)
    big_forward(ZERO, ONE)
    big_forward(ONE, ONE)
    big_far(ZERO, ZERO)
    big_far(ONE, ZERO)
    rise(3)
    own_rows.wait()
    for half in (ZERO, ONE):
        for (name, t, n), u in zip(ORDER, STARTS):
            a, s = half * (m_hbm[INDEX[name]].shape[-ONE] // TWO) + t * LANES, len(THREE) + TWO * t
            for s, r, rows in [(SLOT[u], ZERO, 3)] if n == ONE else [(s, ZERO, 8), (s + ONE, 8, ONE)]:
                old_ref, new_ref, at = (three_in, three_out, places[name] + a) if n == ONE else (nine_in, nine_out, a)
                g = out_g[half, s, ZERO:rows, :]
                here = (slice(r, r + rows), ZERO, slice(at, at + LANES))
                new_ref[(ZERO, *here)] = 0.9 * old_ref[(ZERO, *here)] + 0.1 * g
                new_ref[(ONE, *here)] = 0.95 * old_ref[(ONE, *here)] + 0.05 * g * g
    _mark("ag4")
    big_forward(ZERO, TWO)
    big_forward(ONE, TWO)
    for rel in (3, ONE):
        big_far(ZERO, rel)
        big_far(ONE, rel)
    rise(4)
    _mark("ag5")
    big_far(ZERO, TWO)
    big_far(ONE, TWO)
    arrived(out_w.at[other], r_core)
    gone(out_w.at[core], s_core)
    shared = pl.ds(ZERO, UNITS - NZ)
    gone(out_w.at[core, ZERO, pl.ds(ZERO, 3), shared], s_ag.at[ZERO])
    gone(out_w.at[core, pl.ds(ZERO, 3), :, shared], s_ag.at[ONE])
    gone(out_w.at[core, pl.ds(ZERO, 3), ZERO, pl.ds(ZERO, 5)], s_up.at[ZERO])
    gone(out_w.at[core, :, :, pl.ds(ZERO, 7)], s_up.at[ONE])
    all_norms.wait_send()
    _mark("end")


def layer_step(x, dy, weights, m, v):
    view = lambda t: t.reshape(NX, NY, t.shape[ZERO] // (PLANE * ROWS), ROWS, t.shape[ONE])
    any_ = pl.BlockSpec(memory_space=pl.ANY)
    vmem = pl.BlockSpec(memory_space=pltpu.VMEM)
    low, wide = lambda *s: pltpu.VMEM(s, bf16), lambda *s: pltpu.VMEM(s, f32)
    unit = lambda *lead: low(*lead, ROWS, LANES)
    dma = lambda *shape: pltpu.SemaphoreType.DMA(shape)
    flows = len(FLOWS)
    moments = wide(TWO, 3, ONE, sum(t.shape[-ONE] for t in m[:-ONE])), wide(TWO, 9, ONE, D)
    scratch = [
        wide(4 * FINE, HEAD), wide(T, HEAD), low(D, D), low(T, D), low(D, T), low(HEADS, T, HEAD), low(KV, T, HEAD), low(KV, T, HEAD), low(KV, HEAD, T), low(KV, HEAD + 16, T),
        low(D, T), wide(HEADS, ONE, T), low(T, D), low(T, D), low(D, T),
        low(TWO, D, STEP), low(TWO, D, STEP), low(TWO, STEP, D), low(T, STEP), low(T, STEP),
        low(FF, T), wide(T, D), low(T, D), low(T, D), wide(HEADS, ONE, T),
        unit(NX, NY, GIVE), unit(TWO, TWO, UNITS), unit(TWO, 4, UNITS), unit(TWO, UNITS), unit(TWO, UNITS),
        *(low(*lead(p), ROWS // PART, LANES) for lead in (lambda p: (NZ * p,), lambda p: (NZ - ONE, p), lambda p: (NZ * p,)) for p in PIECE),
        unit(UNITS), *moments, wide(TWO, SLOTS, 8, LANES), wide(COLUMN, SLOTS, 8, LANES),
        wide(UNITS, ROWS, LANES), wide(UNITS, ROWS, LANES), wide(3, 3 * ROWS, LANES), wide(3, 3 * ROWS, LANES),
        wide(TWO * PLANE, ONE, LANES), wide(ROW_SLOTS, 8, LANES), wide(TWO, ROW_SLOTS, 8, LANES),
        dma(12), dma(TWO, 3), dma(), dma(GIVE), dma(flows), dma(TWO), dma(TWO, flows, TWO), dma(TWO, flows), *[dma(len(BATCHES))] * 4, dma(), dma(), dma(), dma(),
        dma(TWO), dma(TWO, TWO), dma(TWO, 4, TWO), dma(TWO), dma(5), dma(), dma(), dma(), dma(),
    ]
    return pl.pallas_call(
        _step,
        in_specs=[any_] * 31,
        out_specs=[vmem] * 3,
        out_shape=[unit(TWO, NX, NY, UNITS), *moments],
        scratch_shapes=scratch,
        compiler_params=pltpu.CompilerParams(collective_id=ZERO, has_side_effects=True, vmem_limit_bytes=50 * TWO**20),
        name="step",
    )(x, dy, jnp.asarray(rotary()), *weights, *map(view, weights), *m, *v)


def _finish(w_ref, three_ref, nine_ref, *refs):
    w_out, moments_out, sem = refs[:7], (refs[7:14], refs[14:21]), refs[21]
    copies = []
    for half in (ZERO, ONE):
        for i, (name, t, n) in enumerate(ORDER):
            o = w_out[INDEX[name]]
            a = half * (o.shape[-ONE] // TWO) + t * LANES
            copies.append(pltpu.make_async_copy(w_ref.at[half, :, :, pl.ds(STARTS[i], n)], o.at[:, :, :, :, pl.ds(a, LANES)], sem.at[ZERO]))
    for k in (ZERO, ONE):
        lane = ZERO
        for name, o in zip(NAMES, moments_out[k]):
            if name == "w_down":
                copies.append(pltpu.make_async_copy(nine_ref.at[k], o, sem.at[TWO]))
            else:
                copies.append(pltpu.make_async_copy(three_ref.at[k, :, :, pl.ds(lane, o.shape[-ONE])], o, sem.at[ONE]))
                lane += o.shape[-ONE]
    for c in copies:
        c.start()
    for k, ref in enumerate((w_ref, three_ref, nine_ref)):
        pltpu.make_async_copy(ref, ref, sem.at[k]).wait()


def finish(new, m, v, like):
    any_ = pl.BlockSpec(memory_space=pl.ANY)
    vmem = pl.BlockSpec(memory_space=pltpu.VMEM)
    view = lambda t: (NX, NY, t.shape[ZERO] // (PLANE * ROWS), ROWS, t.shape[ONE])
    out = pl.pallas_call(
        _finish,
        in_specs=[vmem] * 3,
        out_specs=[any_] * 21,
        out_shape=[jax.ShapeDtypeStruct(view(w), w.dtype) for w in like] + [jax.ShapeDtypeStruct(t.shape, t.dtype) for t in (*m, *v)],
        scratch_shapes=[pltpu.SemaphoreType.DMA((3,))],
        compiler_params=pltpu.CompilerParams(vmem_limit_bytes=16 * TWO**20),
        name="finish",
    )(*new)
    return [o.reshape(ONE, *w.shape) for o, w in zip(out[:7], like)], out[7:14], out[14:]


def solution(mesh):
    def step(x, dy, *arrays):
        weights, m, v = (arrays[i : i + 7] for i in (ZERO, 7, 14))
        weights = [w[ZERO] for w in weights]
        m, v = ([t.transpose(ONE, ZERO, TWO) for t in s] for s in (m, v))
        w, m, v = finish(layer_step(x[ZERO], dy[ZERO], weights, m, v), m, v, weights)
        return (*w, *(t.transpose(ONE, ZERO, TWO) for t in (*m, *v)))

    states, all_of, cut = P(("rep", "dp"), None, None), P(None, None, None), P(None, "dp", None)
    return jax.shard_map(
        step,
        mesh=mesh,
        in_specs=(states, states) + (all_of,) * 7 + (cut,) * 14,
        out_specs=(P("rep", None, None),) * 7 + (P("rep", "dp", None),) * 14,
        check_vma=False,
    )
```

```python
import functools

import jax
import jax.numpy as jnp
import numpy as np
from jax import lax
from jax.experimental import pallas as pl
from jax.experimental.pallas import tpu as pltpu
from jax.sharding import PartitionSpec as P

HIDDEN = -2e30
LOG2E = 1.4426950408889634
HEAD = 128
THETA = 10000
ZERO, ONE, TWO = range(3)
NAMES = ("wq", "wk", "wv", "wo", "w_gate", "w_up", "w_down")
T, D, HEADS, KV, GROUP = 1024, 768, 6, TWO, 3
STEP = 256
SCALE = HEAD**-0.5
E = SCALE * LOG2E
HALF = HEAD // TWO
FINE = 32
bf16, f32 = jnp.bfloat16, jnp.float32


def dot(a, b, ca=ONE, cb=ZERO):
    return lax.dot_general(a, b, (((ca,), (cb,)), ((), ())), preferred_element_type=f32)


def rotary():
    rate = float(THETA) ** (-np.arange(HALF) / HALF)
    (c, s), (d, e) = ([fn(np.arange(FINE)[:, None] * step * rate) for fn in (np.cos, np.sin)] for step in (FINE, ONE))
    return np.concatenate([np.concatenate(pair, axis=ONE) for pair in ((c, s), (s, c), (d, d), (-e, e))]).astype(np.float32)


def cos_sin(table):
    swapped = pltpu.roll(table, HALF, ONE)
    first = lax.broadcasted_iota(jnp.int32, table.shape, ONE) < HALF
    return jnp.where(first, table, swapped), jnp.where(first, -swapped, table)


def norm_scale(wide):
    return lax.rsqrt(jnp.mean(wide * wide, axis=ONE, keepdims=True) + 1e-6)


def causal(n):
    key = lax.broadcasted_iota(jnp.int32, (n, STEP), ZERO)
    return lax.broadcasted_iota(jnp.int32, (n, STEP), ONE) + (n - STEP) >= key


NX, NY, NZ = 4, 4, 8
PLANE = NX * NY
COLUMN = TWO * NZ
ROWS = 3 * COLUMN
LANES = 128
FF = 2304
TILES = FF // STEP
COUNT = 6881280
_run = lambda name, tiles: [(name, t, ONE) for t in range(tiles)]
ORDER = [("w_down", ZERO, 3), ("w_down", TWO, 3), *_run("w_gate", 9), *_run("wq", 3), *_run("w_up", 9), *_run("wo", 3), *_run("wk", ONE), *_run("wv", ONE), ("w_down", ONE, 3)]
STARTS = [sum(n for _, _, n in ORDER[:i]) for i in range(len(ORDER))]
UNITS = sum(n for _, _, n in ORDER)
START = {(name, t): u for (name, t, _), u in zip(ORDER, STARTS)}
SPLIT = START["w_up", ZERO]
UPRIGHT = 14
COLOURS = ((ZERO, UPRIGHT), (UPRIGHT + NZ, UNITS - UPRIGHT - NZ))
INDEX = {name: i for i, name in enumerate(NAMES)}
MESH = pl.DeviceIdType.MESH
THREE = [u for (_, _, n), u in zip(ORDER, STARTS) if n == ONE]
SLOT = {u: s for s, u in enumerate(THREE)}
SLOTS = len(THREE) + 4 * 3
ROW_SLOTS = len(THREE) + TWO * 3


class Flow:
    def __init__(self, number, name, t, n, batch, base, slot):
        self.number, self.u, self.n, self.batch, self.base, self.slot = number, START[name, t], n, batch, base, slot
        self.colour = int(self.u >= SPLIT)


FLOWS, _filled = [], [ZERO] * 4
for _name, _t, _n, _batch, _slot in (
    *(("w_gate", t, 3, t // 6, ZERO) for t in (ZERO, 3, 6)),
    *(("w_up", t, 3, t // 6, 3) for t in (ZERO, 3, 6)),
    ("w_down", ZERO, 3, ONE, 6), ("w_down", ONE, 3, ONE, 9), ("w_down", TWO, 3, TWO, ZERO), ("wo", ZERO, 3, TWO, 3), ("wq", ZERO, 3, 3, 6), ("wk", ZERO, TWO, 3, 9),
):
    FLOWS.append(Flow(len(FLOWS), _name, _t, _n, _batch, _filled[_batch], _slot))
    _filled[_batch] += _n
GATES, UPS, (DOWN0, DOWN1, DOWN2, WO, WQ, WKV) = FLOWS[:3], FLOWS[3:6], FLOWS[6:]
FILLED = tuple(_filled)
BATCHES = range(len(FILLED))
PART = 3
PIECE = [-(-n * PART // NZ) for n in FILLED]
PLACE = {f.u + i: (f.batch, f.base + i) for f in FLOWS for i in range(f.n)}
RUNS = []
for (_name, _t, _n), _u in zip(ORDER, STARTS):
    if UPRIGHT <= _u < UPRIGHT + NZ:
        continue
    _name0, _t0, _n0 = RUNS[-ONE] if RUNS else ("", ZERO, ZERO)
    if _n == ONE and _name == _name0 and _t == _t0 + _n0 and PLACE[_u][ZERO] == PLACE[_u - ONE][ZERO]:
        RUNS[-ONE] = (_name0, _t0, _n0 + ONE)
    else:
        RUNS.append((_name, _t, _n))
KEYS = 512
GIVE = 12


def _mark(name):
    pass


def _step(*refs):
    it = iter(refs)
    take = lambda n: [next(it) for _ in range(n)]
    x_hbm, dy_hbm, table_hbm, wq_hbm, wk_hbm, wv_hbm, wo_hbm, wg_hbm, wu_hbm, wd_hbm = take(10)
    weights, m_hbm, v_hbm = take(7), take(7), take(7)
    out_w, three_out, nine_out = take(3)
    rot_ref, table_ref, wo_ref, dy_ref, at_ref, q_ref, k_ref, v_ref, kt_ref, vt_ref, ot_ref, lse_ref, h_ref, b_ref, bt_ref = take(15)
    wg_s, wu_s, wd_s, dg_s, du_s, act_s, db_s, dh_s, do_s, delta_s = take(10)
    give, relay, fin, relay2, fin2 = take(5)
    cols, zrs, gcs = (take(len(BATCHES)) for _ in range(3))
    old, three_in, nine_in, packed, moments, m_nat, v_nat, m_down, v_down, norms, rows_out, out_g = take(12)
    s_in, s_w, s_old, s_give, r_give, s_hop, r_relay, r_fin, s_zr, r_zr, s_za, r_za, s_norm, r_norm, s_mv, r_mv, s_ag, r_small, r_big, s_up, r_up, s_core, r_core, s_rows, r_rows = take(25)
    x_ref, wq_ref, wk_ref, wv_ref, o_s = act_s.at[:T, :D], act_s.at[T : T + D, :D], act_s.at[:D, D:], act_s.at[D : TWO * D, D:], dh_s
    dq_s, p_s, ds_s = dh_s, act_s.at[:T, :D], act_s.at[T : TWO * T, :D]
    dk_s, dv_s, dkv_s = db_s.at[:, :HEAD], db_s.at[:, HEAD : TWO * HEAD], (dg_s, du_s)

    me = lax.axis_index("dp")
    core, j, here, y, x = lax.rem(me, TWO), lax.rem(me, COLUMN), lax.div(me, COLUMN), lax.rem(lax.div(me, COLUMN), NY), lax.div(me, COLUMN * NY)
    z, other = lax.div(j, TWO), ONE - core
    turns = [[p, *(lax.rem(p + d, NX) for d in range(ONE, NX))] for p in (x, y)]
    above = [z, *(lax.rem(z + k, NZ) for k in range(ONE, NZ))]
    column_start = here * COLUMN
    plane = {(a, b): (turns[ZERO][a] * NY + turns[ONE][b]) * COLUMN + z * TWO for a in range(NX) for b in range(NY)}
    along = [[plane[d, ZERO] + core for d in (ONE, 3)], [plane[ZERO, d] + core for d in (ONE, 3)]]
    upward = [column_start + k * TWO + core for k in above]
    partner = column_start + z * TWO + other

    def copy(src, dst, s, r, to):
        return pltpu.make_async_remote_copy(src_ref=src, dst_ref=dst, send_sem=s, recv_sem=r, device_id={"dp": to}, device_id_type=MESH)

    def lanes(half, t, width):
        return pl.ds(pl.multiple_of(half * (width // TWO) + t * LANES, LANES), LANES)

    wide = lambda v: v.astype(f32)
    low = lambda v: v.astype(bf16)

    _mark("start")

    def stream(i, slot):
        out = []
        for k, half in enumerate((core, other)):
            span, to = lanes(half, i, FF), pl.ds(k * LANES, LANES)
            for n, (src, dst) in enumerate(((wg_hbm.at[:, span], wg_s.at[slot, :, to]), (wu_hbm.at[:, span], wu_s.at[slot, :, to]), (wd_hbm.at[span, :], wd_s.at[slot, to, :]))):
                out.append(pltpu.make_async_copy(src, dst, s_w.at[slot, n]))
        return out

    ahead = [pltpu.make_async_copy(x_hbm.at[r, :], x_ref.at[r, :], s_in.at[i]) for i, r in enumerate(pl.ds(k * STEP, STEP) for k in range(T // STEP))]
    for src, dst in ((wq_hbm, wq_ref), (table_hbm, rot_ref), (wk_hbm, wk_ref), (wv_hbm, wv_ref), (wo_hbm, wo_ref), (dy_hbm, dy_ref)):
        ahead.append(pltpu.make_async_copy(src, dst, s_in.at[len(ahead)]))
    for c in (ahead[5], ahead[ZERO], ahead[4], *ahead[6:8], *ahead[ONE:4], *ahead[8:]):
        c.start()
    places = {}
    for k, ref in enumerate((m_hbm, v_hbm)):
        lane = ZERO
        for name in NAMES:
            src = ref[INDEX[name]]
            if name == "w_down":
                dst, sem = nine_in.at[k], len(ahead) + ONE
            else:
                dst, sem = three_in.at[k, :, :, pl.ds(lane, src.shape[-ONE])], len(ahead)
                places[name] = lane
                lane += src.shape[-ONE]
            pltpu.make_async_copy(src, dst, s_in.at[sem]).start()
    for c in stream(ZERO, ZERO):
        c.start()
    for (name, t, n), u in zip(ORDER, STARTS):
        w = weights[INDEX[name]]
        pltpu.make_async_copy(w.at[x, y, :, :, lanes(core, t, w.shape[-ONE])], old.at[pl.ds(u, n)], s_old).start()

    barrier = pltpu.get_barrier_semaphore()
    peers = [column_start + k * TWO + c for k in above[ONE:] for c in (ZERO, ONE)]
    peers += [first + c for ab, first in plane.items() if any(ab) for c in (ZERO, ONE)]
    peers += [partner]
    for to in peers:
        pl.semaphore_signal(barrier, inc=ONE, device_id={"dp": to}, device_id_type=MESH)

    _mark("front")
    ahead[5].wait()

    def angles(i, _):
        table_ref[pl.ds(pl.multiple_of(i * FINE, FINE), FINE), :] = (
            rot_ref[pl.ds(i, ONE), :] * rot_ref[TWO * FINE : 3 * FINE, :] + rot_ref[pl.ds(FINE + i, ONE), :] * rot_ref[3 * FINE :, :]
        )

    lax.fori_loop(ZERO, FINE, angles, None)
    for i in range(T // STEP):
        r = slice(i * STEP, (i + ONE) * STEP)
        ahead[i].wait()
        if i == ZERO:
            for c in (ahead[4], *ahead[6:8]):
                c.wait()
        w = wide(x_ref[r, :])
        a = low(w * norm_scale(w))
        at_ref[:, r] = a.T
        cos, sin = cos_sin(table_ref[r, :])

        def turned(t):
            t = t.astype(bf16).astype(f32)
            return (t * cos + pltpu.roll(t, HALF, ONE) * sin).astype(bf16)

        q = dot(a, wq_ref[...])
        for h in range(HEADS):
            q_ref[h, r, :] = turned(q[:, h * HEAD : (h + ONE) * HEAD])
        k, v = dot(a, wk_ref[...]), dot(a, wv_ref[...]).astype(bf16)
        for g in range(KV):
            one = turned(k[:, g * HEAD : (g + ONE) * HEAD])
            k_ref[g, r, :] = one
            kt_ref[g, :, r] = one.T
            v_ref[g, r, :] = v[:, g * HEAD : (g + ONE) * HEAD]
            vt_ref[g, :HEAD, r] = v[:, g * HEAD : (g + ONE) * HEAD].T
    for g in range(KV):
        vt_ref[g, HEAD:, :] = jnp.ones((16, T), bf16)


    _mark("moments")
    packed[...] = jnp.zeros_like(packed)
    for k, ref in enumerate((three_in, nine_in)):
        pltpu.make_async_copy(ref, ref, s_in.at[len(ahead) + k]).wait()
    for half in (ZERO, ONE):
        for (name, t, n), u in zip(ORDER, STARTS):
            a = half * (m_hbm[INDEX[name]].shape[-ONE] // TWO) + t * LANES
            for k in (ZERO, ONE):
                if n == ONE:
                    at = places[name] + a
                    packed[half, SLOT[u], 3 * k : 3 * k + 3, :] = three_in[k, :, ZERO, at : at + LANES]
                else:
                    s = len(THREE) + 4 * t + TWO * k
                    packed[half, s] = nine_in[k, ZERO:8, ZERO, a : a + LANES]
                    packed[half, s + ONE, ZERO:ONE, :] = nine_in[k, 8:9, ZERO, a : a + LANES]
    moments[j] = packed[core]
    for k in BATCHES:
        for u in range(FILLED[k] * PART, PIECE[k] * NZ):
            cols[k][u] = jnp.zeros((ROWS // PART, LANES), bf16)
    _mark("barrier")
    pl.semaphore_wait(barrier, len(peers))

    for r in range(ONE, COLUMN):
        to = lax.rem(j + r, COLUMN)
        copy(packed.at[lax.rem(to, TWO)], moments.at[j], s_mv, r_mv, column_start + to).start()
    their_moments = copy(moments.at[pl.ds(ZERO, COLUMN - ONE)], moments.at[pl.ds(ZERO, COLUMN - ONE)], s_mv, r_mv, partner)

    weights_s = (do_s, b_ref)
    _mark("f_att")
    for i in range(T // STEP):
        n = (i + ONE) * STEP
        r = slice(i * STEP, n)
        ok = causal(STEP)

        def heads(g):
            tops = []
            for k in range(GROUP):
                q = q_ref[g * GROUP + k, r, :]
                scores = [dot(k_ref[g, a : min(a + KEYS, n), :], q, ONE, ONE) for a in range(ZERO, n, KEYS)]
                last = scores[-ONE]
                own = jnp.where(ok, last[last.shape[ZERO] - STEP :, :], HIDDEN)
                scores[-ONE] = own if last.shape[ZERO] == STEP else jnp.concatenate([last[: last.shape[ZERO] - STEP, :], own], axis=ZERO)
                top = functools.reduce(jnp.maximum, [jnp.max(t, axis=ZERO, keepdims=True) for t in scores])
                for a, t in zip(range(ZERO, n, KEYS), scores):
                    weights_s[g][a : a + t.shape[ZERO], k * STEP : (k + ONE) * STEP] = low(jnp.exp2((t - top) * E))
                tops.append(top)
            out = dot(vt_ref[g, :, :n], weights_s[g][:n, :])
            for k, top in enumerate(tops):
                h, own = g * GROUP + k, slice(k * STEP, (k + ONE) * STEP)
                total = out[HEAD : HEAD + ONE, own]
                o = low(out[:HEAD, own] * (ONE / total))
                rows = slice(h * HEAD, (h + ONE) * HEAD)
                ot_ref[rows, r] = o
                o_s[r, rows] = o.T
                lse_ref[h, :, r] = top * E + jnp.log2(total)

        for g in range(KV):
            heads(g)

    _mark("f_wo")
    ahead[8].wait()
    for i in range(T // STEP):
        r = slice(i * STEP, (i + ONE) * STEP)
        out = dot(o_s[r, :], wo_ref[...]).astype(bf16)
        h = (x_ref[r, :].astype(f32) + out.astype(f32)).astype(bf16)
        h_ref[r, :] = h
        w = wide(h)
        b = low(w * norm_scale(w))
        b_ref[r, :] = b
        bt_ref[:, r] = b.T

    def d2d(u, n, slot, number):
        return copy(give.at[:, :, pl.ds(slot, n)], out_w.at[core, :, :, pl.ds(u, n)], s_give.at[slot], r_give.at[number], partner)

    def send_half(flow):
        d2d(flow.u, flow.n, flow.slot, flow.number).start()

    def half_sent(flow):
        d2d(flow.u, flow.n, flow.slot, flow.number).wait_send()

    def block(flow, k, a):
        units = pl.ds(flow.u, flow.n)
        return out_w.at[core, k, a, units] if flow.colour == ZERO else out_w.at[core, a, k, units]

    FIRST, LAST = pl.ds(ZERO, TWO), pl.ds(TWO, TWO)

    def hop(flow, i):
        axis, back = (flow.colour, ONE - flow.colour)[i // 6], i % TWO
        k = turns[axis][((TWO, TWO), (ONE, 3), (ONE, 3))[i % 6 // TWO][back]]
        s, r, to = s_hop.at[i // 6], (r_relay.at[i // 6, flow.number, back] if i % 6 < TWO else r_fin.at[i // 6, flow.number]), along[axis][back]
        u, n = flow.u, flow.n
        if i < 6:
            part = (FIRST, LAST, LAST, FIRST, FIRST, LAST)[i]
            dst = relay.at[back, :, pl.ds(u, n)] if i < TWO else fin.at[back, part, pl.ds(u, n)]
            return copy(block(flow, k, part), dst, s, r, to)
        half = n // TWO
        lo, hi = pl.ds(u, half), pl.ds(u + half, n - half)
        part = (lo, hi, hi, lo, lo, hi)[i - 6]
        return copy(fin.at[ZERO, k, part], (relay2 if i < 8 else fin2).at[back, part], s, r, to)

    def summed(batch, i):
        return gcs[batch][pl.ds(i * PART, PART)].reshape(ROWS, LANES)

    def arrived(ref, sem):
        copy(ref, ref, s_rows, sem, partner).wait_recv()

    def gone(ref, sem):
        copy(ref, ref, sem, r_rows, partner).wait_send()

    def stage(flow, k, apart=False):
        u, n = flow.u, flow.n
        units = slice(u, u + n)
        first, second = turns[flow.colour], turns[ONE - flow.colour]
        if k == ZERO:
            d2d(u, n, ZERO, flow.number).wait_recv()

            def add(i, _):
                a, b = lax.div(i, NY), lax.rem(i, NY)
                out_w[core, a, b, units] = low(wide(out_w[core, a, b, units]) + wide(out_w[other, a, b, units]))

            lax.fori_loop(ZERO, PLANE, add, None)
            for i in range(TWO if apart else 4):
                hop(flow, i).start()
        elif k == ONE:
            for d in (ZERO, ONE):
                hop(flow, d).wait_recv()
                for a in range(TWO):
                    dst = block(flow, first[ONE + TWO * d], TWO * d + a)
                    dst[...] = low(wide(dst[...]) + wide(relay[d, a, units]))
                hop(flow, 4 + d).start()
        elif k == TWO:
            arrived(fin.at[:, :, pl.ds(u, n)], r_fin.at[ZERO, flow.number])

            def total(a, _):
                fin[ZERO, a, units] = low(wide(block(flow, first[ZERO], a)[...]) + wide(fin[ZERO, a, units]) + wide(fin[ONE, a, units]))

            lax.fori_loop(ZERO, 4, total, None)
            for i in range(4):
                hop(flow, 6 + i).start()
        elif k == 3:
            half = n // TWO
            for d, part in enumerate((slice(u, u + half), slice(u + half, u + n))):
                hop(flow, 6 + d).wait_recv()
                a = second[ONE + TWO * d]
                fin[ZERO, a, part] = low(wide(fin[ZERO, a, part]) + wide(relay2[d, part]))
                hop(flow, 10 + d).start()
        else:
            arrived(fin2.at[:, pl.ds(u, n)], r_fin.at[ONE, flow.number])
            rows = low(wide(fin[ZERO, second[ZERO], units]) + wide(fin2[ZERO, units]) + wide(fin2[ONE, units]))
            cols[flow.batch][flow.base * PART : (flow.base + n) * PART] = rows.reshape(n * PART, ROWS // PART, LANES)

    def scatter(batch, k):
        n = PIECE[batch]
        return copy(cols[batch].at[pl.ds(above[k] * n, n)], zrs[batch].at[k - ONE], s_zr.at[batch], r_zr.at[batch], upward[k])

    def gather(batch, k):
        own = pl.ds(z * PIECE[batch], PIECE[batch])
        return copy(gcs[batch].at[own], gcs[batch].at[own], s_za.at[batch], r_za.at[batch], upward[k])

    OTHERS = range(ONE, NZ)

    def column(batch, step):
        if step == ZERO:
            for k in OTHERS:
                scatter(batch, k).start()
        elif step == ONE:
            arrived(zrs[batch], r_zr.at[batch])
            n = PIECE[batch]
            for i in range(n):
                total = wide(cols[batch][z * n + i])
                for k in range(NZ - ONE):
                    total += wide(zrs[batch][k, i])
                gcs[batch][z * n + i] = low(total)
            for k in OTHERS:
                gather(batch, k).start()
        else:
            arrived(gcs[batch].at[pl.ds(ZERO, len(OTHERS) * PIECE[batch])], r_za.at[batch])

    def spread_moments():
        their_moments.wait_recv()
        for name, n in (("w_gate", 9), ("wq", 3), ("w_up", 9), ("wo", 5)):
            u = START[name, ZERO]

            def move(i, _):
                for d in range(COLUMN):
                    m_nat[u + i, 3 * d : 3 * d + 3, :] = moments[d, SLOT[u] + i, ZERO:3, :]
                    v_nat[u + i, 3 * d : 3 * d + 3, :] = moments[d, SLOT[u] + i, 3:6, :]

            lax.fori_loop(ZERO, n, move, None)

        def move_down(t, _):
            for d in range(COLUMN):
                for k, nat in enumerate((m_down, v_down)):
                    s = len(THREE) + 4 * t + TWO * k
                    nat[t, 9 * d : 9 * d + 8, :] = moments[d, s]
                    nat[t, 9 * d + 8 : 9 * d + 9, :] = moments[d, s + ONE, ZERO:ONE, :]

        lax.fori_loop(ZERO, 3, move_down, None)

    def keep(r, u, slot):
        for k in range(PLANE):
            rows = slice(k * ROWS, (k + ONE) * ROWS)
            out_w[core, k // NY, k % NY, u] = low(r[rows, :LANES])
            give[k // NY, k % NY, slot] = low(r[rows, LANES:])

    def pair(ref, t):
        n = ref.shape[ONE]
        return jnp.concatenate([ref[:, lanes(core, t, n)], ref[:, lanes(other, t, n)]], axis=ONE)

    during = {}

    def when(i, *stages):
        during[i] = stages

    when(3, (GATES[ZERO], ZERO), (UPS[ZERO], ZERO))
    when(5, (GATES[ZERO], ONE), (UPS[ZERO], ONE))
    when(6, (GATES[ONE], ZERO), (UPS[ONE], ZERO))
    when(7, (GATES[ZERO], TWO), (UPS[ZERO], TWO))
    when(8, (GATES[ONE], ONE), (UPS[ONE], ONE), (GATES[ZERO], 3), (UPS[ZERO], 3))

    ahead[9].wait()
    db_s[...] = jnp.zeros_like(db_s)
    _mark("mlp")

    def step(i, _):
        slot = lax.rem(i, TWO)
        for k, ref in enumerate((wg_s, wu_s, wd_s)):
            pltpu.make_async_copy(ref.at[slot], ref.at[slot], s_w.at[slot, k]).wait()

        @pl.when(i + ONE < TILES)
        def _():
            for c in stream(i + ONE, ONE - slot):
                c.start()

        turn = lax.rem(i, 3)

        @pl.when(i >= 3)
        def _():
            for k in (ZERO, 3):
                d2d(ZERO, ONE, k + turn, ZERO).wait_send()

        wg, wu, wd = wg_s[slot], wu_s[slot], wd_s[slot]
        own_rows, other_rows = lanes(core, i, FF), lanes(other, i, FF)
        for c in range(TWO):
            r = slice(c * (T // TWO), (c + ONE) * (T // TWO))
            g, u = dot(b_ref[r, :], wg), dot(b_ref[r, :], wu)
            da = wide(low(dot(dy_ref[r, :], wd, ONE, ONE)))
            s = ONE / (ONE + jnp.exp(-g))
            silu = g * s
            act = low(silu * u).T
            act_s[own_rows, r] = act[:LANES]
            act_s[other_rows, r] = act[LANES:]
            du_s[r, :] = low(da * silu)
            dg_s[r, :] = low(da * u * (s + silu * (ONE - s)))
        for k, stages in during.items():

            @pl.when(i == k)
            def _(stages=stages):
                for flow, n in stages:
                    stage(flow, n)

        for ref, first, k in ((dg_s, START["w_gate", ZERO], ZERO), (du_s, START["w_up", ZERO], 3)):
            keep(dot(bt_ref[...], ref[...]), first + i, k + turn)
        db_s[...] += dot(dg_s[...], wg, ONE, ONE) + dot(du_s[...], wu, ONE, ONE)
        for first, k in ((START["w_gate", ZERO], ZERO), (START["w_up", ZERO], 3)):
            d2d(first + i, ONE, k + turn, k + lax.div(i, 3)).start()

    lax.fori_loop(ZERO, TILES, step, None)

    def down(flow, t, reused):
        for k in reused:
            d2d(ZERO, ONE, k, ZERO).wait_send()
        dy = pair(dy_ref, t)
        n = FF // NX

        for a in range(NX):
            r = dot(act_s[a * n : (a + ONE) * n, :], dy)
            for k in range(NY):
                for i in range(3):
                    rows = slice((3 * k + i) * ROWS, (3 * k + i + ONE) * ROWS)
                    out_w[core, a, k, flow.u + i] = low(r[rows, :LANES])
                    give[a, k, flow.slot + i] = low(r[rows, LANES:])
        send_half(flow)

    _mark("down0")
    down(DOWN0, ZERO, [])
    stage(GATES[TWO], ZERO)
    stage(UPS[TWO], ZERO)
    _mark("down1")
    down(DOWN1, ONE, [])
    stage(GATES[ZERO], 4)
    stage(UPS[ZERO], 4)
    stage(GATES[ONE], TWO)
    stage(UPS[ONE], TWO)
    _mark("down2")
    down(DOWN2, TWO, range(3))
    stage(DOWN0, ZERO)

    _mark("norm")
    for i in range(T // STEP):
        r = slice(i * STEP, (i + ONE) * STEP)
        w, db = wide(h_ref[r, :]), db_s[r, :]
        s = norm_scale(w)
        dh = low(wide(dy_ref[r, :]) + s * (db - w * (s * s * jnp.mean(db * w, axis=ONE, keepdims=True))))
        dh_s[r, :] = dh
        do = low(dot(dh, wo_ref[...], ONE, ONE))
        do_s[r, :] = do
        for h in range(HEADS):
            rows = slice(h * HEAD, (h + ONE) * HEAD)
            delta_s[h, :, r] = jnp.sum(wide(do[:, rows].T) * wide(ot_ref[rows, r]), axis=ZERO, keepdims=True)
        if i == ONE:
            stage(GATES[ONE], 3)
            stage(UPS[ONE], 3)
            stage(DOWN1, ZERO)
    stage(GATES[TWO], ONE)
    stage(UPS[TWO], ONE)

    _mark("wo")
    for k in range(3):
        d2d(ZERO, ONE, 3 + k, ZERO).wait_send()
    for i in range(3):
        keep(dot(ot_ref[...], pair(dh_s, i)), WO.u + i, WO.slot + i)
    send_half(WO)
    stage(GATES[ONE], 4)
    stage(UPS[ONE], 4)
    column(ZERO, ZERO)
    stage(DOWN0, ONE)
    stage(DOWN2, ZERO)

    _mark("att")
    later = {
        (ZERO, ZERO): [],
        (ZERO, ONE): [(GATES[TWO], TWO), (UPS[TWO], TWO), (DOWN1, ONE), (WO, ZERO)],
        (ZERO, TWO): [],
        (ZERO, 3): [(GATES[TWO], 3), (UPS[TWO], 3), (DOWN0, TWO), (DOWN2, ONE)],
        (ONE, ZERO): [(DOWN1, TWO), (WO, ONE)],
        (ONE, ONE): [(ZERO, ONE), (GATES[TWO], 4), (UPS[TWO], 4), (DOWN0, 3)],
        (ONE, TWO): [(DOWN1, 3), (DOWN2, TWO)],
        (ONE, 3): [(DOWN0, 4), (WO, TWO)],
    }

    def group(g, _):
        for i in range(T // STEP):
            n = (i + ONE) * STEP
            r = slice(i * STEP, n)
            ok = causal(STEP)
            qs, dos = [], []
            for k in range(GROUP):
                h = g * GROUP + k
                q, do = q_ref[h, r, :], do_s[r, pl.ds(pl.multiple_of(h * HEAD, HEAD), HEAD)]
                qs.append(q)
                dos.append(do)
                to = slice(k * STEP, (k + ONE) * STEP)
                for a in range(ZERO, n, KEYS):
                    keys = slice(a, min(a + KEYS, n))
                    p = jnp.exp2(dot(k_ref[g, keys, :], q, ONE, ONE) * E - lse_ref[h, :, r])
                    if a + KEYS >= n:
                        own = jnp.where(ok, p[n - STEP - a :, :], 0.0)
                        p = own if n - STEP == a else jnp.concatenate([p[: n - STEP - a, :], own], axis=ZERO)
                    p_s[keys, to] = low(p)
                    ds_s[keys, to] = low(p * (dot(v_ref[g, keys, :], do, ONE, ONE) - delta_s[h, :, r]))
            dv = dot(p_s[:n, :], jnp.concatenate(dos, axis=ZERO))
            dk = dot(ds_s[:n, :], jnp.concatenate(qs, axis=ZERO))
            dq = dot(kt_ref[g, :, :n], ds_s[:n, :])
            cos, sin = cos_sin(table_ref[r, :])
            for k in range(GROUP):
                t = dq[:, k * STEP : (k + ONE) * STEP].T * SCALE
                dq_s[r, pl.ds(pl.multiple_of((g * GROUP + k) * HEAD, HEAD), HEAD)] = low(t * cos - pltpu.roll(t, HALF, ONE) * sin)
            if i == ZERO:
                dv_s[:n], dk_s[:n] = dv, dk
            else:
                dv_s[: n - STEP] += dv[: n - STEP]
                dk_s[: n - STEP] += dk[: n - STEP]
                dv_s[r], dk_s[r] = dv[n - STEP :], dk[n - STEP :]
            for which in (ZERO, ONE):
                if later[which, i]:

                    @pl.when(g == which)
                    def _():
                        for flow, m in later[which, i]:
                            if isinstance(flow, Flow):
                                stage(flow, m)
                            else:
                                column(flow, m)

        span = pl.ds(pl.multiple_of(g * HEAD, HEAD), HEAD)
        for i in range(T // STEP):
            r = slice(i * STEP, (i + ONE) * STEP)
            cos, sin = cos_sin(table_ref[r, :])
            t = dk_s[r, :] * SCALE
            dkv_s[ZERO][r, span] = low(t * cos - pltpu.roll(t, HALF, ONE) * sin)
            dkv_s[ONE][r, span] = low(dv_s[r, :])

    lax.fori_loop(ZERO, KV, group, None)

    _mark("qkv")
    half_sent(DOWN0)
    half_sent(DOWN1)
    for i in range(3):
        keep(dot(at_ref[...], pair(dq_s, i)), WQ.u + i, WQ.slot + i)
    send_half(WQ)
    for i in (ZERO, ONE):
        keep(dot(at_ref[...], pair(dkv_s[i], ZERO)), WKV.u + i, WKV.slot + i)
    send_half(WKV)

    _mark("tail")
    stage(WQ, ZERO, True)
    stage(WKV, ZERO, True)
    for flow in (WQ, WKV):
        hop(flow, TWO).start()
        hop(flow, 3).start()
    stage(DOWN1, 4)
    column(ONE, ZERO)
    stage(DOWN2, 3)
    stage(WO, 3)
    spread_moments()
    _mark("tail_1")
    stage(WQ, ONE)
    stage(WKV, ONE)
    stage(DOWN2, 4)
    stage(WO, 4)
    column(TWO, ZERO)
    _mark("tail_2")
    stage(WQ, TWO)
    stage(WKV, TWO)
    column(ONE, ONE)
    _mark("tail_3")
    stage(WQ, 3)
    stage(WKV, 3)
    _mark("tail_4")
    stage(WQ, 4)
    stage(WKV, 4)
    column(3, ZERO)
    column(TWO, ONE)
    _mark("tail_z0")
    column(ZERO, TWO)
    gone(out_w.at[core, pl.ds(ZERO, 3)], s_hop.at[ZERO])
    gone(out_w.at[core, ZERO, pl.ds(ZERO, 3)], s_hop.at[ONE])
    _mark("tail_z1")
    column(3, ONE)
    _mark("tail_z2")
    column(ONE, TWO)
    column(TWO, TWO)

    def squares(batch, total):
        def more(i, total):
            g = wide(summed(batch, i))
            return total + (g * g).reshape(ROWS // 8, 8, LANES).sum(ZERO)

        return lax.fori_loop(ZERO, FILLED[batch], more, total)

    first_squares = functools.reduce(lambda total, batch: squares(batch, total), BATCHES[:-ONE], jnp.zeros((8, LANES), f32))
    _mark("tail_z3")
    column(3, TWO)
    for flow in (DOWN2, WO, WQ, WKV):
        half_sent(flow)
    for batch in BATCHES:
        gone(zrs[batch], s_zr.at[batch])
        gone(gcs[batch].at[pl.ds(ZERO, len(OTHERS) * PIECE[batch])], s_za.at[batch])
    their_moments.wait_send()

    _mark("norms")
    mine = norms.at[here * TWO + core]
    mine[...] = jnp.sum(squares(BATCHES[-ONE], first_squares), axis=ZERO, keepdims=True)
    for ab, first in plane.items():
        for c in (core, other):
            if any(ab) or c is other:
                copy(mine, mine, s_norm, r_norm, first + c).start()
    pltpu.make_async_copy(old, old, s_old).wait()
    all_norms = copy(norms.at[pl.ds(ZERO, TWO * PLANE - ONE)], norms.at[pl.ds(ZERO, TWO * PLANE - ONE)], s_norm, r_norm, partner)
    all_norms.wait_recv()
    total = norms[...].sum(axis=ZERO)
    total = jnp.sum(total, axis=ONE, keepdims=True)
    factor = jnp.minimum(1.0, 0.5 * lax.rsqrt(total * (1.0 / COUNT) + 1e-30))

    _mark("adam")

    def stepped(w, m, v, g):
        g = g * factor
        m = 0.9 * m + 0.1 * g
        v = 0.95 * v + 0.05 * g * g
        return low(w - 0.02 * (m * lax.rsqrt(v + 1e-8) + 0.1 * w))

    def new_units(name, t, n):
        u = START[name, t]
        batch, first = PLACE[u]

        def unit(i, _):
            if name == "w_down":
                rows = pl.ds(pl.multiple_of(i * ROWS, ROWS), ROWS)
                m, v = m_down[t, rows, :], v_down[t, rows, :]
            else:
                m, v = m_nat[u + i], v_nat[u + i]
            out_w[core, x, y, u + i] = stepped(wide(old[u + i]), m, v, wide(summed(batch, first + i)))

        lax.fori_loop(ZERO, n, unit, None)

    for k, (name, t) in enumerate((name, t) for (name, t, n), u in zip(ORDER, STARTS) if UPRIGHT <= u < UPRIGHT + NZ):

        @pl.when(z == k)
        def _(name=name, t=t):
            new_units(name, t, ONE)

    def upright(k, part=pl.ds(ZERO, NX)):
        return out_w.at[core, part, :, pl.ds(UPRIGHT + above[k], ONE)]

    mine = out_w.at[core, x, y, pl.ds(UPRIGHT + z, ONE)]
    for ab, first in plane.items():
        if any(ab):
            copy(mine, mine, s_up.at[ZERO], r_up.at[ZERO], first + core).start()
    for name, t, n in RUNS:
        new_units(name, t, n)

    _mark("ag0")

    def slot(colour, ps, pb, h=None):
        u, n = COLOURS[colour]
        if h is not None:
            u, n = (u, n // TWO) if h == ZERO else (u + n // TWO, n - n // TWO)
        units = pl.ds(u, n)
        return out_w.at[core, pb, ps, units] if colour == ZERO else out_w.at[core, ps, pb, units]

    def give_partner(v):
        copy(v, v, s_core, r_core, partner).start()

    def to_partner(colour, ps, pb):
        give_partner(slot(colour, ps, pb))

    def send(colour, big, rel, ps, pb, h, d, kind):
        v = slot(colour, ps, pb, h)
        copy(v, v, s_ag.at[big], r_big.at[colour, rel, kind] if big else r_small.at[colour, kind], along[colour if big else ONE - colour][d]).start()

    def came(colour, big, rel, kind):
        units = pl.ds(*COLOURS[colour])
        arrived(out_w.at[core, pl.ds(ZERO, TWO), ZERO, units] if kind == ZERO else out_w.at[core, ZERO, ZERO, units], r_big.at[colour, rel, kind] if big else r_small.at[colour, kind])

    def spot(colour):
        return turns[ONE - colour], turns[colour]

    def big_own(colour, rel):
        ps, pb = spot(colour)
        for d in (ZERO, ONE):
            send(colour, ONE, rel, ps[rel], pb[ZERO], None, d, ZERO)

    def big_forward(colour, rel):
        ps, pb = spot(colour)
        came(colour, ONE, rel, ZERO)
        for d in (ZERO, ONE):
            send(colour, ONE, rel, ps[rel], pb[3 - TWO * d], d, d, ONE)
        for d in (ZERO, ONE):
            to_partner(colour, ps[rel], pb[3 - TWO * d])

    def big_far(colour, rel):
        ps, pb = spot(colour)
        came(colour, ONE, rel, ONE)
        to_partner(colour, ps[rel], pb[TWO])

    def rise(k):
        arrived(out_w.at[core, pl.ds(ZERO, 3), ZERO, pl.ds(ZERO, 5)] if k == ZERO else out_w.at[core, :, :, pl.ds(ZERO, TWO if k < 4 else ONE)], r_up.at[k])
        came_from = sorted({-k % NZ, k}, reverse=True)
        if k < 4:
            for d in (ZERO, ONE):
                v = upright(came_from[min(d, k)], pl.ds(ZERO, NX) if k < 3 else (FIRST, LAST)[d])
                copy(v, v, s_up.at[ONE], r_up.at[k + ONE], upward[(ONE, NZ - ONE)[d]]).start()
        for c in came_from:
            give_partner(upright(c))

    def small_own(colour):
        ps, pb = spot(colour)
        for d in (ZERO, ONE):
            send(colour, ZERO, ZERO, ps[ZERO], pb[ZERO], None, d, ZERO)

    def small_forward(colour):
        ps, pb = spot(colour)
        came(colour, ZERO, ZERO, ZERO)
        for d in (ZERO, ONE):
            send(colour, ZERO, ZERO, ps[3 - TWO * d], pb[ZERO], d, d, ONE)
        for rel in (3, ONE):
            big_own(colour, rel)
            to_partner(colour, ps[rel], pb[ZERO])

    def small_far(colour):
        ps, pb = spot(colour)
        came(colour, ZERO, ZERO, ONE)
        big_own(colour, TWO)
        to_partner(colour, ps[TWO], pb[ZERO])

    small_own(ZERO)
    small_own(ONE)
    for colour in (ZERO, ONE):
        ps, pb = spot(colour)
        big_own(colour, ZERO)
        to_partner(colour, ps[ZERO], pb[ZERO])

    _mark("rows")

    def picker(height, each, of):
        row, col = lax.broadcasted_iota(jnp.int32, (height, of), ZERO), lax.broadcasted_iota(jnp.int32, (height, of), ONE)
        half = height // TWO
        ours = (row < each) & (col == each * j + row)
        theirs = (row >= half) & (row < half + each) & (col == each * (j + ONE - TWO * core) + row - half)
        return (ours | theirs).astype(f32).astype(bf16)

    three, nine = picker(16, 3, ROWS), picker(32, 9, 3 * ROWS)
    for (name, t, n), u in zip(ORDER, STARTS):
        batch, a = PLACE[u]
        if n == ONE:
            rows = dot(three, summed(batch, a)) * factor
            out_g[core, SLOT[u]], rows_out[SLOT[u]] = rows[:8], rows[8:]
        else:
            rows = dot(nine, jnp.concatenate([summed(batch, a + i) for i in range(3)], axis=ZERO)) * factor
            s = len(THREE) + TWO * t
            for k in (ZERO, ONE):
                out_g[core, s + k], rows_out[s + k] = rows[8 * k : 8 * k + 8], rows[16 + 8 * k : 24 + 8 * k]
    own_rows = copy(rows_out, out_g.at[core], s_rows, r_rows, partner)
    own_rows.start()

    _mark("ag1")
    small_forward(ZERO)
    small_forward(ONE)
    rise(ZERO)
    _mark("ag2")
    big_forward(ZERO, ZERO)
    big_forward(ONE, ZERO)
    rise(ONE)
    small_far(ZERO)
    small_far(ONE)
    _mark("ag3")
    big_forward(ZERO, 3)
    big_forward(ONE, 3)
    rise(TWO)
    big_forward(ZERO, ONE)
    big_forward(ONE, ONE)
    big_far(ZERO, ZERO)
    big_far(ONE, ZERO)
    rise(3)
    own_rows.wait()
    for half in (ZERO, ONE):
        for (name, t, n), u in zip(ORDER, STARTS):
            a, s = half * (m_hbm[INDEX[name]].shape[-ONE] // TWO) + t * LANES, len(THREE) + TWO * t
            for s, r, rows in [(SLOT[u], ZERO, 3)] if n == ONE else [(s, ZERO, 8), (s + ONE, 8, ONE)]:
                old_ref, new_ref, at = (three_in, three_out, places[name] + a) if n == ONE else (nine_in, nine_out, a)
                g = out_g[half, s, ZERO:rows, :]
                here = (slice(r, r + rows), ZERO, slice(at, at + LANES))
                new_ref[(ZERO, *here)] = 0.9 * old_ref[(ZERO, *here)] + 0.1 * g
                new_ref[(ONE, *here)] = 0.95 * old_ref[(ONE, *here)] + 0.05 * g * g
    _mark("ag4")
    big_forward(ZERO, TWO)
    big_forward(ONE, TWO)
    for rel in (3, ONE):
        big_far(ZERO, rel)
        big_far(ONE, rel)
    rise(4)
    _mark("ag5")
    big_far(ZERO, TWO)
    big_far(ONE, TWO)
    arrived(out_w.at[other], r_core)
    gone(out_w.at[core], s_core)
    shared = pl.ds(ZERO, UNITS - NZ)
    gone(out_w.at[core, ZERO, pl.ds(ZERO, 3), shared], s_ag.at[ZERO])
    gone(out_w.at[core, pl.ds(ZERO, 3), :, shared], s_ag.at[ONE])
    gone(out_w.at[core, pl.ds(ZERO, 3), ZERO, pl.ds(ZERO, 5)], s_up.at[ZERO])
    gone(out_w.at[core, :, :, pl.ds(ZERO, 7)], s_up.at[ONE])
    all_norms.wait_send()
    _mark("end")


def layer_step(x, dy, weights, m, v):
    view = lambda t: t.reshape(NX, NY, t.shape[ZERO] // (PLANE * ROWS), ROWS, t.shape[ONE])
    any_ = pl.BlockSpec(memory_space=pl.ANY)
    vmem = pl.BlockSpec(memory_space=pltpu.VMEM)
    low, wide = lambda *s: pltpu.VMEM(s, bf16), lambda *s: pltpu.VMEM(s, f32)
    unit = lambda *lead: low(*lead, ROWS, LANES)
    dma = lambda *shape: pltpu.SemaphoreType.DMA(shape)
    flows = len(FLOWS)
    moments = wide(TWO, 3, ONE, sum(t.shape[-ONE] for t in m[:-ONE])), wide(TWO, 9, ONE, D)
    scratch = [
        wide(4 * FINE, HEAD), wide(T, HEAD), low(D, D), low(T, D), low(D, T), low(HEADS, T, HEAD), low(KV, T, HEAD), low(KV, T, HEAD), low(KV, HEAD, T), low(KV, HEAD + 16, T),
        low(D, T), wide(HEADS, ONE, T), low(T, D), low(T, D), low(D, T),
        low(TWO, D, STEP), low(TWO, D, STEP), low(TWO, STEP, D), low(T, STEP), low(T, STEP),
        low(FF, T), wide(T, D), low(T, D), low(T, D), wide(HEADS, ONE, T),
        unit(NX, NY, GIVE), unit(TWO, TWO, UNITS), unit(TWO, 4, UNITS), unit(TWO, UNITS), unit(TWO, UNITS),
        *(low(*lead(p), ROWS // PART, LANES) for lead in (lambda p: (NZ * p,), lambda p: (NZ - ONE, p), lambda p: (NZ * p,)) for p in PIECE),
        unit(UNITS), *moments, wide(TWO, SLOTS, 8, LANES), wide(COLUMN, SLOTS, 8, LANES),
        wide(UNITS, ROWS, LANES), wide(UNITS, ROWS, LANES), wide(3, 3 * ROWS, LANES), wide(3, 3 * ROWS, LANES),
        wide(TWO * PLANE, ONE, LANES), wide(ROW_SLOTS, 8, LANES), wide(TWO, ROW_SLOTS, 8, LANES),
        dma(12), dma(TWO, 3), dma(), dma(GIVE), dma(flows), dma(TWO), dma(TWO, flows, TWO), dma(TWO, flows), *[dma(len(BATCHES))] * 4, dma(), dma(), dma(), dma(),
        dma(TWO), dma(TWO, TWO), dma(TWO, 4, TWO), dma(TWO), dma(5), dma(), dma(), dma(), dma(),
    ]
    return pl.pallas_call(
        _step,
        in_specs=[any_] * 31,
        out_specs=[vmem] * 3,
        out_shape=[unit(TWO, NX, NY, UNITS), *moments],
        scratch_shapes=scratch,
        compiler_params=pltpu.CompilerParams(collective_id=ZERO, has_side_effects=True, vmem_limit_bytes=50 * TWO**20),
        name="step",
    )(x, dy, jnp.asarray(rotary()), *weights, *map(view, weights), *m, *v)


def _finish(w_ref, three_ref, nine_ref, *refs):
    w_out, moments_out, sem = refs[:7], (refs[7:14], refs[14:21]), refs[21]
    copies = []
    for half in (ZERO, ONE):
        for i, (name, t, n) in enumerate(ORDER):
            o = w_out[INDEX[name]]
            a = half * (o.shape[-ONE] // TWO) + t * LANES
            copies.append(pltpu.make_async_copy(w_ref.at[half, :, :, pl.ds(STARTS[i], n)], o.at[:, :, :, :, pl.ds(a, LANES)], sem.at[ZERO]))
    for k in (ZERO, ONE):
        lane = ZERO
        for name, o in zip(NAMES, moments_out[k]):
            if name == "w_down":
                copies.append(pltpu.make_async_copy(nine_ref.at[k], o, sem.at[TWO]))
            else:
                copies.append(pltpu.make_async_copy(three_ref.at[k, :, :, pl.ds(lane, o.shape[-ONE])], o, sem.at[ONE]))
                lane += o.shape[-ONE]
    for c in copies:
        c.start()
    for k, ref in enumerate((w_ref, three_ref, nine_ref)):
        pltpu.make_async_copy(ref, ref, sem.at[k]).wait()


def finish(new, m, v, like):
    any_ = pl.BlockSpec(memory_space=pl.ANY)
    vmem = pl.BlockSpec(memory_space=pltpu.VMEM)
    view = lambda t: (NX, NY, t.shape[ZERO] // (PLANE * ROWS), ROWS, t.shape[ONE])
    out = pl.pallas_call(
        _finish,
        in_specs=[vmem] * 3,
        out_specs=[any_] * 21,
        out_shape=[jax.ShapeDtypeStruct(view(w), w.dtype) for w in like] + [jax.ShapeDtypeStruct(t.shape, t.dtype) for t in (*m, *v)],
        scratch_shapes=[pltpu.SemaphoreType.DMA((3,))],
        compiler_params=pltpu.CompilerParams(vmem_limit_bytes=16 * TWO**20),
        name="finish",
    )(*new)
    return [o.reshape(ONE, *w.shape) for o, w in zip(out[:7], like)], out[7:14], out[14:]


def solution(mesh):
    def step(x, dy, *arrays):
        weights, m, v = (arrays[i : i + 7] for i in (ZERO, 7, 14))
        weights = [w[ZERO] for w in weights]
        m, v = ([t.transpose(ONE, ZERO, TWO) for t in s] for s in (m, v))
        w, m, v = finish(layer_step(x[ZERO], dy[ZERO], weights, m, v), m, v, weights)
        return (*w, *(t.transpose(ONE, ZERO, TWO) for t in (*m, *v)))

    states, all_of, cut = P(("rep", "dp"), None, None), P(None, None, None), P(None, "dp", None)
    return jax.shard_map(
        step,
        mesh=mesh,
        in_specs=(states, states) + (all_of,) * 7 + (cut,) * 14,
        out_specs=(P("rep", None, None),) * 7 + (P("rep", "dp", None),) * 14,
        check_vma=False,
    )
```
